32 devices in a mesh: dp: 32 (over z, y, x, core).
Axes of the slice: x: 2, y: 2, z: 4, core: 2. Of those that a mesh axis runs over, the one named last changes fastest.
Arguments:
- block_input: bfloat16 [32768, 640], P('dp'), may hold values from -6 to 6
- out_cotangent: bfloat16 [32768, 640], P('dp'), may hold values from -6 to 6
- segment_ids: int32 [32768], P('dp'), may hold values from 0 to 1023, as said below
- positions: int32 [32768], P('dp'), may hold values from 0 to 1023, as said below
- tile_count: int32 [32], P('dp'), may hold values from 1 to 8, as said below
- qkv_weight: float32 [640, 1536], P('dp'), may hold values from -0.25 to 0.25
- qkv_first: float32 [640, 1536], P('dp'), may hold values from -6 to 6
- qkv_second: float32 [640, 1536], P('dp'), may hold values from 0.01 to 1
- out_weight: float32 [1024, 640], P('dp'), may hold values from -0.1875 to 0.1875
- out_first: float32 [1024, 640], P('dp'), may hold values from -6 to 6
- out_second: float32 [1024, 640], P('dp'), may hold values from 0.01 to 1
- gate_up_weight: float32 [640, 4096], P('dp'), may hold values from -0.25 to 0.25
- gate_up_first: float32 [640, 4096], P('dp'), may hold values from -6 to 6
- gate_up_second: float32 [640, 4096], P('dp'), may hold values from 0.01 to 1
- down_weight: float32 [2048, 640], P('dp'), may hold values from -0.125 to 0.125
- down_first: float32 [2048, 640], P('dp'), may hold values from -6 to 6
- down_second: float32 [2048, 640], P('dp'), may hold values from 0.01 to 1
- norm_scales: float32 [3072], P('dp'), may hold values from -0.6 to 0.6
- norm_first: float32 [3072], P('dp'), may hold values from -6 to 6
- norm_second: float32 [3072], P('dp'), may hold values from 0.01 to 1
Outputs:
- block_output: bfloat16 [32768, 640], P('dp')
- input_grad: float32 [32768, 640], P('dp')
- qkv_grad: float32 [640, 1536], P('dp')
- out_grad: float32 [1024, 640], P('dp')
- gate_up_grad: float32 [640, 4096], P('dp')
- down_grad: float32 [2048, 640], P('dp')
- norm_grad: float32 [3072], P('dp')
- qkv_new: float32 [640, 1536], P('dp')
- out_new: float32 [1024, 640], P('dp')
- gate_up_new: float32 [640, 4096], P('dp')
- down_new: float32 [2048, 640], P('dp')
- norms_new: float32 [3072], P('dp')
- qkv_first_new: float32 [640, 1536], P('dp')
- out_first_new: float32 [1024, 640], P('dp')
- gate_up_first_new: float32 [640, 4096], P('dp')
- down_first_new: float32 [2048, 640], P('dp')
- norm_first_new: float32 [3072], P('dp')
- qkv_second_new: float32 [640, 1536], P('dp')
- out_second_new: float32 [1024, 640], P('dp')
- gate_up_second_new: float32 [640, 4096], P('dp')
- down_second_new: float32 [2048, 640], P('dp')
- norm_second_new: float32 [3072], P('dp')
The draws below stay inside these ranges and needn't reach their ends.
Inputs may be any that keep to these rules, and one draw needn't show every extreme that they name: `tile_count`: how many of a device's 8 tiles hold tokens; the rows of the remaining tiles are padding. `segment_ids`: within each device's 1024 slots: 0 at the first slot, never falling, rising by at most one from slot to slot; no sequence spans two devices. `positions`: within each device: 0 at every slot where segment_ids changes (and at the device's first slot), else one more than at the slot before.
All inputs are finite; a program needn't handle non-finite values.
Results may differ from the reference program's by a relative error of at most 0.02.
The reference program's roundings to bfloat16 on the way count: a program that leaves them out, or rounds other values in their place, can miss the bound.
Values may be sent and summed in bfloat16 or wider, within the bound.
A program may use at most 192 MiB of HBM per device.

```python
import math
import jax
import jax.numpy as jnp
from jax import lax

D = 640
HQ = 4
HD = 256
FF = 2048
WIN = 512
TILE = 128
TILES_DEV = 8
TOK_DEV = 1024
TOKENS = 32768


def token_layout(key):
    base_key = jax.random.fold_in(key, 11)
    subkeys = jax.random.split(base_key, 5)
    device_count = TOKENS // TOK_DEV
    device_ids = jnp.arange(device_count, dtype=jnp.int32)
    counts = jax.random.randint(subkeys[0], (device_count,), 1, TILES_DEV // 2 + 1, dtype=jnp.int32)
    busy_dev = jax.random.randint(subkeys[1], (device_count,), 0, 8, dtype=jnp.int32) == 0
    counts = jnp.where(busy_dev, TILES_DEV, counts)
    full_dev = jax.random.randint(subkeys[2], (), 0, device_count, dtype=jnp.int32)
    least_dev = (full_dev + 1 + jax.random.randint(subkeys[3], (), 0, device_count - 1, dtype=jnp.int32)) % device_count
    counts = jnp.where(device_ids == full_dev, TILES_DEV, jnp.where(device_ids == least_dev, 1, counts))
    slot_ids = jnp.arange(TOK_DEV, dtype=jnp.int32)
    starts = jax.random.randint(subkeys[4], (device_count, TOK_DEV), 0, 3 * TILE, dtype=jnp.int32) == 0
    starts = starts | (slot_ids == 0)[None, :]
    starts = jnp.where((device_ids == full_dev)[:, None], (slot_ids == 0)[None, :], starts)
    starts = jnp.where((device_ids == least_dev)[:, None], True, starts)
    segments = jnp.cumsum(starts.astype(jnp.int32), axis=1, dtype=jnp.int32) - 1
    begins = lax.cummax(jnp.where(starts, slot_ids[None, :], 0), axis=1)
    positions = slot_ids[None, :] - begins
    return (counts, segments.reshape(-1), positions.reshape(-1))


def draw_tile_count(key, part):
    return token_layout(key)[0]


def draw_segment_ids(key, part):
    return token_layout(key)[1]


def draw_positions(key, part):
    return token_layout(key)[2]


def block_levels(own_key, dims, pieces, smallest, top_value):
    loudness = 1.0
    for dim, shards_of in pieces:
        draws = jax.random.uniform(jax.random.fold_in(jax.random.fold_in(own_key, 6), dim), (shards_of,), jnp.float32, smallest / len(pieces), top_value / len(pieces))
        loudness = loudness * jnp.repeat(jnp.exp(draws), dims[dim] // shards_of).reshape((-1,) + (1,) * (len(dims) - 1 - dim))
    return loudness


def gaussian(rng, dims, scale, bound, cuts=(), held_as=jnp.bfloat16):
    loudness = block_levels(rng, dims, cuts, -0.22, 0.18) if cuts else 1.0
    drawn = jax.random.normal(rng, dims, jnp.float32) * scale * loudness
    return jnp.minimum(jnp.maximum(drawn, -bound), bound).astype(held_as)


def setup_inputs(seed: int = 0) -> dict:
    keys = jax.random.split(jax.random.key(seed), 21)
    block_input = gaussian(keys[0], (TOKENS, D), 1.0, 6.0, ((0, 32),))
    out_cotangent = gaussian(keys[1], (TOKENS, D), 1.0, 6.0, ((0, 32),))
    segment_ids = draw_segment_ids(jax.random.fold_in(keys[20], 71), 0)
    positions = draw_positions(jax.random.fold_in(keys[20], 71), 0)
    tile_count = draw_tile_count(jax.random.fold_in(keys[20], 71), 0)
    qkv_weight = gaussian(keys[5], (D, (HQ + 2) * HD), D ** -0.5, 0.25, ((0, 32),), jnp.float32)
    qkv_first = gaussian(keys[6], (D, (HQ + 2) * HD), 1.0, 6.0, ((0, 32),), jnp.float32)
    qkv_second = jnp.clip(jnp.exp(math.log(1.0) - 4.6051702 * jax.random.uniform(keys[7], (D, (HQ + 2) * HD), jnp.float32) ** block_levels(keys[7], (D, (HQ + 2) * HD), ((0, 32),), -0.2, 0.2)), 0.01, 1.0)
    out_weight = gaussian(keys[8], (HQ * HD, D), (HQ * HD) ** -0.5, 0.1875, ((0, 32),), jnp.float32)
    out_first = gaussian(keys[9], (HQ * HD, D), 1.0, 6.0, ((0, 32),), jnp.float32)
    out_second = jnp.clip(jnp.exp(math.log(1.0) - 4.6051702 * jax.random.uniform(keys[10], (HQ * HD, D), jnp.float32) ** block_levels(keys[10], (HQ * HD, D), ((0, 32),), -0.2, 0.2)), 0.01, 1.0)
    gate_up_weight = gaussian(keys[11], (D, 2 * FF), D ** -0.5, 0.25, ((0, 32),), jnp.float32)
    gate_up_first = gaussian(keys[12], (D, 2 * FF), 1.0, 6.0, ((0, 32),), jnp.float32)
    gate_up_second = jnp.clip(jnp.exp(math.log(1.0) - 4.6051702 * jax.random.uniform(keys[13], (D, 2 * FF), jnp.float32) ** block_levels(keys[13], (D, 2 * FF), ((0, 32),), -0.2, 0.2)), 0.01, 1.0)
    down_weight = gaussian(keys[14], (FF, D), FF ** -0.5, 0.125, ((0, 32),), jnp.float32)
    down_first = gaussian(keys[15], (FF, D), 1.0, 6.0, ((0, 32),), jnp.float32)
    down_second = jnp.clip(jnp.exp(math.log(1.0) - 4.6051702 * jax.random.uniform(keys[16], (FF, D), jnp.float32) ** block_levels(keys[16], (FF, D), ((0, 32),), -0.2, 0.2)), 0.01, 1.0)
    norm_scales = gaussian(keys[17], (4 * D + 2 * HD,), 0.15, 0.6, ((0, 32),), jnp.float32)
    norm_first = gaussian(keys[18], (4 * D + 2 * HD,), 1.0, 6.0, ((0, 32),), jnp.float32)
    norm_second = jnp.clip(jnp.exp(math.log(1.0) - 4.6051702 * jax.random.uniform(keys[19], (4 * D + 2 * HD,), jnp.float32) ** block_levels(keys[19], (4 * D + 2 * HD,), ((0, 32),), -0.2, 0.2)), 0.01, 1.0)
    return dict(block_input=block_input, out_cotangent=out_cotangent, segment_ids=segment_ids, positions=positions, tile_count=tile_count, qkv_weight=qkv_weight, qkv_first=qkv_first, qkv_second=qkv_second, out_weight=out_weight, out_first=out_first, out_second=out_second, gate_up_weight=gate_up_weight, gate_up_first=gate_up_first, gate_up_second=gate_up_second, down_weight=down_weight, down_first=down_first, down_second=down_second, norm_scales=norm_scales, norm_first=norm_first, norm_second=norm_second)


norm_eps = 1e-06
rope_base = 10000.0
beta_one = 0.9
beta_two = 0.999
adam_eps = 1e-08
learn_rate = 0.02
weight_decay = 0.1
adam_step = 3

def rms_scale(values, scales):
    mean_square = lax.optimization_barrier(jnp.mean(values * values, axis=-1, keepdims=True))
    return values * lax.rsqrt(mean_square + norm_eps) * (1.0 + scales)

def gelu_tanh(values):
    inner_term = 0.7978845608028654 * (values + 0.044715 * values * values * values)
    return 0.5 * values * (1.0 + jnp.tanh(inner_term))

def gated_unit(gate_act, up_act):
    return gelu_tanh(gate_act) * up_act

def rotate(values, cosine, sine_table):
    half_dim = values.shape[-1] // 2
    front_half = values[..., :half_dim]
    back_half = values[..., half_dim:]
    return jnp.concatenate([front_half * cosine - back_half * sine_table, back_half * cosine + front_half * sine_table], axis=-1)

def rope_tables(positions, head_dim):
    exponent = jnp.arange(head_dim // 2, dtype=jnp.float32) * (2.0 / head_dim)
    frequency = jnp.power(jnp.float32(rope_base), -exponent)
    angles = positions.astype(jnp.float32)[:, None] * frequency[None, :]
    return (jnp.cos(angles)[:, None, :], jnp.sin(angles)[:, None, :])

def qk_prepare(query_raw, key_raw, q_scale, k_scale, cosine, sine_table):
    return (rotate(rms_scale(query_raw, q_scale), cosine, sine_table), rotate(rms_scale(key_raw, k_scale), cosine, sine_table))

def contract(form, left, right):
    return jnp.einsum(form, left.astype(jnp.float32), right.astype(jnp.float32))

def window_mask(block_index, window, segment_pad, position_pad, live_pad):
    start_row = block_index * window
    query_rows = start_row + jnp.arange(window, dtype=jnp.int32)
    key_rows = start_row - window + jnp.arange(2 * window, dtype=jnp.int32)
    query_seg = segment_pad[start_row + window:start_row + 2 * window]
    key_seg = segment_pad[start_row:start_row + 2 * window]
    query_live = live_pad[start_row + window:start_row + 2 * window]
    key_live = live_pad[start_row:start_row + 2 * window]
    diagonal = key_rows[None, :] == query_rows[:, None]
    earlier = (key_rows[None, :] < query_rows[:, None]) & (query_rows[:, None] - key_rows[None, :] < window)
    same_seq = (query_seg[:, None] == key_seg[None, :]) & query_live[:, None] & key_live[None, :]
    return diagonal | earlier & same_seq

def front_pad(values, window):
    return jnp.concatenate([jnp.zeros((window,) + values.shape[1:], values.dtype), values], axis=0)

def attend_forward(query_bf, key_bf, value_bf, segment_pad, position_pad, live_pad):
    row_count = query_bf.shape[0]
    score_scale = HD ** (-0.5)
    key_padded = front_pad(key_bf, WIN)
    value_padded = front_pad(value_bf, WIN)
    out_blocks = []
    log_blocks = []
    for block_index in range(row_count // WIN):
        start_row = block_index * WIN
        allowed = window_mask(block_index, WIN, segment_pad, position_pad, live_pad)
        query_block = query_bf[start_row:start_row + WIN]
        key_block = key_padded[start_row:start_row + 2 * WIN]
        value_block = value_padded[start_row:start_row + 2 * WIN]
        scores = contract('qhd,kd->hqk', query_block, key_block) * score_scale
        exp_scores = jnp.where(allowed[None], jnp.exp(scores), 0.0)
        exp_total = lax.optimization_barrier(jnp.sum(exp_scores, axis=-1))
        probs_bf = (exp_scores / exp_total[..., None]).astype(jnp.bfloat16)
        out_blocks.append(contract('hqk,kd->qhd', probs_bf, value_block).reshape(WIN, HQ * HD))
        log_blocks.append(jnp.log(exp_total))
    return (jnp.concatenate(out_blocks, axis=0), jnp.concatenate(log_blocks, axis=1))

def attend_backward(query_bf, key_bf, value_bf, attn_bf, dattn_bf, log_total, segment_pad, position_pad, live_pad):
    row_count = query_bf.shape[0]
    score_scale = HD ** (-0.5)
    key_padded = front_pad(key_bf, WIN)
    value_padded = front_pad(value_bf, WIN)
    attn_heads = attn_bf.reshape(row_count, HQ, HD)
    dattn_heads = dattn_bf.reshape(row_count, HQ, HD)
    delta_rows = lax.optimization_barrier(jnp.sum(dattn_heads.astype(jnp.float32) * attn_heads.astype(jnp.float32), axis=-1))
    key_grad = jnp.zeros((row_count + WIN, HD), jnp.float32)
    value_grad = jnp.zeros((row_count + WIN, HD), jnp.float32)
    query_parts = []
    for block_index in range(row_count // WIN):
        start_row = block_index * WIN
        allowed = window_mask(block_index, WIN, segment_pad, position_pad, live_pad)
        query_block = query_bf[start_row:start_row + WIN]
        key_block = key_padded[start_row:start_row + 2 * WIN]
        value_block = value_padded[start_row:start_row + 2 * WIN]
        dout_block = dattn_heads[start_row:start_row + WIN]
        scores = contract('qhd,kd->hqk', query_block, key_block) * score_scale
        probs = jnp.where(allowed[None], jnp.exp(scores - log_total[:, start_row:start_row + WIN, None]), 0.0)
        probs_bf = probs.astype(jnp.bfloat16)
        value_grad = value_grad.at[start_row:start_row + 2 * WIN].add(contract('hqk,qhd->kd', probs_bf, dout_block))
        dprobs = contract('qhd,kd->hqk', dout_block, value_block)
        dscores = probs * (dprobs - delta_rows[start_row:start_row + WIN].T[:, :, None]) * score_scale
        dscores_bf = dscores.astype(jnp.bfloat16)
        query_parts.append(contract('hqk,kd->qhd', dscores_bf, key_block))
        key_grad = key_grad.at[start_row:start_row + 2 * WIN].add(contract('hqk,qhd->kd', dscores_bf, query_block))
    return (jnp.concatenate(query_parts, axis=0), key_grad[WIN:], value_grad[WIN:])

def device_pass(weights, norm_values, device_item):
    qkv_w, out_w, gate_up_w, down_w = weights
    inputs, cotangent, segments, positions, tile_total = device_item
    row_count = inputs.shape[0]
    live_rows = jnp.arange(row_count, dtype=jnp.int32) // TILE < tile_total
    scale_in = norm_values[0:D]
    scale_post = norm_values[D:2 * D]
    scale_ffn = norm_values[2 * D:3 * D]
    scale_out = norm_values[3 * D:4 * D]
    scale_query = norm_values[4 * D:4 * D + HD]
    scale_key = norm_values[4 * D + HD:4 * D + 2 * HD]
    resid_in = inputs.astype(jnp.float32)
    normed = rms_scale(resid_in, scale_in).astype(jnp.bfloat16)
    qkv_proj = jnp.dot(normed, qkv_w, preferred_element_type=jnp.float32)
    query_raw = qkv_proj[:, :HQ * HD].reshape(row_count, HQ, HD)
    key_raw = qkv_proj[:, HQ * HD:(HQ + 1) * HD].reshape(row_count, 1, HD)
    value_bf = qkv_proj[:, (HQ + 1) * HD:].astype(jnp.bfloat16)
    cosine, sine_table = rope_tables(positions, HD)

    def prepare(query_in, key_in, q_in, k_in):
        return qk_prepare(query_in, key_in, q_in, k_in, cosine, sine_table)
    query_rot, key_rot = prepare(query_raw, key_raw, scale_query, scale_key)
    query_bf = query_rot.astype(jnp.bfloat16)
    key_bf = key_rot[:, 0, :].astype(jnp.bfloat16)
    segment_pad = front_pad(segments, WIN)
    position_pad = front_pad(positions, WIN)
    live_pad = front_pad(live_rows, WIN)
    attn_out, log_total = attend_forward(query_bf, key_bf, value_bf, segment_pad, position_pad, live_pad)
    attn_bf = attn_out.astype(jnp.bfloat16)
    attn_proj = jnp.dot(attn_bf, out_w, preferred_element_type=jnp.float32)
    mid_resid = resid_in + rms_scale(attn_proj, scale_post)
    ffn_in = rms_scale(mid_resid, scale_ffn).astype(jnp.bfloat16)
    gate_up = jnp.dot(ffn_in, gate_up_w, preferred_element_type=jnp.float32)
    gate_act = gate_up[:, :FF]
    up_act = gate_up[:, FF:]
    hidden = gated_unit(gate_act, up_act).astype(jnp.bfloat16)
    down_act = jnp.dot(hidden, down_w, preferred_element_type=jnp.float32)
    output = mid_resid + rms_scale(down_act, scale_out)
    grad_out = cotangent.astype(jnp.float32) * live_rows[:, None].astype(jnp.float32)
    d_down, out_scale_grad = jax.vjp(rms_scale, down_act, scale_out)[1](grad_out)
    d_down_bf = d_down.astype(jnp.bfloat16)
    d_hidden = jnp.dot(d_down_bf, down_w.T, preferred_element_type=jnp.float32)
    down_term = jnp.dot(hidden.T, d_down_bf, preferred_element_type=jnp.float32)
    d_gate, d_up = jax.vjp(gated_unit, gate_act, up_act)[1](d_hidden)
    d_gate_up = jnp.concatenate([d_gate, d_up], axis=1).astype(jnp.bfloat16)
    d_ffn_in = jnp.dot(d_gate_up, gate_up_w.T, preferred_element_type=jnp.float32)
    gate_up_term = jnp.dot(ffn_in.T, d_gate_up, preferred_element_type=jnp.float32)
    d_mid_part, ffn_scale_grad = jax.vjp(rms_scale, mid_resid, scale_ffn)[1](d_ffn_in)
    d_mid = grad_out + d_mid_part
    d_proj, post_scale_grad = jax.vjp(rms_scale, attn_proj, scale_post)[1](d_mid)
    d_proj_bf = d_proj.astype(jnp.bfloat16)
    out_term = jnp.dot(attn_bf.T, d_proj_bf, preferred_element_type=jnp.float32)
    dattn_bf = jnp.dot(d_proj_bf, out_w.T, preferred_element_type=jnp.float32).astype(jnp.bfloat16)
    d_query, d_key, d_value = attend_backward(query_bf, key_bf, value_bf, attn_bf, dattn_bf, log_total, segment_pad, position_pad, live_pad)
    d_query_raw, d_key_raw, query_scale_grad, key_scale_grad = jax.vjp(prepare, query_raw, key_raw, scale_query, scale_key)[1]((d_query, d_key[:, None, :]))
    d_qkv = jnp.concatenate([d_query_raw.reshape(row_count, HQ * HD), d_key_raw.reshape(row_count, HD), d_value], axis=1).astype(jnp.bfloat16)
    d_normed = jnp.dot(d_qkv, qkv_w.T, preferred_element_type=jnp.float32)
    qkv_term = jnp.dot(normed.T, d_qkv, preferred_element_type=jnp.float32)
    d_input_part, in_scale_grad = jax.vjp(rms_scale, resid_in, scale_in)[1](d_normed)
    input_grad = d_mid + d_input_part
    norm_term = jnp.concatenate([in_scale_grad, post_scale_grad, ffn_scale_grad, out_scale_grad, query_scale_grad, key_scale_grad])
    return (output.astype(jnp.bfloat16), input_grad, (qkv_term, out_term, gate_up_term, down_term, norm_term))

def adam_update(weight, grad, first_moment, second_moment):
    first_new = beta_one * first_moment + (1.0 - beta_one) * grad
    second_new = beta_two * second_moment + (1.0 - beta_two) * grad * grad
    corr_one = 1.0 - beta_one ** adam_step
    corr_two = 1.0 - beta_two ** adam_step
    step_dir = first_new / corr_one / (jnp.sqrt(second_new / corr_two) + adam_eps) + weight_decay * weight
    return (weight - learn_rate * step_dir, first_new, second_new)

def reference(block_input, out_cotangent, segment_ids, positions, tile_count, qkv_weight, qkv_first, qkv_second, out_weight, out_first, out_second, gate_up_weight, gate_up_first, gate_up_second, down_weight, down_first, down_second, norm_scales, norm_first, norm_second):
    device_total = TOKENS // TOK_DEV
    weights = (qkv_weight.astype(jnp.bfloat16), out_weight.astype(jnp.bfloat16), gate_up_weight.astype(jnp.bfloat16), down_weight.astype(jnp.bfloat16))
    norm_values = lax.optimization_barrier(norm_scales.astype(jnp.bfloat16)).astype(jnp.float32)
    device_data = (block_input.reshape(device_total, TOK_DEV, D), out_cotangent.reshape(device_total, TOK_DEV, D), segment_ids.reshape(device_total, TOK_DEV), positions.reshape(device_total, TOK_DEV), tile_count)
    zero_grads = (jnp.zeros(qkv_weight.shape, jnp.float32), jnp.zeros(out_weight.shape, jnp.float32), jnp.zeros(gate_up_weight.shape, jnp.float32), jnp.zeros(down_weight.shape, jnp.float32), jnp.zeros(norm_scales.shape, jnp.float32))

    def scan_step(running, device_item):
        output, input_grad, grad_terms = device_pass(weights, norm_values, device_item)
        return (tuple((total + term for total, term in zip(running, grad_terms))), (output, input_grad))
    grad_sums, (outputs, input_grads) = lax.scan(scan_step, zero_grads, device_data)
    qkv_grad, out_grad, gate_up_grad, down_grad, norm_grad = grad_sums
    qkv_new, qkv_first_new, qkv_second_new = adam_update(qkv_weight, qkv_grad, qkv_first, qkv_second)
    out_new, out_first_new, out_second_new = adam_update(out_weight, out_grad, out_first, out_second)
    gate_up_new, gate_up_first_new, gate_up_second_new = adam_update(gate_up_weight, gate_up_grad, gate_up_first, gate_up_second)
    down_new, down_first_new, down_second_new = adam_update(down_weight, down_grad, down_first, down_second)
    norms_new, norm_first_new, norm_second_new = adam_update(norm_scales, norm_grad, norm_first, norm_second)
    return (outputs.reshape(TOKENS, D), input_grads.reshape(TOKENS, D), qkv_grad, out_grad, gate_up_grad, down_grad, norm_grad, qkv_new, out_new, gate_up_new, down_new, norms_new, qkv_first_new, out_first_new, gate_up_first_new, down_first_new, norm_first_new, qkv_second_new, out_second_new, gate_up_second_new, down_second_new, norm_second_new)
```

```python
import functools

import jax
import jax.numpy as jnp
from jax import lax
from jax.experimental import pallas as pl
from jax.experimental.pallas import tpu as pltpu
from jax.sharding import PartitionSpec as P

D = 640
HQ = 4
HD = 256
FF = 2048
WIN = 512
TILE = 128


norm_eps = 1e-06
rope_base = 10000.0
beta_one = 0.9
beta_two = 0.999
adam_eps = 1e-08
learn_rate = 0.02
weight_decay = 0.1
adam_step = 3


def rms_scale(values, scales):
    mean_square = jnp.mean(values * values, axis=-1, keepdims=True)
    return values * lax.rsqrt(mean_square + norm_eps) * (1.0 + scales)


def gelu_tanh(values):
    inner_term = 0.7978845608028654 * (values + 0.044715 * values * values * values)
    return 0.5 * values * (1.0 + jnp.tanh(inner_term))


def gated_unit(gate_act, up_act):
    return gelu_tanh(gate_act) * up_act


def rotate(values, cosine, sine_table):
    half_dim = values.shape[-1] // 2
    front_half = values[..., :half_dim]
    back_half = values[..., half_dim:]
    return jnp.concatenate(
        [
            front_half * cosine - back_half * sine_table,
            back_half * cosine + front_half * sine_table,
        ],
        axis=-1,
    )


def rope_tables(positions, head_dim):
    exponent = jnp.arange(head_dim // 2, dtype=jnp.float32) * (2.0 / head_dim)
    frequency = jnp.power(jnp.float32(rope_base), -exponent)
    angles = positions.astype(jnp.float32)[:, None] * frequency[None, :]
    return (jnp.cos(angles)[:, None, :], jnp.sin(angles)[:, None, :])


def qk_prepare(query_raw, key_raw, q_scale, k_scale, cosine, sine_table):
    return (
        rotate(rms_scale(query_raw, q_scale), cosine, sine_table),
        rotate(rms_scale(key_raw, k_scale), cosine, sine_table),
    )


def contract(form, left, right):
    return jnp.einsum(form, left, right, preferred_element_type=jnp.float32)


def window_mask(block_index, window, segment_pad, live_pad):
    start_row = block_index * window
    query_rows = start_row + jnp.arange(window, dtype=jnp.int32)
    key_rows = start_row - window + jnp.arange(2 * window, dtype=jnp.int32)
    query_seg = segment_pad[start_row + window : start_row + 2 * window]
    key_seg = segment_pad[start_row : start_row + 2 * window]
    query_live = live_pad[start_row + window : start_row + 2 * window]
    key_live = live_pad[start_row : start_row + 2 * window]
    diagonal = key_rows[None, :] == query_rows[:, None]
    earlier = (key_rows[None, :] < query_rows[:, None]) & (
        query_rows[:, None] - key_rows[None, :] < window
    )
    same_seq = (query_seg[:, None] == key_seg[None, :]) & query_live[:, None] & key_live[None, :]
    return diagonal | earlier & same_seq


def front_pad(values, window):
    return jnp.concatenate([jnp.zeros((window,) + values.shape[1:], values.dtype), values], axis=0)


def attend_forward(query_bf, key_bf, value_bf, segment_pad, live_pad):
    row_count = query_bf.shape[0]
    score_scale = HD ** (-0.5)
    key_padded = front_pad(key_bf, WIN)
    value_padded = front_pad(value_bf, WIN)
    out_blocks = []
    log_blocks = []
    for block_index in range(row_count // WIN):
        start_row = block_index * WIN
        allowed = window_mask(block_index, WIN, segment_pad, live_pad)
        query_block = query_bf[start_row : start_row + WIN]
        key_block = key_padded[start_row : start_row + 2 * WIN]
        value_block = value_padded[start_row : start_row + 2 * WIN]
        scores = contract("qhd,kd->hqk", query_block, key_block) * score_scale
        exp_scores = jnp.where(allowed[None], jnp.exp(scores), 0.0)
        exp_total = jnp.sum(exp_scores, axis=-1)
        probs_bf = (exp_scores / exp_total[..., None]).astype(jnp.bfloat16)
        out_blocks.append(contract("hqk,kd->qhd", probs_bf, value_block).reshape(WIN, HQ * HD))
        log_blocks.append(jnp.log(exp_total))
    return (jnp.concatenate(out_blocks, axis=0), jnp.concatenate(log_blocks, axis=1))


def attend_backward(
    query_bf, key_bf, value_bf, attn_bf, dattn_bf, log_total, segment_pad, live_pad
):
    row_count = query_bf.shape[0]
    score_scale = HD ** (-0.5)
    key_padded = front_pad(key_bf, WIN)
    value_padded = front_pad(value_bf, WIN)
    attn_heads = attn_bf.reshape(row_count, HQ, HD)
    dattn_heads = dattn_bf.reshape(row_count, HQ, HD)
    delta_rows = jnp.sum(dattn_heads.astype(jnp.float32) * attn_heads.astype(jnp.float32), axis=-1)
    key_grad = jnp.zeros((row_count + WIN, HD), jnp.float32)
    value_grad = jnp.zeros((row_count + WIN, HD), jnp.float32)
    query_parts = []
    for block_index in range(row_count // WIN):
        start_row = block_index * WIN
        allowed = window_mask(block_index, WIN, segment_pad, live_pad)
        query_block = query_bf[start_row : start_row + WIN]
        key_block = key_padded[start_row : start_row + 2 * WIN]
        value_block = value_padded[start_row : start_row + 2 * WIN]
        dout_block = dattn_heads[start_row : start_row + WIN]
        scores = contract("qhd,kd->hqk", query_block, key_block) * score_scale
        probs = jnp.where(
            allowed[None], jnp.exp(scores - log_total[:, start_row : start_row + WIN, None]), 0.0
        )
        probs_bf = probs.astype(jnp.bfloat16)
        value_grad = value_grad.at[start_row : start_row + 2 * WIN].add(
            contract("hqk,qhd->kd", probs_bf, dout_block)
        )
        dprobs = contract("qhd,kd->hqk", dout_block, value_block)
        dscores = (
            probs * (dprobs - delta_rows[start_row : start_row + WIN].T[:, :, None]) * score_scale
        )
        dscores_bf = dscores.astype(jnp.bfloat16)
        query_parts.append(contract("hqk,kd->qhd", dscores_bf, key_block))
        key_grad = key_grad.at[start_row : start_row + 2 * WIN].add(
            contract("hqk,qhd->kd", dscores_bf, query_block)
        )
    return (jnp.concatenate(query_parts, axis=0), key_grad[WIN:], value_grad[WIN:])


def forward_pass(attn_full, ffn_full, block_input, segment_ids, positions, live_rows):
    qkv_w, out_w, norm_bf = attn_full
    gate_up_w, down_w = ffn_full
    norm_values = norm_bf.astype(jnp.float32)
    row_count = block_input.shape[0]
    resid_in = block_input.astype(jnp.float32)
    normed = rms_scale(resid_in, norm_values[0:D]).astype(jnp.bfloat16)
    qkv_proj = jnp.dot(normed, qkv_w, preferred_element_type=jnp.float32)
    query_raw = qkv_proj[:, : HQ * HD].reshape(row_count, HQ, HD)
    key_raw = qkv_proj[:, HQ * HD : (HQ + 1) * HD].reshape(row_count, 1, HD)
    value_bf = qkv_proj[:, (HQ + 1) * HD :].astype(jnp.bfloat16)
    cosine, sine_table = rope_tables(positions, HD)
    query_rot, key_rot = qk_prepare(
        query_raw,
        key_raw,
        norm_values[4 * D : 4 * D + HD],
        norm_values[4 * D + HD : 4 * D + 2 * HD],
        cosine,
        sine_table,
    )
    query_bf = query_rot.astype(jnp.bfloat16)
    key_bf = key_rot[:, 0, :].astype(jnp.bfloat16)
    segment_pad = front_pad(segment_ids, WIN)
    position_pad = front_pad(positions, WIN)
    live_pad = front_pad(live_rows, WIN)
    attn_out, log_total = attend_forward(query_bf, key_bf, value_bf, segment_pad, live_pad)
    attn_bf = attn_out.astype(jnp.bfloat16)
    attn_proj = jnp.dot(attn_bf, out_w, preferred_element_type=jnp.float32)
    mid_resid = resid_in + rms_scale(attn_proj, norm_values[D : 2 * D])
    ffn_in = rms_scale(mid_resid, norm_values[2 * D : 3 * D]).astype(jnp.bfloat16)
    gate_up = jnp.dot(ffn_in, gate_up_w, preferred_element_type=jnp.float32)
    gate_act = gate_up[:, :FF]
    up_act = gate_up[:, FF:]
    hidden = gated_unit(gate_act, up_act).astype(jnp.bfloat16)
    down_act = jnp.dot(hidden, down_w, preferred_element_type=jnp.float32)
    block_output = (mid_resid + rms_scale(down_act, norm_values[3 * D : 4 * D])).astype(
        jnp.bfloat16
    )
    attn_saved = (
        resid_in,
        normed,
        query_raw,
        key_raw,
        query_bf,
        key_bf,
        value_bf,
        cosine,
        sine_table,
        segment_pad,
        position_pad,
        live_pad,
        attn_bf,
        log_total,
        attn_proj,
    )
    ffn_saved = (mid_resid, ffn_in, gate_act, up_act, hidden, down_act)
    return (block_output, attn_saved, ffn_saved)


def ffn_backward(ffn_back, norm_values, ffn_saved, grad_out):
    gate_up_w, down_w = ffn_back
    mid_resid, ffn_in, gate_act, up_act, hidden, down_act = ffn_saved
    d_down, out_scale_grad = jax.vjp(rms_scale, down_act, norm_values[3 * D : 4 * D])[1](grad_out)
    d_down_bf = d_down.astype(jnp.bfloat16)
    d_hidden = jnp.dot(d_down_bf, down_w.T, preferred_element_type=jnp.float32)
    down_term = jnp.dot(hidden.T, d_down_bf, preferred_element_type=jnp.float32)
    d_gate, d_up = jax.vjp(gated_unit, gate_act, up_act)[1](d_hidden)
    d_gate_up = jnp.concatenate([d_gate, d_up], axis=1).astype(jnp.bfloat16)
    d_ffn_in = jnp.dot(d_gate_up, gate_up_w.T, preferred_element_type=jnp.float32)
    gate_up_term = jnp.dot(ffn_in.T, d_gate_up, preferred_element_type=jnp.float32)
    d_mid_part, ffn_scale_grad = jax.vjp(rms_scale, mid_resid, norm_values[2 * D : 3 * D])[1](
        d_ffn_in
    )
    return (grad_out + d_mid_part, gate_up_term, down_term, ffn_scale_grad, out_scale_grad)


def attn_backward(attn_back, attn_saved, d_mid):
    qkv_w, out_w, norm_bf = attn_back
    norm_values = norm_bf.astype(jnp.float32)
    (
        resid_in,
        normed,
        query_raw,
        key_raw,
        query_bf,
        key_bf,
        value_bf,
        cosine,
        sine_table,
        segment_pad,
        position_pad,
        live_pad,
        attn_bf,
        log_total,
        attn_proj,
    ) = attn_saved
    row_count = resid_in.shape[0]
    d_proj, post_scale_grad = jax.vjp(rms_scale, attn_proj, norm_values[D : 2 * D])[1](d_mid)
    d_proj_bf = d_proj.astype(jnp.bfloat16)
    out_term = jnp.dot(attn_bf.T, d_proj_bf, preferred_element_type=jnp.float32)
    dattn_bf = jnp.dot(d_proj_bf, out_w.T, preferred_element_type=jnp.float32).astype(jnp.bfloat16)
    d_query, d_key, d_value = attend_backward(
        query_bf, key_bf, value_bf, attn_bf, dattn_bf, log_total, segment_pad, live_pad
    )

    def prepare(query_in, key_in, q_in, k_in):
        return qk_prepare(query_in, key_in, q_in, k_in, cosine, sine_table)

    d_query_raw, d_key_raw, query_scale_grad, key_scale_grad = jax.vjp(
        prepare,
        query_raw,
        key_raw,
        norm_values[4 * D : 4 * D + HD],
        norm_values[4 * D + HD : 4 * D + 2 * HD],
    )[1]((d_query, d_key[:, None, :]))
    d_qkv = jnp.concatenate(
        [d_query_raw.reshape(row_count, HQ * HD), d_key_raw.reshape(row_count, HD), d_value], axis=1
    ).astype(jnp.bfloat16)
    d_normed = jnp.dot(d_qkv, qkv_w.T, preferred_element_type=jnp.float32)
    qkv_term = jnp.dot(normed.T, d_qkv, preferred_element_type=jnp.float32)
    d_input_part, in_scale_grad = jax.vjp(rms_scale, resid_in, norm_values[0:D])[1](d_normed)
    return (
        d_mid + d_input_part,
        qkv_term,
        out_term,
        in_scale_grad,
        post_scale_grad,
        query_scale_grad,
        key_scale_grad,
    )


def adam_update(weight, grad, first_moment, second_moment):
    first_new = beta_one * first_moment + (1.0 - beta_one) * grad
    second_new = beta_two * second_moment + (1.0 - beta_two) * grad * grad
    corr_one = 1.0 - beta_one**adam_step
    corr_two = 1.0 - beta_two**adam_step
    step_dir = (
        first_new / corr_one / (jnp.sqrt(second_new / corr_two) + adam_eps) + weight_decay * weight
    )
    return (weight - learn_rate * step_dir, first_new, second_new)


LOGICAL = pl.DeviceIdType.LOGICAL
ALL = slice(None)
SLOTS = 10


def grid_dims(count):
    return (count // 8, 2, 2, 2)


def my_place(dims):
    index = lax.axis_index("dp")
    core = lax.rem(index, dims[3])
    index = lax.div(index, dims[3])
    x = lax.rem(index, dims[2])
    index = lax.div(index, dims[2])
    return (lax.div(index, dims[1]), lax.rem(index, dims[1]), x, core)


def device_at(dims, z, y, x, core):
    return ((z * dims[1] + y) * dims[2] + x) * dims[3] + core


def enter(dims, place):
    z, y, x, core = place
    barrier = pltpu.get_barrier_semaphore()
    peers = [device_at(dims, lax.rem(z + k, dims[0]), y, x, core) for k in range(1, dims[0])]
    peers.append(device_at(dims, z, 1 - y, x, core))
    peers.append(device_at(dims, z, y, 1 - x, core))
    peers.append(device_at(dims, z, y, x, 1 - core))
    for peer in peers:
        pl.semaphore_signal(barrier, inc=1, device_id=peer, device_id_type=LOGICAL)
    pl.semaphore_wait(barrier, len(peers))


class Link:
    def __init__(self, dims, place, send_sems, recv_sems, base):
        self.dims, self.place = dims, place
        self.send_sems, self.recv_sems, self.base = send_sems, recv_sems, base
        self.pending = []

    def copy(self, src, dst, target, slot):
        return pltpu.make_async_remote_copy(
            src_ref=src,
            dst_ref=dst,
            send_sem=self.send_sems.at[self.base + slot],
            recv_sem=self.recv_sems.at[self.base + slot],
            device_id=target,
            device_id_type=LOGICAL,
        )

    def send(self, src, dst, target, slot):
        copy = self.copy(src, dst, target, slot)
        copy.start()
        self.pending.append(copy)

    def finish(self):
        for copy in self.pending:
            copy.wait_send()
        self.pending = []

    def z_peer(self, k):
        z, y, x, core = self.place
        return device_at(self.dims, lax.rem(z + k, self.dims[0]), y, x, core)

    def y_peer(self):
        z, y, x, core = self.place
        return device_at(self.dims, z, 1 - y, x, core)

    def x_peer(self):
        z, y, x, core = self.place
        return device_at(self.dims, z, y, 1 - x, core)

    def core_peer(self):
        z, y, x, core = self.place
        return device_at(self.dims, z, y, x, 1 - core)


class Gather(Link):
    def __init__(self, dims, place, view, swap, send_sems, recv_sems, base):
        super().__init__(dims, place, send_sems, recv_sems, base)
        self.view, self.swap = view, swap

    def plan(self, stage):
        z, y, x, core = self.place
        count = self.dims[0]
        view = self.view
        if stage == 0:
            return [
                (view(z, y, x, core), self.z_peer(k), k - 1, view(lax.rem(z + count - k, count), y, x, core))
                for k in range(1, count)
            ]
        slot = count + stage
        near, far = (self.y_peer(), self.x_peer()) if self.swap else (self.x_peer(), self.y_peer())
        if stage == 1:
            got = view(ALL, 1 - y, x, core) if self.swap else view(ALL, y, 1 - x, core)
            return [(view(ALL, y, x, core), near, slot, got)]
        if stage == 2:
            mine = view(ALL, ALL, x, core) if self.swap else view(ALL, y, ALL, core)
            got = view(ALL, ALL, 1 - x, core) if self.swap else view(ALL, 1 - y, ALL, core)
            return [(mine, far, slot, got)]
        if stage == 3:
            mine = view(ALL, ALL, x, core) if self.swap else view(ALL, y, ALL, core)
            got = view(ALL, ALL, x, 1 - core) if self.swap else view(ALL, y, ALL, 1 - core)
        else:
            mine = view(ALL, ALL, 1 - x, core) if self.swap else view(ALL, 1 - y, ALL, core)
            got = view(ALL, ALL, 1 - x, 1 - core) if self.swap else view(ALL, 1 - y, ALL, 1 - core)
        return [(mine, self.core_peer(), slot, got)]

    def start(self, stage):
        for src, target, slot, _ in self.plan(stage):
            self.send(src, src, target, slot)

    def wait(self, stage):
        for _, target, slot, got in self.plan(stage):
            self.copy(got, got, target, slot).wait_recv()


class Scatter(Link):
    def __init__(self, dims, place, given, held, near, far, last, swap, send_sems, recv_sems, base):
        super().__init__(dims, place, send_sems, recv_sems, base)
        self.given, self.held, self.near, self.far, self.last, self.swap = given, held, near, far, last, swap

    def start(self, stage):
        z, y, x, core = self.place
        count = self.dims[0]
        held = self.held
        if stage == 0:
            self.send(self.given(1 - core), held, self.core_peer(), 0)
        elif stage == 1:
            if self.swap:
                self.send(held.at[:, :, 1 - x], self.near, self.x_peer(), 1)
            else:
                self.send(held.at[:, 1 - y], self.near, self.y_peer(), 1)
        elif stage == 2:
            if self.swap:
                self.send(held.at[:, 1 - y, x], self.far, self.y_peer(), 2)
            else:
                self.send(held.at[:, y, 1 - x], self.far, self.x_peer(), 2)
        else:
            for k in range(1, count):
                self.send(held.at[lax.rem(z + k, count), y, x], self.last.at[k - 1], self.z_peer(k), 2 + k)

    def wait(self, stage):
        z, y, x, core = self.place
        count = self.dims[0]
        held = self.held
        if stage == 0:
            self.copy(self.given(1 - core), held, self.core_peer(), 0).wait_recv()
            mine = self.given(core)

            def add(row, carry):
                held[row] = held[row] + mine[row]
                return carry

            lax.fori_loop(0, count, add, 0)
        elif stage == 1:
            self.copy(self.near, self.near, self.core_peer(), 1).wait_recv()

            def add(row, carry):
                if self.swap:
                    held[row, :, x] = held[row, :, x] + self.near[row]
                else:
                    held[row, y] = held[row, y] + self.near[row]
                return carry

            lax.fori_loop(0, count, add, 0)
        elif stage == 2:
            self.copy(self.far, self.far, self.core_peer(), 2).wait_recv()

            def add(row, carry):
                held[row, y, x] = held[row, y, x] + self.far[row]
                return carry

            lax.fori_loop(0, count, add, 0)
        else:
            total = held[z, y, x].astype(jnp.float32)
            for k in range(1, count):
                self.copy(self.last.at[k - 1], self.last.at[k - 1], self.core_peer(), 2 + k).wait_recv()
                total = total + self.last[k - 1].astype(jnp.float32)
            return total


def gather_kernel(dims, qkv_ref, out_ref, gate_up_ref, down_ref, norm_ref, qkv_all, out_all, gate_up_all, down_all,
                  norm_all, qkv_got, gate_up_got, pair, send_sems, recv_sems):
    place = my_place(dims)
    z, y, x, core = place
    enter(dims, place)
    link = Link(dims, place, send_sems, recv_sems, 0)
    for slot, (ref, got) in enumerate(((qkv_ref, qkv_got), (gate_up_ref, gate_up_got))):
        half = got.shape[1]
        other = pl.multiple_of((1 - core) * half, 128)
        link.send(ref.at[:, pl.ds(other, half)], got, link.core_peer(), slot)
    norm_all[z, y, x, core] = jnp.zeros(norm_all.shape[4:], jnp.float32)
    norm_all[z, y, x, core, 0:1, 0 : norm_ref.shape[1]] = norm_ref[...].astype(jnp.bfloat16).astype(jnp.float32)
    out_all[z, y, x, core] = out_ref[...].astype(jnp.bfloat16).reshape(out_all.shape[4:])
    down_all[z, y, x, core] = down_ref[...].astype(jnp.bfloat16).reshape(down_all.shape[4:])
    for slot, (ref, got, whole) in enumerate(((qkv_ref, qkv_got, qkv_all), (gate_up_ref, gate_up_got, gate_up_all))):
        rows, half = got.shape
        width = half // 2
        link.copy(got, got, link.core_peer(), slot).wait_recv()
        mine = ref[:, pl.ds(pl.multiple_of(core * half, 128), half)]
        other = got[...]
        first = core == 0
        pair[0:rows, 0:half] = jnp.where(first, mine, other)
        pair[rows : 2 * rows, 0:half] = jnp.where(first, other, mine)
        for part in range(2):
            whole[core, part, z, y, x] = pair[:, part * width : (part + 1) * width].astype(jnp.bfloat16)
    step = dims[0] + 5
    items = []
    base = 2
    for colours in (
        (lambda z, y, x, core: norm_all.at[z, y, x, core],),
        tuple((lambda z, y, x, core, h=h: qkv_all.at[core, h, z, y, x]) for h in range(2)),
        tuple((lambda z, y, x, core, h=h: out_all.at[z, y, x, core, h]) for h in range(2)),
        tuple((lambda z, y, x, core, h=h: gate_up_all.at[core, h, z, y, x]) for h in range(2)),
        tuple((lambda z, y, x, core, h=h: down_all.at[z, y, x, core, h]) for h in range(2)),
    ):
        item = []
        for swap, view in enumerate(colours):
            item.append(Gather(dims, place, view, swap == 1, send_sems, recv_sems, base))
            base += step
        items.append(item)
    items = [items[0] + items[1]] + items[2:]
    for item in items:
        for part in item:
            part.start(0)
    count = len(items)
    for turn in range(count + 2):
        if turn < count:
            for part in items[turn]:
                part.wait(0)
                part.start(1)
        if 0 <= turn - 1 < count:
            for part in items[turn - 1]:
                part.wait(1)
                part.start(2)
                part.start(3)
        if 0 <= turn - 2 < count:
            for part in items[turn - 2]:
                part.wait(2)
                part.start(4)
    link.finish()
    for item in items:
        for part in item:
            part.wait(3)
            part.wait(4)
            part.finish()


def gather_weights(dims, qkv_weight, out_weight, gate_up_weight, down_weight, norm_scales):
    grid = dims[:3]
    rows, width = qkv_weight.shape
    wide = gate_up_weight.shape[1]
    narrow = out_weight.shape[1]
    shapes = [
        (2, 2) + grid + (2 * rows, width // 4),
        grid + (2, 2, out_weight.shape[0] // 2, narrow),
        (2, 2) + grid + (2 * rows, wide // 4),
        grid + (2, 2, down_weight.shape[0] // 2, narrow),
    ]
    sems = 2 + 9 * (dims[0] + 5)
    outs = pl.pallas_call(
        functools.partial(gather_kernel, dims),
        out_shape=[jax.ShapeDtypeStruct(shape, jnp.bfloat16) for shape in shapes]
        + [jax.ShapeDtypeStruct(grid + (2, 8, 128), jnp.float32)],
        in_specs=[pl.BlockSpec(memory_space=pltpu.VMEM)] * 5,
        out_specs=[pl.BlockSpec(memory_space=pltpu.VMEM)] * 5,
        scratch_shapes=[
            pltpu.VMEM((rows, width // 2), jnp.float32),
            pltpu.VMEM((rows, wide // 2), jnp.float32),
            pltpu.VMEM((2 * rows, wide // 2), jnp.float32),
            pltpu.SemaphoreType.DMA((sems,)),
            pltpu.SemaphoreType.DMA((sems,)),
        ],
        compiler_params=pltpu.CompilerParams(collective_id=0, has_side_effects=True, vmem_limit_bytes=60 << 20),
        name="gather_weights",
    )(qkv_weight, out_weight, gate_up_weight, down_weight, norm_scales[None, :])
    qkv_all, out_all, gate_up_all, down_all, norm_all = outs
    whole = rows * grid[0] * 8
    return (
        qkv_all.reshape(4, whole, width // 4).transpose(1, 0, 2).reshape(whole, width),
        out_all.reshape(-1, narrow),
        gate_up_all.reshape(4, whole, wide // 4).transpose(1, 0, 2).reshape(whole, wide),
        down_all.reshape(-1, narrow),
        norm_all[..., 0, : norm_scales.shape[0]].reshape(-1),
    )


def scatter_kernel(dims, qkv_ref, out_ref, gate_up_ref, down_ref, norm_ref, qkv_sum, out_sum, gate_up_sum, down_sum,
                   norm_sum, *scratch):
    place = my_place(dims)
    core = place[3]
    enter(dims, place)
    buffers = scratch[:36]
    swaps, halves, sums, send_sems, recv_sems = scratch[36:]
    step = dims[0] + 5
    items = []
    base = 4
    for index, colours in enumerate((
        tuple((lambda core, h=h: down_ref.at[:, :, :, core, h]) for h in range(2)),
        tuple((lambda core, h=h: gate_up_ref.at[core, h]) for h in range(2)),
        tuple((lambda core, h=h: out_ref.at[:, :, :, core, h]) for h in range(2)),
        (lambda core: norm_ref.at[:, :, :, core],),
        tuple((lambda core, h=h: qkv_ref.at[core, h]) for h in range(2)),
    )):
        item = []
        for swap, given in enumerate(colours):
            held, near, far, last = buffers[4 * len(sum(items, [])) + 4 * swap :][:4]
            item.append(Scatter(dims, place, given, held, near, far, last, swap == 1, send_sems, recv_sems, base))
            base += step
        items.append(item)
    for item in items:
        for part in item:
            part.start(0)
    count = len(items)
    results = {}
    for turn in range(count + 3):
        for stage in range(3):
            if 0 <= turn - stage < count:
                for part in items[turn - stage]:
                    part.wait(stage)
                    part.start(stage + 1)
        if 0 <= turn - 3 < count:
            which = turn - 3
            link = Link(dims, place, send_sems, recv_sems, 0)
            if which in (0, 2):
                target = (down_sum, None, out_sum)[which]
                half = target.shape[0] // 2
                for h, part in enumerate(items[which]):
                    target[h * half : (h + 1) * half, :] = part.wait(3)
            elif which == 3:
                norm_sum[...] = items[3][0].wait(3)
            else:
                target = gate_up_sum if which == 1 else qkv_sum
                rows, width = target.shape[0], target.shape[1] // 4
                first = 0 if which == 1 else 2
                for h, part in enumerate(items[which]):
                    sums[:, 0:width] = part.wait(3)
                    low, high = sums[0:rows, 0:width], sums[rows : 2 * rows, 0:width]
                    target[:, pl.ds(pl.multiple_of((2 * core + h) * width, 128), width)] = jnp.where(core == 0, low, high)
                    swaps[first + h, :, 0:width] = jnp.where(core == 0, high, low)
                    link.send(swaps.at[first + h, :, pl.ds(0, width)], halves.at[first + h, :, pl.ds(0, width)], link.core_peer(), first + h)
                results[which] = (link, target, rows, width, first)
    for link, target, rows, width, first in results.values():
        for h in range(2):
            got = halves.at[first + h, :, pl.ds(0, width)]
            link.copy(got, got, link.core_peer(), first + h).wait_recv()
            target[:, pl.ds(pl.multiple_of((2 * (1 - core) + h) * width, 128), width)] = halves[first + h, :, 0:width]
        link.finish()
    for item in items:
        for part in item:
            part.finish()


def scatter_gradients(dims, qkv_grad, out_grad, gate_up_grad, down_grad, norm_grad):
    grid = dims[:3]
    count = grid[0] * 8
    rows = qkv_grad.shape[0] // count
    width, wide, narrow = qkv_grad.shape[1], gate_up_grad.shape[1], out_grad.shape[1]
    blocks = [
        (down_grad.shape[0] // count // 2, narrow),
        (2 * rows, wide // 4),
        (out_grad.shape[0] // count // 2, narrow),
        (8, 128),
        (2 * rows, width // 4),
    ]
    small = jnp.bfloat16

    def columns(grad):
        return grad.astype(small).reshape(grad.shape[0], 4, -1).transpose(1, 0, 2).reshape((2, 2) + grid + (2 * rows, -1))

    norm_rows = norm_grad.reshape(grid + (2, 1, -1))
    norm_rows = jnp.pad(norm_rows, ((0, 0),) * 4 + ((0, 7), (0, 128 - norm_rows.shape[-1])))
    scratch = []
    for index, block in enumerate(blocks):
        kind = jnp.float32 if index == 3 else small
        for swap in range(1 if index == 3 else 2):
            scratch.append(pltpu.VMEM(grid + block, kind))
            scratch.append(pltpu.VMEM(((grid[0], grid[1]) if swap else (grid[0], grid[2])) + block, kind))
            scratch.append(pltpu.VMEM((grid[0],) + block, kind))
            scratch.append(pltpu.VMEM((grid[0] - 1,) + block, kind))
    sems = 4 + 9 * (dims[0] + 5)
    scratch += [
        pltpu.VMEM((4, rows, wide // 4), jnp.float32),
        pltpu.VMEM((4, rows, wide // 4), jnp.float32),
        pltpu.VMEM((2 * rows, wide // 4), jnp.float32),
        pltpu.SemaphoreType.DMA((sems,)),
        pltpu.SemaphoreType.DMA((sems,)),
    ]
    outs = [(rows, width), (out_grad.shape[0] // count, narrow), (rows, wide), (down_grad.shape[0] // count, narrow), (8, 128)]
    sums = pl.pallas_call(
        functools.partial(scatter_kernel, dims),
        out_shape=[jax.ShapeDtypeStruct(shape, jnp.float32) for shape in outs],
        in_specs=[pl.BlockSpec(memory_space=pltpu.VMEM)] * 5,
        out_specs=[pl.BlockSpec(memory_space=pltpu.VMEM)] * 5,
        scratch_shapes=scratch,
        compiler_params=pltpu.CompilerParams(collective_id=1, has_side_effects=True, vmem_limit_bytes=62 << 20),
        name="scatter_gradients",
    )(
        columns(qkv_grad),
        out_grad.astype(small).reshape(grid + (2, 2) + blocks[2]),
        columns(gate_up_grad),
        down_grad.astype(small).reshape(grid + (2, 2) + blocks[0]),
        norm_rows,
    )
    return tuple(sums[:4]) + (sums[4][0, : norm_grad.shape[0] // count],)


def own_transfers(count, width, rows):
    return count % 8 == 0 and rows * 2 % 8 == 0 and width % 512 == 0


def shards(
    count,
    block_input,
    out_cotangent,
    segment_ids,
    positions,
    tile_count,
    qkv_weight,
    qkv_first,
    qkv_second,
    out_weight,
    out_first,
    out_second,
    gate_up_weight,
    gate_up_first,
    gate_up_second,
    down_weight,
    down_first,
    down_second,
    norm_scales,
    norm_first,
    norm_second,
):
    dims = grid_dims(count)
    own = own_transfers(count, qkv_weight.shape[1], qkv_weight.shape[0])
    if own:
        qkv_full, out_full, gate_up_full, down_full, norm_full = gather_weights(
            dims, qkv_weight, out_weight, gate_up_weight, down_weight, norm_scales
        )
    else:
        qkv_full, out_full, gate_up_full, down_full, norm_full = (
            lax.all_gather(array.astype(jnp.bfloat16), "dp", axis=0, tiled=True)
            for array in (qkv_weight, out_weight, gate_up_weight, down_weight, norm_scales)
        )
    attn_full = (qkv_full, out_full, norm_full)
    ffn_full = (gate_up_full, down_full)
    row_count = block_input.shape[0]
    live_rows = jnp.arange(row_count, dtype=jnp.int32) // TILE < tile_count[0]
    block_output, attn_saved, ffn_saved = forward_pass(
        attn_full, ffn_full, block_input, segment_ids, positions, live_rows
    )
    attn_back, ffn_back = attn_full, ffn_full
    grad_out = out_cotangent.astype(jnp.float32) * live_rows[:, None].astype(jnp.float32)
    d_mid, gate_up_term, down_term, ffn_scale_grad, out_scale_grad = ffn_backward(
        ffn_back, attn_back[2].astype(jnp.float32), ffn_saved, grad_out
    )
    (
        input_grad,
        qkv_term,
        out_term,
        in_scale_grad,
        post_scale_grad,
        query_scale_grad,
        key_scale_grad,
    ) = attn_backward(attn_back, attn_saved, d_mid)
    norm_term = jnp.concatenate(
        [
            in_scale_grad,
            post_scale_grad,
            ffn_scale_grad,
            out_scale_grad,
            query_scale_grad,
            key_scale_grad,
        ]
    )
    terms = (qkv_term, out_term, gate_up_term, down_term, norm_term)
    if own:
        qkv_grad, out_grad, gate_up_grad, down_grad, norm_grad = scatter_gradients(dims, *terms)
    else:
        qkv_grad, out_grad, gate_up_grad, down_grad, norm_grad = (
            lax.psum_scatter(term, "dp", scatter_dimension=0, tiled=True) for term in terms
        )
    qkv_new, qkv_first_new, qkv_second_new = adam_update(
        qkv_weight, qkv_grad, qkv_first, qkv_second
    )
    out_new, out_first_new, out_second_new = adam_update(
        out_weight, out_grad, out_first, out_second
    )
    gate_up_new, gate_up_first_new, gate_up_second_new = adam_update(
        gate_up_weight, gate_up_grad, gate_up_first, gate_up_second
    )
    down_new, down_first_new, down_second_new = adam_update(
        down_weight, down_grad, down_first, down_second
    )
    norms_new, norm_first_new, norm_second_new = adam_update(
        norm_scales, norm_grad, norm_first, norm_second
    )
    return (
        block_output,
        input_grad,
        qkv_grad,
        out_grad,
        gate_up_grad,
        down_grad,
        norm_grad,
        qkv_new,
        out_new,
        gate_up_new,
        down_new,
        norms_new,
        qkv_first_new,
        out_first_new,
        gate_up_first_new,
        down_first_new,
        norm_first_new,
        qkv_second_new,
        out_second_new,
        gate_up_second_new,
        down_second_new,
        norm_second_new,
    )


def solution(mesh):
    in_specs = (
        P("dp", None),
        P("dp", None),
        P("dp"),
        P("dp"),
        P("dp"),
        P("dp", None),
        P("dp", None),
        P("dp", None),
        P("dp", None),
        P("dp", None),
        P("dp", None),
        P("dp", None),
        P("dp", None),
        P("dp", None),
        P("dp", None),
        P("dp", None),
        P("dp", None),
        P("dp"),
        P("dp"),
        P("dp"),
    )
    out_specs = (
        P("dp", None),
        P("dp", None),
        P("dp", None),
        P("dp", None),
        P("dp", None),
        P("dp", None),
        P("dp"),
        P("dp", None),
        P("dp", None),
        P("dp", None),
        P("dp", None),
        P("dp"),
        P("dp", None),
        P("dp", None),
        P("dp", None),
        P("dp", None),
        P("dp"),
        P("dp", None),
        P("dp", None),
        P("dp", None),
        P("dp", None),
        P("dp"),
    )
    body = functools.partial(shards, mesh.shape["dp"])
    return jax.shard_map(body, mesh=mesh, in_specs=in_specs, out_specs=out_specs, check_vma=False)
```

```python
import functools

import jax
import jax.numpy as jnp
from jax import lax
from jax.experimental import pallas as pl
from jax.experimental.pallas import tpu as pltpu
from jax.sharding import PartitionSpec as P

D = 640
HQ = 4
HD = 256
FF = 2048
WIN = 512
TILE = 128


norm_eps = 1e-06
rope_base = 10000.0
beta_one = 0.9
beta_two = 0.999
adam_eps = 1e-08
learn_rate = 0.02
weight_decay = 0.1
adam_step = 3


def rms_scale(values, scales):
    mean_square = jnp.mean(values * values, axis=-1, keepdims=True)
    return values * lax.rsqrt(mean_square + norm_eps) * (1.0 + scales)


def gelu_tanh(values):
    inner_term = 0.7978845608028654 * (values + 0.044715 * values * values * values)
    return 0.5 * values * (1.0 + jnp.tanh(inner_term))


def gated_unit(gate_act, up_act):
    return gelu_tanh(gate_act) * up_act


def rotate(values, cosine, sine_table):
    half_dim = values.shape[-1] // 2
    front_half = values[..., :half_dim]
    back_half = values[..., half_dim:]
    return jnp.concatenate(
        [
            front_half * cosine - back_half * sine_table,
            back_half * cosine + front_half * sine_table,
        ],
        axis=-1,
    )


def rope_tables(positions, head_dim):
    exponent = jnp.arange(head_dim // 2, dtype=jnp.float32) * (2.0 / head_dim)
    frequency = jnp.power(jnp.float32(rope_base), -exponent)
    angles = positions.astype(jnp.float32)[:, None] * frequency[None, :]
    return (jnp.cos(angles)[:, None, :], jnp.sin(angles)[:, None, :])


def qk_prepare(query_raw, key_raw, q_scale, k_scale, cosine, sine_table):
    return (
        rotate(rms_scale(query_raw, q_scale), cosine, sine_table),
        rotate(rms_scale(key_raw, k_scale), cosine, sine_table),
    )


def contract(form, left, right):
    return jnp.einsum(form, left, right, preferred_element_type=jnp.float32)


def window_mask(block_index, window, segment_pad, live_pad):
    start_row = block_index * window
    query_rows = start_row + jnp.arange(window, dtype=jnp.int32)
    key_rows = start_row - window + jnp.arange(2 * window, dtype=jnp.int32)
    query_seg = segment_pad[start_row + window : start_row + 2 * window]
    key_seg = segment_pad[start_row : start_row + 2 * window]
    query_live = live_pad[start_row + window : start_row + 2 * window]
    key_live = live_pad[start_row : start_row + 2 * window]
    diagonal = key_rows[None, :] == query_rows[:, None]
    earlier = (key_rows[None, :] < query_rows[:, None]) & (
        query_rows[:, None] - key_rows[None, :] < window
    )
    same_seq = (query_seg[:, None] == key_seg[None, :]) & query_live[:, None] & key_live[None, :]
    return diagonal | earlier & same_seq


def front_pad(values, window):
    return jnp.concatenate([jnp.zeros((window,) + values.shape[1:], values.dtype), values], axis=0)


def attend_forward(query_bf, key_bf, value_bf, segment_pad, live_pad):
    row_count = query_bf.shape[0]
    score_scale = HD ** (-0.5)
    key_padded = front_pad(key_bf, WIN)
    value_padded = front_pad(value_bf, WIN)
    out_blocks = []
    log_blocks = []
    for block_index in range(row_count // WIN):
        start_row = block_index * WIN
        allowed = window_mask(block_index, WIN, segment_pad, live_pad)
        query_block = query_bf[start_row : start_row + WIN]
        key_block = key_padded[start_row : start_row + 2 * WIN]
        value_block = value_padded[start_row : start_row + 2 * WIN]
        scores = contract("qhd,kd->hqk", query_block, key_block) * score_scale
        exp_scores = jnp.where(allowed[None], jnp.exp(scores), 0.0)
        exp_total = jnp.sum(exp_scores, axis=-1)
        probs_bf = (exp_scores / exp_total[..., None]).astype(jnp.bfloat16)
        out_blocks.append(contract("hqk,kd->qhd", probs_bf, value_block).reshape(WIN, HQ * HD))
        log_blocks.append(jnp.log(exp_total))
    return (jnp.concatenate(out_blocks, axis=0), jnp.concatenate(log_blocks, axis=1))


def attend_backward(
    query_bf, key_bf, value_bf, attn_bf, dattn_bf, log_total, segment_pad, live_pad
):
    row_count = query_bf.shape[0]
    score_scale = HD ** (-0.5)
    key_padded = front_pad(key_bf, WIN)
    value_padded = front_pad(value_bf, WIN)
    attn_heads = attn_bf.reshape(row_count, HQ, HD)
    dattn_heads = dattn_bf.reshape(row_count, HQ, HD)
    delta_rows = jnp.sum(dattn_heads.astype(jnp.float32) * attn_heads.astype(jnp.float32), axis=-1)
    key_grad = jnp.zeros((row_count + WIN, HD), jnp.float32)
    value_grad = jnp.zeros((row_count + WIN, HD), jnp.float32)
    query_parts = []
    for block_index in range(row_count // WIN):
        start_row = block_index * WIN
        allowed = window_mask(block_index, WIN, segment_pad, live_pad)
        query_block = query_bf[start_row : start_row + WIN]
        key_block = key_padded[start_row : start_row + 2 * WIN]
        value_block = value_padded[start_row : start_row + 2 * WIN]
        dout_block = dattn_heads[start_row : start_row + WIN]
        scores = contract("qhd,kd->hqk", query_block, key_block) * score_scale
        probs = jnp.where(
            allowed[None], jnp.exp(scores - log_total[:, start_row : start_row + WIN, None]), 0.0
        )
        probs_bf = probs.astype(jnp.bfloat16)
        value_grad = value_grad.at[start_row : start_row + 2 * WIN].add(
            contract("hqk,qhd->kd", probs_bf, dout_block)
        )
        dprobs = contract("qhd,kd->hqk", dout_block, value_block)
        dscores = (
            probs * (dprobs - delta_rows[start_row : start_row + WIN].T[:, :, None]) * score_scale
        )
        dscores_bf = dscores.astype(jnp.bfloat16)
        query_parts.append(contract("hqk,kd->qhd", dscores_bf, key_block))
        key_grad = key_grad.at[start_row : start_row + 2 * WIN].add(
            contract("hqk,qhd->kd", dscores_bf, query_block)
        )
    return (jnp.concatenate(query_parts, axis=0), key_grad[WIN:], value_grad[WIN:])


def forward_pass(attn_full, ffn_full, block_input, segment_ids, positions, live_rows):
    qkv_w, out_w, norm_bf = attn_full
    gate_up_w, down_w = ffn_full
    norm_values = norm_bf.astype(jnp.float32)
    row_count = block_input.shape[0]
    resid_in = block_input.astype(jnp.float32)
    normed = rms_scale(resid_in, norm_values[0:D]).astype(jnp.bfloat16)
    qkv_proj = jnp.dot(normed, qkv_w, preferred_element_type=jnp.float32)
    query_raw = qkv_proj[:, : HQ * HD].reshape(row_count, HQ, HD)
    key_raw = qkv_proj[:, HQ * HD : (HQ + 1) * HD].reshape(row_count, 1, HD)
    value_bf = qkv_proj[:, (HQ + 1) * HD :].astype(jnp.bfloat16)
    cosine, sine_table = rope_tables(positions, HD)
    query_rot, key_rot = qk_prepare(
        query_raw,
        key_raw,
        norm_values[4 * D : 4 * D + HD],
        norm_values[4 * D + HD : 4 * D + 2 * HD],
        cosine,
        sine_table,
    )
    query_bf = query_rot.astype(jnp.bfloat16)
    key_bf = key_rot[:, 0, :].astype(jnp.bfloat16)
    segment_pad = front_pad(segment_ids, WIN)
    position_pad = front_pad(positions, WIN)
    live_pad = front_pad(live_rows, WIN)
    attn_out, log_total = attend_forward(query_bf, key_bf, value_bf, segment_pad, live_pad)
    attn_bf = attn_out.astype(jnp.bfloat16)
    attn_proj = jnp.dot(attn_bf, out_w, preferred_element_type=jnp.float32)
    mid_resid = resid_in + rms_scale(attn_proj, norm_values[D : 2 * D])
    ffn_in = rms_scale(mid_resid, norm_values[2 * D : 3 * D]).astype(jnp.bfloat16)
    gate_up = jnp.dot(ffn_in, gate_up_w, preferred_element_type=jnp.float32)
    gate_act = gate_up[:, :FF]
    up_act = gate_up[:, FF:]
    hidden = gated_unit(gate_act, up_act).astype(jnp.bfloat16)
    down_act = jnp.dot(hidden, down_w, preferred_element_type=jnp.float32)
    block_output = (mid_resid + rms_scale(down_act, norm_values[3 * D : 4 * D])).astype(
        jnp.bfloat16
    )
    attn_saved = (
        resid_in,
        normed,
        query_raw,
        key_raw,
        query_bf,
        key_bf,
        value_bf,
        cosine,
        sine_table,
        segment_pad,
        position_pad,
        live_pad,
        attn_bf,
        log_total,
        attn_proj,
    )
    ffn_saved = (mid_resid, ffn_in, gate_act, up_act, hidden, down_act)
    return (block_output, attn_saved, ffn_saved)


def ffn_backward(ffn_back, norm_values, ffn_saved, grad_out):
    gate_up_w, down_w = ffn_back
    mid_resid, ffn_in, gate_act, up_act, hidden, down_act = ffn_saved
    d_down, out_scale_grad = jax.vjp(rms_scale, down_act, norm_values[3 * D : 4 * D])[1](grad_out)
    d_down_bf = d_down.astype(jnp.bfloat16)
    d_hidden = jnp.dot(d_down_bf, down_w.T, preferred_element_type=jnp.float32)
    down_term = jnp.dot(hidden.T, d_down_bf, preferred_element_type=jnp.float32)
    d_gate, d_up = jax.vjp(gated_unit, gate_act, up_act)[1](d_hidden)
    d_gate_up = jnp.concatenate([d_gate, d_up], axis=1).astype(jnp.bfloat16)
    d_ffn_in = jnp.dot(d_gate_up, gate_up_w.T, preferred_element_type=jnp.float32)
    gate_up_term = jnp.dot(ffn_in.T, d_gate_up, preferred_element_type=jnp.float32)
    d_mid_part, ffn_scale_grad = jax.vjp(rms_scale, mid_resid, norm_values[2 * D : 3 * D])[1](
        d_ffn_in
    )
    return (grad_out + d_mid_part, gate_up_term, down_term, ffn_scale_grad, out_scale_grad)


def attn_backward(attn_back, attn_saved, d_mid):
    qkv_w, out_w, norm_bf = attn_back
    norm_values = norm_bf.astype(jnp.float32)
    (
        resid_in,
        normed,
        query_raw,
        key_raw,
        query_bf,
        key_bf,
        value_bf,
        cosine,
        sine_table,
        segment_pad,
        position_pad,
        live_pad,
        attn_bf,
        log_total,
        attn_proj,
    ) = attn_saved
    row_count = resid_in.shape[0]
    d_proj, post_scale_grad = jax.vjp(rms_scale, attn_proj, norm_values[D : 2 * D])[1](d_mid)
    d_proj_bf = d_proj.astype(jnp.bfloat16)
    out_term = jnp.dot(attn_bf.T, d_proj_bf, preferred_element_type=jnp.float32)
    dattn_bf = jnp.dot(d_proj_bf, out_w.T, preferred_element_type=jnp.float32).astype(jnp.bfloat16)
    d_query, d_key, d_value = attend_backward(
        query_bf, key_bf, value_bf, attn_bf, dattn_bf, log_total, segment_pad, live_pad
    )

    def prepare(query_in, key_in, q_in, k_in):
        return qk_prepare(query_in, key_in, q_in, k_in, cosine, sine_table)

    d_query_raw, d_key_raw, query_scale_grad, key_scale_grad = jax.vjp(
        prepare,
        query_raw,
        key_raw,
        norm_values[4 * D : 4 * D + HD],
        norm_values[4 * D + HD : 4 * D + 2 * HD],
    )[1]((d_query, d_key[:, None, :]))
    d_qkv = jnp.concatenate(
        [d_query_raw.reshape(row_count, HQ * HD), d_key_raw.reshape(row_count, HD), d_value], axis=1
    ).astype(jnp.bfloat16)
    d_normed = jnp.dot(d_qkv, qkv_w.T, preferred_element_type=jnp.float32)
    qkv_term = jnp.dot(normed.T, d_qkv, preferred_element_type=jnp.float32)
    d_input_part, in_scale_grad = jax.vjp(rms_scale, resid_in, norm_values[0:D])[1](d_normed)
    return (
        d_mid + d_input_part,
        qkv_term,
        out_term,
        in_scale_grad,
        post_scale_grad,
        query_scale_grad,
        key_scale_grad,
    )


def adam_update(weight, grad, first_moment, second_moment):
    first_new = beta_one * first_moment + (1.0 - beta_one) * grad
    second_new = beta_two * second_moment + (1.0 - beta_two) * grad * grad
    corr_one = 1.0 - beta_one**adam_step
    corr_two = 1.0 - beta_two**adam_step
    step_dir = (
        first_new / corr_one / (jnp.sqrt(second_new / corr_two) + adam_eps) + weight_decay * weight
    )
    return (weight - learn_rate * step_dir, first_new, second_new)


LOGICAL = pl.DeviceIdType.LOGICAL
ALL = slice(None)
SLOTS = 10


def grid_dims(count):
    return (count // 8, 2, 2, 2)


def my_place(dims):
    index = lax.axis_index("dp")
    core = lax.rem(index, dims[3])
    index = lax.div(index, dims[3])
    x = lax.rem(index, dims[2])
    index = lax.div(index, dims[2])
    return (lax.div(index, dims[1]), lax.rem(index, dims[1]), x, core)


def device_at(dims, z, y, x, core):
    return ((z * dims[1] + y) * dims[2] + x) * dims[3] + core


def enter(dims, place):
    z, y, x, core = place
    barrier = pltpu.get_barrier_semaphore()
    peers = [device_at(dims, lax.rem(z + k, dims[0]), y, x, core) for k in range(1, dims[0])]
    peers.append(device_at(dims, z, 1 - y, x, core))
    peers.append(device_at(dims, z, y, 1 - x, core))
    peers.append(device_at(dims, z, y, x, 1 - core))
    for peer in peers:
        pl.semaphore_signal(barrier, inc=1, device_id=peer, device_id_type=LOGICAL)
    pl.semaphore_wait(barrier, len(peers))


class Link:
    def __init__(self, dims, place, send_sems, recv_sems, base):
        self.dims, self.place = dims, place
        self.send_sems, self.recv_sems, self.base = send_sems, recv_sems, base
        self.pending = []

    def copy(self, src, dst, target, slot):
        return pltpu.make_async_remote_copy(
            src_ref=src,
            dst_ref=dst,
            send_sem=self.send_sems.at[self.base + slot],
            recv_sem=self.recv_sems.at[self.base + slot],
            device_id=target,
            device_id_type=LOGICAL,
        )

    def send(self, src, dst, target, slot):
        copy = self.copy(src, dst, target, slot)
        copy.start()
        self.pending.append(copy)

    def finish(self):
        for copy in self.pending:
            copy.wait_send()
        self.pending = []

    def z_peer(self, k):
        z, y, x, core = self.place
        return device_at(self.dims, lax.rem(z + k, self.dims[0]), y, x, core)

    def y_peer(self):
        z, y, x, core = self.place
        return device_at(self.dims, z, 1 - y, x, core)

    def x_peer(self):
        z, y, x, core = self.place
        return device_at(self.dims, z, y, 1 - x, core)

    def core_peer(self):
        z, y, x, core = self.place
        return device_at(self.dims, z, y, x, 1 - core)


class Gather(Link):
    def __init__(self, dims, place, view, swap, send_sems, recv_sems, base):
        super().__init__(dims, place, send_sems, recv_sems, base)
        self.view, self.swap = view, swap

    def plan(self, stage):
        z, y, x, core = self.place
        count = self.dims[0]
        view = self.view
        if stage == 0:
            return [
                (view(z, y, x, core), self.z_peer(k), k - 1, view(lax.rem(z + count - k, count), y, x, core))
                for k in range(1, count)
            ]
        slot = count + stage
        near, far = (self.y_peer(), self.x_peer()) if self.swap else (self.x_peer(), self.y_peer())
        if stage == 1:
            got = view(ALL, 1 - y, x, core) if self.swap else view(ALL, y, 1 - x, core)
            return [(view(ALL, y, x, core), near, slot, got)]
        if stage == 2:
            mine = view(ALL, ALL, x, core) if self.swap else view(ALL, y, ALL, core)
            got = view(ALL, ALL, 1 - x, core) if self.swap else view(ALL, 1 - y, ALL, core)
            return [(mine, far, slot, got)]
        if stage == 3:
            mine = view(ALL, ALL, x, core) if self.swap else view(ALL, y, ALL, core)
            got = view(ALL, ALL, x, 1 - core) if self.swap else view(ALL, y, ALL, 1 - core)
        else:
            mine = view(ALL, ALL, 1 - x, core) if self.swap else view(ALL, 1 - y, ALL, core)
            got = view(ALL, ALL, 1 - x, 1 - core) if self.swap else view(ALL, 1 - y, ALL, 1 - core)
        return [(mine, self.core_peer(), slot, got)]

    def start(self, stage):
        for src, target, slot, _ in self.plan(stage):
            self.send(src, src, target, slot)

    def wait(self, stage):
        for _, target, slot, got in self.plan(stage):
            self.copy(got, got, target, slot).wait_recv()


class Scatter(Link):
    def __init__(self, dims, place, given, held, near, far, last, swap, send_sems, recv_sems, base):
        super().__init__(dims, place, send_sems, recv_sems, base)
        self.given, self.held, self.near, self.far, self.last, self.swap = given, held, near, far, last, swap

    def start(self, stage):
        z, y, x, core = self.place
        count = self.dims[0]
        held = self.held
        if stage == 0:
            self.send(self.given(1 - core), held, self.core_peer(), 0)
        elif stage == 1:
            if self.swap:
                self.send(held.at[:, :, 1 - x], self.near, self.x_peer(), 1)
            else:
                self.send(held.at[:, 1 - y], self.near, self.y_peer(), 1)
        elif stage == 2:
            if self.swap:
                self.send(held.at[:, 1 - y, x], self.far, self.y_peer(), 2)
            else:
                self.send(held.at[:, y, 1 - x], self.far, self.x_peer(), 2)
        else:
            for k in range(1, count):
                self.send(held.at[lax.rem(z + k, count), y, x], self.last.at[k - 1], self.z_peer(k), 2 + k)

    def wait(self, stage):
        z, y, x, core = self.place
        count = self.dims[0]
        held = self.held
        if stage == 0:
            self.copy(self.given(1 - core), held, self.core_peer(), 0).wait_recv()
            mine = self.given(core)

            def add(row, carry):
                held[row] = held[row] + mine[row]
                return carry

            lax.fori_loop(0, count, add, 0)
        elif stage == 1:
            self.copy(self.near, self.near, self.core_peer(), 1).wait_recv()

            def add(row, carry):
                if self.swap:
                    held[row, :, x] = held[row, :, x] + self.near[row]
                else:
                    held[row, y] = held[row, y] + self.near[row]
                return carry

            lax.fori_loop(0, count, add, 0)
        elif stage == 2:
            self.copy(self.far, self.far, self.core_peer(), 2).wait_recv()

            def add(row, carry):
                held[row, y, x] = held[row, y, x] + self.far[row]
                return carry

            lax.fori_loop(0, count, add, 0)
        else:
            total = held[z, y, x].astype(jnp.float32)
            for k in range(1, count):
                self.copy(self.last.at[k - 1], self.last.at[k - 1], self.core_peer(), 2 + k).wait_recv()
                total = total + self.last[k - 1].astype(jnp.float32)
            return total


def own_transfers(count, width, rows):
    return count % 8 == 0 and rows * 2 % 8 == 0 and width % 512 == 0


BF16 = jnp.bfloat16
F32 = jnp.float32
LOG2E = 1.4426950408889634
ROWS = 256


def dot(left, right):
    return jnp.dot(left, right, preferred_element_type=F32)


def dot_nt(left, right):
    return lax.dot_general(left, right, (((1,), (1,)), ((), ())), preferred_element_type=F32)


def dot_tn(left, right):
    return lax.dot_general(left, right, (((0,), (0,)), ((), ())), preferred_element_type=F32)


def fold(values):
    return jnp.sum(values.reshape(values.shape[0] // 8, 8, values.shape[1]), axis=0)


def unit(values):
    scale = lax.rsqrt(jnp.mean(values * values, axis=-1, keepdims=True) + norm_eps)
    return values * scale, scale


def unit_back(grad, normal, scale):
    return scale * (grad - normal * jnp.mean(grad * normal, axis=-1, keepdims=True))


def turn_pairs(values, cosine, sine, sign):
    front, back = values[:, : HD // 2], values[:, HD // 2 :]
    if sign > 0:
        return jnp.concatenate([front * cosine - back * sine, back * cosine + front * sine], axis=1)
    return jnp.concatenate([front * cosine + back * sine, back * cosine - front * sine], axis=1)


def column_of(row):
    return jnp.broadcast_to(row, (128, 128)).T


def chunk_masks(per, start, width):
    def owner(count):
        column = lax.broadcasted_iota(jnp.int32, (count, width), 1) + start
        first = lax.broadcasted_iota(jnp.int32, (count, width), 0) * per
        return (column >= first) & (column < first + per)

    entry = lax.broadcasted_iota(jnp.int32, (128, width), 0)
    gap = (lax.broadcasted_iota(jnp.int32, (128, width), 1) + start - entry).astype(F32)
    place = (jnp.floor((gap + 0.5) * (1.0 / per)) * per == gap) & (entry < per)
    return owner, place


def spread_scales(norm_all, rows_ref, scale_ref, per, count):
    flat = norm_all.reshape(count, 8, 128)
    for device in range(count):
        rows_ref[device : device + 1, :] = flat[device, 0:1, :]
    table = rows_ref[...].astype(BF16)
    step = 512
    for start in range(0, count * per, step):
        owner, place = chunk_masks(per, start, step)
        spread = dot_tn(table, owner(count).astype(F32).astype(BF16))
        scale_ref[:, start : start + step] = jnp.sum(jnp.where(place, spread, 0.0), axis=0, keepdims=True)


class Relay:
    def __init__(self, items):
        self.items, self.next = items, 0

    def turn(self):
        items, now = self.items, self.next
        self.next += 1
        if now < len(items):
            for part in items[now]:
                part.wait(0)
                part.start(1)
        if 0 <= now - 1 < len(items):
            for part in items[now - 1]:
                part.wait(1)
                part.start(2)
                part.start(3)
        if 0 <= now - 2 < len(items):
            for part in items[now - 2]:
                part.wait(2)
                part.start(4)

    def until(self, which):
        while self.next < which + 3:
            self.turn()
        for part in self.items[which]:
            part.wait(3)
            part.wait(4)


QKV_CUTS = ((0, 256), (256, 128), (384, 128), (512, 256))


def forward_kernel(dims, x_hbm, cot_hbm, pos_ref, count_ref, freq_ref, qkv_ref, out_ref, gate_up_ref, down_ref, norm_ref,
                   *rest):
    outs, scratch = rest[:25], rest[25:]
    (o_q0, o_q1, o_q2, o_q3, o_wo, o_wgu, o_wd, o_scale, o_normed, o_raw, o_query, o_key, o_value, o_attn, o_cos, o_sin,
     o_ffn_in, o_mid, o_proj, o_hidden, o_gate, o_up, o_ddown, o_out, o_sgrad) = outs
    (q0, q1, q2, q3, wo, wgu, wd, scale, normed, raw, query, key, value, attn_t, cosine, sine,
     ffn_in_t, mid, proj, hidden, gate, up, ddown, out, sgrad,
     x_ref, cot_ref, attn, ffn_in, low, down, norm_all, norm_rows, qkv_got, gate_up_got, pair,
     send_sems, recv_sems, in_sems, out_sems) = scratch
    place = my_place(dims)
    z, y, x, core = place
    count = dims[0] * 8
    tokens = x_ref.shape[0]
    tiles = tokens // ROWS
    loads = [pltpu.make_async_copy(x_hbm, x_ref, in_sems.at[0]), pltpu.make_async_copy(cot_hbm, cot_ref, in_sems.at[1])]
    for load in loads:
        load.start()
    enter(dims, place)
    stores = []

    def put(index):
        store = pltpu.make_async_copy(scratch[index], outs[index], out_sems.at[index])
        store.start()
        stores.append(store)

    link = Link(dims, place, send_sems, recv_sems, 0)
    for slot, (ref, got) in enumerate(((qkv_ref, qkv_got), (gate_up_ref, gate_up_got))):
        half = got.shape[1]
        other = pl.multiple_of((1 - core) * half, 128)
        link.send(ref.at[:, pl.ds(other, half)], got, link.core_peer(), slot)
    norm_all[z, y, x, core] = jnp.zeros(norm_all.shape[4:], F32)
    norm_all[z, y, x, core, 0:1, 0 : norm_ref.shape[1]] = norm_ref[...].astype(BF16).astype(F32)

    def pair_up(ref, got, slot):
        rows, half = got.shape
        link.copy(got, got, link.core_peer(), slot).wait_recv()
        mine = ref[:, pl.ds(pl.multiple_of(core * half, 128), half)]
        other = got[...]
        first = core == 0
        pair[0:rows, 0:half] = jnp.where(first, mine, other)
        pair[rows : 2 * rows, 0:half] = jnp.where(first, other, mine)

    step = dims[0] + 5
    bases = iter(range(2, 2 + 17 * step, step))

    def item(views):
        return [Gather(dims, place, view, swap == 1, send_sems, recv_sems, next(bases)) for swap, view in enumerate(views)]

    def block(ref, *lead):
        return lambda z, y, x, core: ref.at[(*lead, core, z, y, x)]

    def rows_of(ref, part):
        return lambda z, y, x, core: ref.at[z, y, x, core, part]

    pair_up(qkv_ref, qkv_got, 0)
    for ref, (start, width) in zip((q0, q1, q2, q3), QKV_CUTS):
        ref[core, z, y, x] = pair[:, start : start + width].astype(BF16)
    norm_item = item((lambda z, y, x, core: norm_all.at[z, y, x, core],))
    items = [norm_item + item((block(q0), block(q1))), item((block(q2), block(q3)))]
    for parts in items:
        for part in parts:
            part.start(0)
    wo[z, y, x, core] = out_ref[...].astype(BF16).reshape(wo.shape[4:])
    wd[z, y, x, core] = down_ref[...].astype(BF16).reshape(wd.shape[4:])
    items.append(item((rows_of(wo, 0), rows_of(wo, 1))))
    items.append(item((rows_of(wd, 0), rows_of(wd, 1))))
    for parts in items[2:]:
        for part in parts:
            part.start(0)
    pair_up(gate_up_ref, gate_up_got, 1)
    quarters = wgu.shape[0]
    cut = wgu.shape[-1]
    for quarter in range(quarters):
        for colour in range(2):
            start = (2 * quarter + colour) * cut
            wgu[quarter, colour, core, z, y, x] = pair[:, start : start + cut].astype(BF16)
        items.append(item((block(wgu, quarter, 0), block(wgu, quarter, 1))))
        for part in items[-1]:
            part.start(0)
    relay = Relay(items)
    relay.turn()
    live_tiles = count_ref[0]
    for tile in range(tokens // 128):
        span = slice(tile * 128, (tile + 1) * 128)
        position = column_of(pos_ref[tile : tile + 1, :].astype(F32))
        angle = position * freq_ref[...]
        cosine[span] = jnp.cos(angle)
        sine[span] = jnp.sin(angle)
        row = lax.broadcasted_iota(jnp.int32, (128, 128), 0) + tile * 128
        low[span] = row - jnp.where(tile < live_tiles, jnp.minimum(position.astype(jnp.int32), WIN - 1), 0)
        if tile == 3:
            relay.turn()
    put(14)
    put(15)
    relay.turn()
    for load in loads:
        load.wait()
    for part in items[0]:
        part.wait(3)
        part.wait(4)
    spread_scales(norm_all, norm_rows, scale, norm_ref.shape[1], count)
    put(7)
    relay.until(1)
    for index in range(4):
        put(index)

    def scales(which):
        start = (0, D, 2 * D, 3 * D, 4 * D, 4 * D + HD)[which]
        return 1.0 + scale[:, start : start + (D if which < 4 else HD)]

    def weight(ref, c):
        return ref[c].reshape(-1, ref.shape[-1])

    def project(tile):
        rows = slice(tile * ROWS, (tile + 1) * ROWS)
        normal, _ = unit(x_ref[rows].astype(F32))
        inner = (normal * scales(0)).astype(BF16)
        normed[:, rows] = inner.T
        parts = []
        for c in range(2):
            parts.append(dot(inner, weight(q0, c)))
            parts.append(dot(inner, jnp.concatenate([weight(q1, c), weight(q2, c)], axis=1)))
            parts.append(dot(inner, weight(q3, c)))
        for head in range(HQ + 2):
            part = parts[head]
            if head == HQ + 1:
                value[rows] = part.astype(BF16)
                continue
            raw[rows, head * HD : (head + 1) * HD] = part.astype(BF16)
            normal, _ = unit(part)
            turned = turn_pairs(normal * scales(5 if head == HQ else 4), cosine[rows], sine[rows], 1).astype(BF16)
            if head == HQ:
                key[rows] = turned
            else:
                query[rows, head * HD : (head + 1) * HD] = turned

    def attend(tile):
        start = tile * ROWS
        rows = slice(start, start + ROWS)
        first = max(0, start - WIN)
        keys = slice(first, start + ROWS)
        lane = lax.broadcasted_iota(jnp.int32, (ROWS, 128), 1)
        row = lax.broadcasted_iota(jnp.int32, (ROWS, 128), 0) + start
        least = low[rows]
        for head in range(HQ):
            span = slice(head * HD, (head + 1) * HD)
            scores = dot_nt(query[rows, span], key[keys])
            parts, total = [], None
            for at in range(first, start + ROWS, 128):
                column = lane + at
                allowed = column >= least
                if at >= start:
                    allowed = allowed & (column <= row)
                part = jnp.where(allowed, jnp.exp2(scores[:, at - first : at - first + 128] * (LOG2E / HD**0.5)), 0.0)
                parts.append(part)
                total = part if total is None else total + part
            inverse = 1.0 / jnp.sum(total, axis=1, keepdims=True)
            probs = jnp.concatenate([(part * inverse).astype(BF16) for part in parts], axis=1)
            attn[rows, span] = dot(probs, value[keys]).astype(BF16)
            attn_t[span, rows] = attn[rows, span].T

    def mix(tile):
        rows = slice(tile * ROWS, (tile + 1) * ROWS)
        projected = dot(attn[rows], wo[...].reshape(-1, D))
        proj[rows] = projected
        normal, _ = unit(projected)
        middle = x_ref[rows].astype(F32) + normal * scales(1)
        mid[rows] = middle
        normal, _ = unit(middle)
        inner = (normal * scales(2)).astype(BF16)
        ffn_in[rows] = inner
        ffn_in_t[:, rows] = inner.T

    for tile in range(tiles):
        project(tile)
    relay.turn()
    for index in (8, 9, 10, 11, 12):
        put(index)
    for tile in range(tiles):
        attend(tile)
        if tile == 1:
            relay.turn()
    put(13)
    relay.until(2)
    put(4)
    for tile in range(tiles):
        mix(tile)
    for index in (16, 17, 18):
        put(index)
    relay.until(3)
    put(6)
    wide = 2 * cut
    for quarter in range(quarters):
        relay.until(4 + quarter)

        def feed(tile, carry):
            rows = pl.ds(pl.multiple_of(tile * ROWS, ROWS), ROWS)
            inner = ffn_in[rows]
            total = None
            for colour in range(2):
                at = colour * cut
                gated = dot(inner, weight(wgu.at[quarter, colour], 0))
                upper = dot(inner, weight(wgu.at[quarter, colour], 1))
                square = gated * gated
                bend = jnp.tanh(0.7978845608028654 * (gated + 0.044715 * square * gated))
                half = 0.5 * (1.0 + bend)
                active = gated * half
                slope = half + 0.5 * gated * (1.0 - bend * bend) * (0.7978845608028654 * (1.0 + 0.134145 * square))
                gate[quarter, rows, at : at + cut] = (slope * upper).astype(BF16)
                up[quarter, rows, at : at + cut] = active.astype(BF16)
                inside = (active * upper).astype(BF16)
                first = quarter * wide + at
                hidden[first : first + cut, rows] = inside.T
                part = wd.reshape(FF, D)[first : first + cut, :]
                part = dot(inside, part)
                total = part if total is None else total + part
            if quarter == 0:
                down[rows] = total
            else:
                down[rows] = down[rows] + total
            return carry

        lax.fori_loop(0, tiles, feed, 0)
    for index in (5, 19, 20, 21):
        put(index)
    sgrad[...] = jnp.zeros_like(sgrad)

    def finish(tile, carry):
        start = pl.multiple_of(tile * ROWS, ROWS)
        rows = pl.ds(start, ROWS)
        normal, factor = unit(down[rows])
        out[rows] = (mid[rows] + normal * scales(3)).astype(BF16)
        row = start + lax.broadcasted_iota(jnp.int32, (ROWS, 1), 0)
        grad = jnp.where(row < live_tiles * TILE, cot_ref[rows].astype(F32), 0.0)
        sgrad[...] += fold(grad * normal)
        ddown[rows] = unit_back(grad * scales(3), normal, factor).astype(BF16)
        return carry

    lax.fori_loop(0, tiles, finish, 0)
    for index in (22, 23, 24):
        put(index)
    link.finish()
    for parts in items:
        for part in parts:
            part.finish()
    for store in stores:
        store.wait()


def forward_call(dims, block_input, out_cotangent, positions, tile_count, qkv_weight, out_weight, gate_up_weight,
                 down_weight, norm_scales):
    grid = dims[:3]
    tokens = block_input.shape[0]
    rows = qkv_weight.shape[0]
    width, wide = qkv_weight.shape[1], gate_up_weight.shape[1]
    shapes = [((2,) + grid + (2 * rows, cut), BF16) for _, cut in QKV_CUTS] + [
        (grid + (2, 2, out_weight.shape[0] // 2, D), BF16),
        ((4, 2, 2) + grid + (2 * rows, FF // 8), BF16),
        (grid + (2, 2, down_weight.shape[0] // 2, D), BF16),
        ((1, norm_scales.shape[0] * dims[0] * 8), F32),
        ((D, tokens), BF16),
        ((tokens, (HQ + 1) * HD), BF16),
        ((tokens, HQ * HD), BF16),
        ((tokens, HD), BF16),
        ((tokens, HD), BF16),
        ((HQ * HD, tokens), BF16),
        ((tokens, HD // 2), F32),
        ((tokens, HD // 2), F32),
        ((D, tokens), BF16),
        ((tokens, D), F32),
        ((tokens, D), F32),
        ((FF, tokens), BF16),
        ((4, tokens, FF // 4), BF16),
        ((4, tokens, FF // 4), BF16),
        ((tokens, D), BF16),
        ((tokens, D), BF16),
        ((8, D), F32),
    ]
    sems = 2 + 17 * (dims[0] + 5)
    scratch = [pltpu.VMEM(*shape) for shape in shapes] + [
        pltpu.VMEM((tokens, D), BF16),
        pltpu.VMEM((tokens, D), BF16),
        pltpu.VMEM((tokens, HQ * HD), BF16),
        pltpu.VMEM((tokens, D), BF16),
        pltpu.VMEM((tokens, 128), jnp.int32),
        pltpu.VMEM((tokens, D), F32),
        pltpu.VMEM(grid + (2, 8, 128), F32),
        pltpu.VMEM((dims[0] * 8, 128), F32),
        pltpu.VMEM((rows, width // 2), F32),
        pltpu.VMEM((rows, wide // 2), F32),
        pltpu.VMEM((2 * rows, wide // 2), F32),
        pltpu.SemaphoreType.DMA((sems,)),
        pltpu.SemaphoreType.DMA((sems,)),
        pltpu.SemaphoreType.DMA((2,)),
        pltpu.SemaphoreType.DMA((25,)),
    ]
    vmem = pl.BlockSpec(memory_space=pltpu.VMEM)
    hbm = pl.BlockSpec(memory_space=pltpu.HBM)
    exponent = jnp.arange(HD // 2, dtype=jnp.float32) * (2.0 / HD)
    frequency = jnp.power(jnp.float32(rope_base), -exponent)[None, :]
    return pl.pallas_call(
        functools.partial(forward_kernel, dims),
        out_shape=[jax.ShapeDtypeStruct(*shape) for shape in shapes],
        in_specs=[hbm, hbm, vmem, pl.BlockSpec(memory_space=pltpu.SMEM)] + [vmem] * 6,
        out_specs=[hbm] * len(shapes),
        scratch_shapes=scratch,
        compiler_params=pltpu.CompilerParams(collective_id=0, has_side_effects=True, vmem_limit_bytes=63 << 20),
        name="forward",
    )(block_input, out_cotangent, positions.reshape(-1, 128), tile_count, frequency, qkv_weight, out_weight,
      gate_up_weight, down_weight, norm_scales[None, :])


class Pump:
    def __init__(self):
        self.active = []

    def add(self, key, steps):
        self.active.append([key, 0, steps])

    def poll(self, times=1):
        for _ in range(times):
            waiting = [entry for entry in self.active if entry[1] < len(entry[2])]
            if not waiting:
                return
            entry = min(waiting, key=lambda entry: (entry[0] + entry[1], -entry[1]))
            entry[2][entry[1]]()
            entry[1] += 1

    def drain(self):
        while any(entry[1] < len(entry[2]) for entry in self.active):
            self.poll()


def backward_kernel(dims, *refs):
    (h_q0, h_q1, h_q2, h_q3, h_wo, h_wgu, h_wd, scale, h_normed, h_raw, h_query, h_key, h_value, h_attn, h_cos, h_sin,
     h_ffn_in, h_mid, h_proj, h_hidden, h_gate, h_up, h_ddown, sgrad_out, h_x, h_cot, pos_ref, count_ref) = refs[:28]
    o_input, o_qkv, o_wo, o_wgu, o_wd, o_norm = refs[28:34]
    (wo, wgu, wd, gq0, gq1, gq2, gq3, go, gg, gd, gn,
     pool, dgu, ddown, ffn_in, attn, dproj, dmid, proj, sine, sgrad, grow, gtab, bounce, swaps, halves,
     in_sems, out_sem, send_sems, recv_sems) = refs[34:64]
    buffers = list(refs[64:])
    place = my_place(dims)
    z, y, x, core = place
    count = dims[0] * 8
    tokens = dmid.shape[0]
    tiles = tokens // ROWS
    cut = wgu.shape[-1]
    serial = iter(range(64))

    def load(src, dst):
        copy = pltpu.make_async_copy(src, dst, in_sems.at[next(serial)])
        copy.start()
        return copy

    c_ddown = load(h_ddown, ddown)
    c_hidden = [load(h_hidden.at[pl.ds(512 * j, 512)], pool.at[pl.ds(512 * j, 512)]) for j in range(4)]
    c_wd = load(h_wd, wd)
    c_gate = []
    for j in range(4):
        c_gate.append((load(h_gate.at[j], dgu.at[0, j]), load(h_up.at[j], dgu.at[1, j])))
    c_ffn_in = load(h_ffn_in, ffn_in)
    c_wgu = load(h_wgu, wgu)
    c_p3 = [load(h_mid, dmid), load(h_proj, proj), load(h_attn, attn), load(h_wo, wo)]
    enter(dims, place)

    pump = Pump()
    step = dims[0] + 5
    bases = iter(range(12, 12 + 19 * step, step))
    links = []

    def scatter(key, givens, done):
        parts = []
        for swap, given in enumerate(givens):
            held, near, far, last = buffers[:4]
            del buffers[:4]
            parts.append(Scatter(dims, place, given, held, near, far, last, swap == 1, send_sems, recv_sems, next(bases)))
        links.extend(parts)

        def stage(which):
            def run():
                for part in parts:
                    part.wait(which)
                    part.start(which + 1)

            return run

        def last_stage():
            for colour, part in enumerate(parts):
                done(colour, part.wait(3))

        for part in parts:
            part.start(0)
        pump.add(key, [stage(0), stage(1), stage(2), last_stage])

    swap_link = Link(dims, place, send_sems, recv_sems, 0)
    links.append(swap_link)
    fetched = []

    def split_rows(slot, target, start):
        def done(colour, total):
            at = slot + colour
            rows, width = target.shape[0], total.shape[1]
            first = start[colour]
            half = target.shape[1] // 2
            bounce[at % 2, :, 0:width] = total
            low, high = bounce[at % 2, 0:rows, 0:width], bounce[at % 2, rows : 2 * rows, 0:width]
            target[:, pl.ds(pl.multiple_of(core * half + first, 128), width)] = jnp.where(core == 0, low, high)
            swaps[at, :, 0:width] = jnp.where(core == 0, high, low)
            span = (at, slice(None), pl.ds(0, width))
            swap_link.send(swaps.at[span], halves.at[span], swap_link.core_peer(), at)

            def fetch():
                swap_link.copy(halves.at[span], halves.at[span], swap_link.core_peer(), at).wait_recv()
                target[:, pl.ds(pl.multiple_of((1 - core) * half + first, 128), width)] = halves[at, :, 0:width]

            fetched.append(fetch)

        return done

    def rows_done(target, start):
        def done(colour, total):
            height = total.shape[0]
            first = start + colour * height
            target[first : first + height, :] = total

        return done

    def scales(which):
        start = (0, D, 2 * D, 3 * D, 4 * D, 4 * D + HD)[which]
        return 1.0 + scale[:, start : start + (D if which < 4 else HD)]

    def weight(ref, c):
        return ref[c].reshape(-1, ref.shape[-1])

    def tile_rows(tile):
        return slice(tile * ROWS, (tile + 1) * ROWS)

    c_ddown.wait()
    grown = gd.reshape(FF, D)
    for quarter in range(4):
        c_hidden[quarter].wait()
        rows = slice(quarter * 512, (quarter + 1) * 512)
        grown[rows, :] = dot(pool[rows, :], ddown[...]).astype(BF16)
    for sub in range(2):
        scatter(sub, [(lambda core, k=2 * sub + k: gd.at[:, :, :, core, k]) for k in range(2)],
                rows_done(o_wd, sub * 2 * gd.shape[5]))
    queries, others = pool.at[pl.ds(0, tokens)], pool.at[pl.ds(tokens, tokens)]
    c_query = [load(h_query, queries), load(h_key, others.at[:, pl.ds(0, HD)]), load(h_value, others.at[:, pl.ds(HD, HD)])]
    c_wd.wait()
    c_ffn_in.wait()
    down_rows = wd.reshape(FF, D)
    for quarter in range(4):
        for copy in c_gate[quarter]:
            copy.wait()
        rows_w = down_rows[quarter * 512 : (quarter + 1) * 512, :]
        for tile in range(tiles):
            rows = tile_rows(tile)
            grad = dot_nt(ddown[rows], rows_w)
            dgu[0, quarter, rows] = (grad * dgu[0, quarter, rows].astype(F32)).astype(BF16)
            dgu[1, quarter, rows] = (grad * dgu[1, quarter, rows].astype(F32)).astype(BF16)
        for c in range(2):
            for colour in range(2):
                span = slice(colour * cut, (colour + 1) * cut)
                gg[quarter, colour, c] = dot(ffn_in[...], dgu[c, quarter, :, span]).astype(BF16).reshape(gg.shape[3:])
        scatter(2 + quarter, [(lambda core, q=quarter, k=k: gg.at[q, k, core]) for k in range(2)],
                split_rows(2 * quarter, o_wgu, [(2 * quarter + k) * cut for k in range(2)]))
        pump.poll(POLLS[0])
    xc = ddown
    c_p3.append(load(h_cot, xc))
    c_normed = load(h_normed, ffn_in)
    c_wgu.wait()
    for copy in c_p3:
        copy.wait()
    sums = [None] * 6

    def collect(which, values):
        part = fold(values)
        sums[which] = part if sums[which] is None else sums[which] + part

    for tile in range(tiles):
        rows = tile_rows(tile)
        grad = None
        for quarter in range(4):
            for c in range(2):
                part = jnp.concatenate([weight(wgu.at[quarter, colour], c) for colour in range(2)], axis=1)
                part = dot_nt(dgu[c, quarter, rows], part)
                grad = part if grad is None else grad + part
        row = tile * ROWS + lax.broadcasted_iota(jnp.int32, (ROWS, 1), 0)
        given = jnp.where(row < count_ref[0] * TILE, xc[rows].astype(F32), 0.0)
        normal, factor = unit(dmid[rows])
        collect(2, grad * normal)
        middle = given + unit_back(grad * scales(2), normal, factor)
        dmid[rows] = middle
        normal, factor = unit(proj[rows])
        collect(1, middle * normal)
        dproj[rows] = unit_back(middle * scales(1), normal, factor).astype(BF16)
        pump.poll(POLLS[1])
    c_raw = [load(h_raw.at[:, pl.ds(0, 512)], dgu.at[0, 0]), load(h_raw.at[:, pl.ds(512, 512)], dgu.at[0, 1]),
             load(h_raw.at[:, pl.ds(1024, HD)], dgu.at[0, 2, :, pl.ds(0, HD)])]
    cosine = proj.at[:, pl.ds(2 * HD, HD // 2)]
    c_rest = [load(h_cos, cosine), load(h_sin, sine), load(h_x, xc)]
    wq = wd.reshape(FF, D)
    c_qkv = []
    for c in range(2):
        for ref, within, lane in ((h_q0, 0, 0), (h_q1, 1, 0), (h_q2, 1, 128), (h_q3, 2, 0)):
            head = 3 * c + within
            at = pl.ds(head % 2 * HD + lane, ref.shape[-1])
            c_qkv.append(load(ref.at[c], wq.at[pl.ds(head // 2 * D, D), at]))
    grown_out = go.reshape(HQ * HD, D)
    for half in range(2):
        rows = slice(half * 512, (half + 1) * 512)
        grown_out[rows, :] = dot(attn[rows, :], dproj[...]).astype(BF16)
    scatter(6, [(lambda core, k=k: go.at[:, :, :, core, k]) for k in range(2)], rows_done(o_wo, 0))
    out_rows = wo.reshape(HQ * HD, D)
    for tile in range(tiles):
        rows = tile_rows(tile)
        attn[rows] = dot_nt(dproj[rows], out_rows[...]).astype(BF16)
    pump.poll(POLLS[2])
    for copy in c_query + c_raw + c_rest:
        copy.wait()
    dkey, dvalue = proj.at[:, pl.ds(0, HD)], proj.at[:, pl.ds(HD, HD)]

    for tile in range(tiles):
        start = tile * ROWS
        rows = slice(start, start + ROWS)
        first = max(0, start - WIN)
        keys = slice(first, start + ROWS)
        height = start + ROWS - first
        position = jnp.concatenate([pos_ref[2 * tile : 2 * tile + 1, :], pos_ref[2 * tile + 1 : 2 * tile + 2, :]], axis=1)
        row = lax.broadcasted_iota(jnp.int32, (1, ROWS), 1) + start
        reach = jnp.where(row < count_ref[0] * TILE, jnp.minimum(position, WIN - 1), 0)
        column = lax.broadcasted_iota(jnp.int32, (height, ROWS), 0) + first
        allowed = (column >= row - reach) & (column <= row)
        key, value = others[keys, 0:HD], others[keys, HD : 2 * HD]
        probs_all, scores_all, query_all, grads_all = [], [], [], []
        for head in range(HQ):
            span = slice(head * HD, (head + 1) * HD)
            query = queries[rows, span]
            grad = attn[rows, span]
            weights = jnp.where(allowed, jnp.exp2(dot_nt(key, query) * (LOG2E / HD**0.5)), 0.0)
            probs = weights * (1.0 / jnp.sum(weights, axis=0, keepdims=True))
            grad_probs = dot_nt(value, grad)
            both = probs * grad_probs
            delta = jnp.sum(both, axis=0, keepdims=True)
            scores = ((both - probs * delta) * HD**-0.5).astype(BF16)
            probs_all.append(probs.astype(BF16))
            scores_all.append(scores)
            query_all.append(query)
            grads_all.append(grad)
        value_part = dot(jnp.concatenate(probs_all, axis=1), jnp.concatenate(grads_all, axis=0))
        key_part = dot(jnp.concatenate(scores_all, axis=1), jnp.concatenate(query_all, axis=0))
        if height > ROWS:
            old = slice(first, start)
            dvalue[old, :] = dvalue[old, :] + value_part[: height - ROWS]
            dkey[old, :] = dkey[old, :] + key_part[: height - ROWS]
        dvalue[rows, :] = value_part[height - ROWS :]
        dkey[rows, :] = key_part[height - ROWS :]
        for head in range(HQ):
            span = slice(head * HD, (head + 1) * HD)
            grad = turn_pairs(dot_tn(scores_all[head], key), cosine[rows, :], sine[rows, :], -1)
            normal, factor = unit(dgu[0, head // 2, rows, (head % 2) * HD : (head % 2 + 1) * HD].astype(F32))
            collect(4, grad * normal)
            queries[rows, span] = unit_back(grad * scales(4), normal, factor).astype(BF16)
        pump.poll(POLLS[3])
    for tile in range(tiles):
        rows = tile_rows(tile)
        grad = turn_pairs(dkey[rows, :], cosine[rows, :], sine[rows, :], -1)
        normal, factor = unit(dgu[0, 2, rows, 0:HD].astype(F32))
        collect(5, grad * normal)
        others[rows, 2 * HD : 3 * HD] = unit_back(grad * scales(5), normal, factor).astype(BF16)
        others[rows, 3 * HD : 4 * HD] = dvalue[rows, :].astype(BF16)
    c_normed.wait()

    def grad_columns(rows, head):
        ref, at = (queries, head * HD) if head < HQ else (others, (head - HQ + 2) * HD)
        return ref[rows, at : at + HD]

    for head in range(HQ + 2):
        term = dot(ffn_in[...], grad_columns(slice(0, tokens), head)).astype(BF16)
        c, within = head // 3, head % 3
        if within == 0:
            gq0[c] = term.reshape(gq0.shape[1:])
        elif within == 2:
            gq3[c] = term.reshape(gq3.shape[1:])
        else:
            gq1[c] = term[:, 0:128].reshape(gq1.shape[1:])
            gq2[c] = term[:, 128:256].reshape(gq2.shape[1:])
    for sub, pair in enumerate(((gq0, gq1), (gq2, gq3))):
        scatter(7 + sub, [(lambda core, ref=ref: ref.at[core]) for ref in pair],
                split_rows(8 + 2 * sub, o_qkv, [QKV_CUTS[2 * sub + k][0] for k in range(2)]))
    for copy in c_qkv:
        copy.wait()
    for tile in range(tiles):
        rows = tile_rows(tile)
        grad = None
        for head in range(HQ + 2):
            part = wq[head // 2 * D : (head // 2 + 1) * D, head % 2 * HD : (head % 2 + 1) * HD]
            part = dot_nt(grad_columns(rows, head), part)
            grad = part if grad is None else grad + part
        normal, factor = unit(xc[rows].astype(F32))
        collect(0, grad * normal)
        dmid[rows] = dmid[rows] + unit_back(grad * scales(0), normal, factor)
        pump.poll(POLLS[4])
    store = pltpu.make_async_copy(dmid, o_input, out_sem)
    store.start()
    sums[3] = sgrad_out[...]
    at = 0
    for part in sums:
        grow[:, at : at + part.shape[1]] = jnp.sum(part, axis=0, keepdims=True)
        at += part.shape[1]
    per = at // count
    table = jnp.zeros((count, 128), F32)
    for begin in range(0, at, 512):
        owner, entry = chunk_masks(per, begin, 512)
        picked = entry.astype(F32).astype(BF16)
        rest = jnp.where(owner(count), grow[:, begin : begin + 512], 0.0)
        for _ in range(3):
            piece = rest.astype(BF16)
            rest = rest - piece.astype(F32)
            table = table + dot_nt(piece, picked)
    gtab[...] = table
    flat = gn.reshape(count, 8, 128)
    for device in range(count):
        flat[device] = jnp.broadcast_to(gtab[device : device + 1, :], (8, 128))

    def norm_done(colour, total):
        o_norm[...] = total

    scatter(8.5, [lambda core: gn.at[:, :, :, core]], norm_done)
    pump.drain()
    for fetch in fetched:
        fetch()
    for link in links:
        link.finish()
    store.wait()


POLLS = (3, 2, 2, 2, 2)


def backward_call(dims, saved, block_input, out_cotangent, positions, tile_count, shard_rows):
    grid = dims[:3]
    count = dims[0] * 8
    tokens = block_input.shape[0]
    qkv_rows, out_rows, down_rows, norm_rows = shard_rows
    width = (HQ + 2) * HD
    bf = lambda *shape: pltpu.VMEM(shape, BF16)
    fp = lambda *shape: pltpu.VMEM(shape, F32)
    pair = 2 * qkv_rows
    weights = [bf(*((2,) + grid + (pair, cut))) for _, cut in QKV_CUTS] + [
        bf(*(grid + (2, 2, out_rows // 2, D))),
        bf(*((4, 2, 2) + grid + (pair, FF // 8))),
        bf(*(grid + (2, 2, down_rows // 2, D))),
    ]
    scratch = weights[4:] + weights[:6] + [
        bf(*(grid + (2, 4, down_rows // 4, D))),
        fp(*(grid + (2, 8, 128))),
        bf(FF, tokens),
        bf(2, 4, tokens, FF // 4),
        bf(tokens, D),
        bf(D, tokens),
        bf(HQ * HD, tokens),
        bf(tokens, D),
        fp(tokens, D),
        fp(tokens, D),
        fp(tokens, HD // 2),
        fp(8, D),
        fp(1, 4 * D + 2 * HD),
        fp(count, 128),
        fp(2, pair, 256),
        fp(12, qkv_rows, 256),
        fp(12, qkv_rows, 256),
        pltpu.SemaphoreType.DMA((64,)),
        pltpu.SemaphoreType.DMA,
    ]
    sems = 12 + 19 * (dims[0] + 5)
    scratch += [pltpu.SemaphoreType.DMA((sems,)), pltpu.SemaphoreType.DMA((sems,))]
    blocks = [[(down_rows // 4, D)] * 2] * 2 + [[(pair, FF // 8)] * 2] * 4 + [[(out_rows // 2, D)] * 2]
    blocks += [[(pair, QKV_CUTS[0][1]), (pair, QKV_CUTS[1][1])], [(pair, QKV_CUTS[2][1]), (pair, QKV_CUTS[3][1])], [(8, 128)]]
    for colours in blocks:
        for swap, block in enumerate(colours):
            make = fp if block == (8, 128) else bf
            scratch.append(make(*(grid + block)))
            scratch.append(make(*(((grid[0], grid[1]) if swap else (grid[0], grid[2])) + block)))
            scratch.append(make(*((grid[0],) + block)))
            scratch.append(make(*((grid[0] - 1,) + block)))
    vmem = pl.BlockSpec(memory_space=pltpu.VMEM)
    hbm = pl.BlockSpec(memory_space=pltpu.HBM)
    outs = [(tokens, D), (qkv_rows, width), (out_rows, D), (qkv_rows, 2 * FF), (down_rows, D), (8, 128)]
    saved = list(saved)
    saved[:4] = [array.reshape(2, D, -1) for array in saved[:4]]
    inputs = saved[:23] + [saved[24], block_input, out_cotangent, positions.reshape(-1, 128), tile_count]
    specs = [hbm] * 28
    specs[7] = specs[23] = specs[26] = vmem
    specs[27] = pl.BlockSpec(memory_space=pltpu.SMEM)
    return pl.pallas_call(
        functools.partial(backward_kernel, dims),
        out_shape=[jax.ShapeDtypeStruct(shape, F32) for shape in outs],
        in_specs=specs,
        out_specs=[hbm] + [vmem] * 5,
        scratch_shapes=scratch,
        compiler_params=pltpu.CompilerParams(collective_id=1, has_side_effects=True, vmem_limit_bytes=67043328),
        name="backward",
    )(*inputs)


def plain_pass(
    block_input,
    out_cotangent,
    segment_ids,
    positions,
    tile_count,
    qkv_weight,
    out_weight,
    gate_up_weight,
    down_weight,
    norm_scales,
):
    qkv_full, out_full, gate_up_full, down_full, norm_full = (
        lax.all_gather(array.astype(jnp.bfloat16), "dp", axis=0, tiled=True)
        for array in (qkv_weight, out_weight, gate_up_weight, down_weight, norm_scales)
    )
    attn_full = (qkv_full, out_full, norm_full)
    ffn_full = (gate_up_full, down_full)
    row_count = block_input.shape[0]
    live_rows = jnp.arange(row_count, dtype=jnp.int32) // TILE < tile_count[0]
    block_output, attn_saved, ffn_saved = forward_pass(
        attn_full, ffn_full, block_input, segment_ids, positions, live_rows
    )
    attn_back, ffn_back = attn_full, ffn_full
    grad_out = out_cotangent.astype(jnp.float32) * live_rows[:, None].astype(jnp.float32)
    d_mid, gate_up_term, down_term, ffn_scale_grad, out_scale_grad = ffn_backward(
        ffn_back, attn_back[2].astype(jnp.float32), ffn_saved, grad_out
    )
    (
        input_grad,
        qkv_term,
        out_term,
        in_scale_grad,
        post_scale_grad,
        query_scale_grad,
        key_scale_grad,
    ) = attn_backward(attn_back, attn_saved, d_mid)
    norm_term = jnp.concatenate(
        [
            in_scale_grad,
            post_scale_grad,
            ffn_scale_grad,
            out_scale_grad,
            query_scale_grad,
            key_scale_grad,
        ]
    )
    sums = tuple(
        lax.psum_scatter(term, "dp", scatter_dimension=0, tiled=True)
        for term in (qkv_term, out_term, gate_up_term, down_term, norm_term)
    )
    return (block_output, input_grad) + sums


def shards(
    count,
    block_input,
    out_cotangent,
    segment_ids,
    positions,
    tile_count,
    qkv_weight,
    qkv_first,
    qkv_second,
    out_weight,
    out_first,
    out_second,
    gate_up_weight,
    gate_up_first,
    gate_up_second,
    down_weight,
    down_first,
    down_second,
    norm_scales,
    norm_first,
    norm_second,
):
    dims = grid_dims(count)
    if own_transfers(count, qkv_weight.shape[1], qkv_weight.shape[0]):
        saved = forward_call(
            dims, block_input, out_cotangent, positions, tile_count, qkv_weight, out_weight, gate_up_weight, down_weight,
            norm_scales,
        )
        block_output = saved[23]
        shard_rows = (qkv_weight.shape[0], out_weight.shape[0], down_weight.shape[0], norm_scales.shape[0])
        input_grad, qkv_grad, out_grad, gate_up_grad, down_grad, norm_rows = backward_call(
            dims, saved, block_input, out_cotangent, positions, tile_count, shard_rows
        )
        norm_grad = norm_rows[0, : norm_scales.shape[0]]
    else:
        block_output, input_grad, qkv_grad, out_grad, gate_up_grad, down_grad, norm_grad = plain_pass(
            block_input, out_cotangent, segment_ids, positions, tile_count, qkv_weight, out_weight, gate_up_weight,
            down_weight, norm_scales,
        )
    qkv_new, qkv_first_new, qkv_second_new = adam_update(
        qkv_weight, qkv_grad, qkv_first, qkv_second
    )
    out_new, out_first_new, out_second_new = adam_update(
        out_weight, out_grad, out_first, out_second
    )
    gate_up_new, gate_up_first_new, gate_up_second_new = adam_update(
        gate_up_weight, gate_up_grad, gate_up_first, gate_up_second
    )
    down_new, down_first_new, down_second_new = adam_update(
        down_weight, down_grad, down_first, down_second
    )
    norms_new, norm_first_new, norm_second_new = adam_update(
        norm_scales, norm_grad, norm_first, norm_second
    )
    return (
        block_output,
        input_grad,
        qkv_grad,
        out_grad,
        gate_up_grad,
        down_grad,
        norm_grad,
        qkv_new,
        out_new,
        gate_up_new,
        down_new,
        norms_new,
        qkv_first_new,
        out_first_new,
        gate_up_first_new,
        down_first_new,
        norm_first_new,
        qkv_second_new,
        out_second_new,
        gate_up_second_new,
        down_second_new,
        norm_second_new,
    )


def solution(mesh):
    in_specs = (
        P("dp", None),
        P("dp", None),
        P("dp"),
        P("dp"),
        P("dp"),
        P("dp", None),
        P("dp", None),
        P("dp", None),
        P("dp", None),
        P("dp", None),
        P("dp", None),
        P("dp", None),
        P("dp", None),
        P("dp", None),
        P("dp", None),
        P("dp", None),
        P("dp", None),
        P("dp"),
        P("dp"),
        P("dp"),
    )
    out_specs = (
        P("dp", None),
        P("dp", None),
        P("dp", None),
        P("dp", None),
        P("dp", None),
        P("dp", None),
        P("dp"),
        P("dp", None),
        P("dp", None),
        P("dp", None),
        P("dp", None),
        P("dp"),
        P("dp", None),
        P("dp", None),
        P("dp", None),
        P("dp", None),
        P("dp"),
        P("dp", None),
        P("dp", None),
        P("dp", None),
        P("dp", None),
        P("dp"),
    )
    body = functools.partial(shards, mesh.shape["dp"])
    return jax.shard_map(body, mesh=mesh, in_specs=in_specs, out_specs=out_specs, check_vma=False)
```

```python
import functools
import math

import numpy as np

import jax
import jax.numpy as jnp
from jax import lax
from jax.experimental import pallas as pl
from jax.experimental.pallas import tpu as pltpu
from jax.sharding import PartitionSpec as P

D = 640
HQ = 4
HD = 256
FF = 2048
WIN = 512
TILE = 128


norm_eps = 1e-06
rope_base = 10000.0
beta_one = 0.9
beta_two = 0.999
adam_eps = 1e-08
learn_rate = 0.02
weight_decay = 0.1
adam_step = 3


def rms_scale(values, scales):
    mean_square = jnp.mean(values * values, axis=-1, keepdims=True)
    return values * lax.rsqrt(mean_square + norm_eps) * (1.0 + scales)


def gelu_tanh(values):
    inner_term = 0.7978845608028654 * (values + 0.044715 * values * values * values)
    return 0.5 * values * (1.0 + jnp.tanh(inner_term))


def gated_unit(gate_act, up_act):
    return gelu_tanh(gate_act) * up_act


def rotate(values, cosine, sine_table):
    half_dim = values.shape[-1] // 2
    front_half = values[..., :half_dim]
    back_half = values[..., half_dim:]
    return jnp.concatenate(
        [
            front_half * cosine - back_half * sine_table,
            back_half * cosine + front_half * sine_table,
        ],
        axis=-1,
    )


def rope_tables(positions, head_dim):
    exponent = jnp.arange(head_dim // 2, dtype=jnp.float32) * (2.0 / head_dim)
    frequency = jnp.power(jnp.float32(rope_base), -exponent)
    angles = positions.astype(jnp.float32)[:, None] * frequency[None, :]
    return (jnp.cos(angles)[:, None, :], jnp.sin(angles)[:, None, :])


def qk_prepare(query_raw, key_raw, q_scale, k_scale, cosine, sine_table):
    return (
        rotate(rms_scale(query_raw, q_scale), cosine, sine_table),
        rotate(rms_scale(key_raw, k_scale), cosine, sine_table),
    )


def contract(form, left, right):
    return jnp.einsum(form, left, right, preferred_element_type=jnp.float32)


def window_mask(block_index, window, segment_pad, live_pad):
    start_row = block_index * window
    query_rows = start_row + jnp.arange(window, dtype=jnp.int32)
    key_rows = start_row - window + jnp.arange(2 * window, dtype=jnp.int32)
    query_seg = segment_pad[start_row + window : start_row + 2 * window]
    key_seg = segment_pad[start_row : start_row + 2 * window]
    query_live = live_pad[start_row + window : start_row + 2 * window]
    key_live = live_pad[start_row : start_row + 2 * window]
    diagonal = key_rows[None, :] == query_rows[:, None]
    earlier = (key_rows[None, :] < query_rows[:, None]) & (
        query_rows[:, None] - key_rows[None, :] < window
    )
    same_seq = (query_seg[:, None] == key_seg[None, :]) & query_live[:, None] & key_live[None, :]
    return diagonal | earlier & same_seq


def front_pad(values, window):
    return jnp.concatenate([jnp.zeros((window,) + values.shape[1:], values.dtype), values], axis=0)


def attend_forward(query_bf, key_bf, value_bf, segment_pad, live_pad):
    row_count = query_bf.shape[0]
    score_scale = HD ** (-0.5)
    key_padded = front_pad(key_bf, WIN)
    value_padded = front_pad(value_bf, WIN)
    out_blocks = []
    log_blocks = []
    for block_index in range(row_count // WIN):
        start_row = block_index * WIN
        allowed = window_mask(block_index, WIN, segment_pad, live_pad)
        query_block = query_bf[start_row : start_row + WIN]
        key_block = key_padded[start_row : start_row + 2 * WIN]
        value_block = value_padded[start_row : start_row + 2 * WIN]
        scores = contract("qhd,kd->hqk", query_block, key_block) * score_scale
        exp_scores = jnp.where(allowed[None], jnp.exp(scores), 0.0)
        exp_total = jnp.sum(exp_scores, axis=-1)
        probs_bf = (exp_scores / exp_total[..., None]).astype(jnp.bfloat16)
        out_blocks.append(contract("hqk,kd->qhd", probs_bf, value_block).reshape(WIN, HQ * HD))
        log_blocks.append(jnp.log(exp_total))
    return (jnp.concatenate(out_blocks, axis=0), jnp.concatenate(log_blocks, axis=1))


def attend_backward(
    query_bf, key_bf, value_bf, attn_bf, dattn_bf, log_total, segment_pad, live_pad
):
    row_count = query_bf.shape[0]
    score_scale = HD ** (-0.5)
    key_padded = front_pad(key_bf, WIN)
    value_padded = front_pad(value_bf, WIN)
    attn_heads = attn_bf.reshape(row_count, HQ, HD)
    dattn_heads = dattn_bf.reshape(row_count, HQ, HD)
    delta_rows = jnp.sum(dattn_heads.astype(jnp.float32) * attn_heads.astype(jnp.float32), axis=-1)
    key_grad = jnp.zeros((row_count + WIN, HD), jnp.float32)
    value_grad = jnp.zeros((row_count + WIN, HD), jnp.float32)
    query_parts = []
    for block_index in range(row_count // WIN):
        start_row = block_index * WIN
        allowed = window_mask(block_index, WIN, segment_pad, live_pad)
        query_block = query_bf[start_row : start_row + WIN]
        key_block = key_padded[start_row : start_row + 2 * WIN]
        value_block = value_padded[start_row : start_row + 2 * WIN]
        dout_block = dattn_heads[start_row : start_row + WIN]
        scores = contract("qhd,kd->hqk", query_block, key_block) * score_scale
        probs = jnp.where(
            allowed[None], jnp.exp(scores - log_total[:, start_row : start_row + WIN, None]), 0.0
        )
        probs_bf = probs.astype(jnp.bfloat16)
        value_grad = value_grad.at[start_row : start_row + 2 * WIN].add(
            contract("hqk,qhd->kd", probs_bf, dout_block)
        )
        dprobs = contract("qhd,kd->hqk", dout_block, value_block)
        dscores = (
            probs * (dprobs - delta_rows[start_row : start_row + WIN].T[:, :, None]) * score_scale
        )
        dscores_bf = dscores.astype(jnp.bfloat16)
        query_parts.append(contract("hqk,kd->qhd", dscores_bf, key_block))
        key_grad = key_grad.at[start_row : start_row + 2 * WIN].add(
            contract("hqk,qhd->kd", dscores_bf, query_block)
        )
    return (jnp.concatenate(query_parts, axis=0), key_grad[WIN:], value_grad[WIN:])


def forward_pass(attn_full, ffn_full, block_input, segment_ids, positions, live_rows):
    qkv_w, out_w, norm_bf = attn_full
    gate_up_w, down_w = ffn_full
    norm_values = norm_bf.astype(jnp.float32)
    row_count = block_input.shape[0]
    resid_in = block_input.astype(jnp.float32)
    normed = rms_scale(resid_in, norm_values[0:D]).astype(jnp.bfloat16)
    qkv_proj = jnp.dot(normed, qkv_w, preferred_element_type=jnp.float32)
    query_raw = qkv_proj[:, : HQ * HD].reshape(row_count, HQ, HD)
    key_raw = qkv_proj[:, HQ * HD : (HQ + 1) * HD].reshape(row_count, 1, HD)
    value_bf = qkv_proj[:, (HQ + 1) * HD :].astype(jnp.bfloat16)
    cosine, sine_table = rope_tables(positions, HD)
    query_rot, key_rot = qk_prepare(
        query_raw,
        key_raw,
        norm_values[4 * D : 4 * D + HD],
        norm_values[4 * D + HD : 4 * D + 2 * HD],
        cosine,
        sine_table,
    )
    query_bf = query_rot.astype(jnp.bfloat16)
    key_bf = key_rot[:, 0, :].astype(jnp.bfloat16)
    segment_pad = front_pad(segment_ids, WIN)
    position_pad = front_pad(positions, WIN)
    live_pad = front_pad(live_rows, WIN)
    attn_out, log_total = attend_forward(query_bf, key_bf, value_bf, segment_pad, live_pad)
    attn_bf = attn_out.astype(jnp.bfloat16)
    attn_proj = jnp.dot(attn_bf, out_w, preferred_element_type=jnp.float32)
    mid_resid = resid_in + rms_scale(attn_proj, norm_values[D : 2 * D])
    ffn_in = rms_scale(mid_resid, norm_values[2 * D : 3 * D]).astype(jnp.bfloat16)
    gate_up = jnp.dot(ffn_in, gate_up_w, preferred_element_type=jnp.float32)
    gate_act = gate_up[:, :FF]
    up_act = gate_up[:, FF:]
    hidden = gated_unit(gate_act, up_act).astype(jnp.bfloat16)
    down_act = jnp.dot(hidden, down_w, preferred_element_type=jnp.float32)
    block_output = (mid_resid + rms_scale(down_act, norm_values[3 * D : 4 * D])).astype(
        jnp.bfloat16
    )
    attn_saved = (
        resid_in,
        normed,
        query_raw,
        key_raw,
        query_bf,
        key_bf,
        value_bf,
        cosine,
        sine_table,
        segment_pad,
        position_pad,
        live_pad,
        attn_bf,
        log_total,
        attn_proj,
    )
    ffn_saved = (mid_resid, ffn_in, gate_act, up_act, hidden, down_act)
    return (block_output, attn_saved, ffn_saved)


def ffn_backward(ffn_back, norm_values, ffn_saved, grad_out):
    gate_up_w, down_w = ffn_back
    mid_resid, ffn_in, gate_act, up_act, hidden, down_act = ffn_saved
    d_down, out_scale_grad = jax.vjp(rms_scale, down_act, norm_values[3 * D : 4 * D])[1](grad_out)
    d_down_bf = d_down.astype(jnp.bfloat16)
    d_hidden = jnp.dot(d_down_bf, down_w.T, preferred_element_type=jnp.float32)
    down_term = jnp.dot(hidden.T, d_down_bf, preferred_element_type=jnp.float32)
    d_gate, d_up = jax.vjp(gated_unit, gate_act, up_act)[1](d_hidden)
    d_gate_up = jnp.concatenate([d_gate, d_up], axis=1).astype(jnp.bfloat16)
    d_ffn_in = jnp.dot(d_gate_up, gate_up_w.T, preferred_element_type=jnp.float32)
    gate_up_term = jnp.dot(ffn_in.T, d_gate_up, preferred_element_type=jnp.float32)
    d_mid_part, ffn_scale_grad = jax.vjp(rms_scale, mid_resid, norm_values[2 * D : 3 * D])[1](
        d_ffn_in
    )
    return (grad_out + d_mid_part, gate_up_term, down_term, ffn_scale_grad, out_scale_grad)


def attn_backward(attn_back, attn_saved, d_mid):
    qkv_w, out_w, norm_bf = attn_back
    norm_values = norm_bf.astype(jnp.float32)
    (
        resid_in,
        normed,
        query_raw,
        key_raw,
        query_bf,
        key_bf,
        value_bf,
        cosine,
        sine_table,
        segment_pad,
        position_pad,
        live_pad,
        attn_bf,
        log_total,
        attn_proj,
    ) = attn_saved
    row_count = resid_in.shape[0]
    d_proj, post_scale_grad = jax.vjp(rms_scale, attn_proj, norm_values[D : 2 * D])[1](d_mid)
    d_proj_bf = d_proj.astype(jnp.bfloat16)
    out_term = jnp.dot(attn_bf.T, d_proj_bf, preferred_element_type=jnp.float32)
    dattn_bf = jnp.dot(d_proj_bf, out_w.T, preferred_element_type=jnp.float32).astype(jnp.bfloat16)
    d_query, d_key, d_value = attend_backward(
        query_bf, key_bf, value_bf, attn_bf, dattn_bf, log_total, segment_pad, live_pad
    )

    def prepare(query_in, key_in, q_in, k_in):
        return qk_prepare(query_in, key_in, q_in, k_in, cosine, sine_table)

    d_query_raw, d_key_raw, query_scale_grad, key_scale_grad = jax.vjp(
        prepare,
        query_raw,
        key_raw,
        norm_values[4 * D : 4 * D + HD],
        norm_values[4 * D + HD : 4 * D + 2 * HD],
    )[1]((d_query, d_key[:, None, :]))
    d_qkv = jnp.concatenate(
        [d_query_raw.reshape(row_count, HQ * HD), d_key_raw.reshape(row_count, HD), d_value], axis=1
    ).astype(jnp.bfloat16)
    d_normed = jnp.dot(d_qkv, qkv_w.T, preferred_element_type=jnp.float32)
    qkv_term = jnp.dot(normed.T, d_qkv, preferred_element_type=jnp.float32)
    d_input_part, in_scale_grad = jax.vjp(rms_scale, resid_in, norm_values[0:D])[1](d_normed)
    return (
        d_mid + d_input_part,
        qkv_term,
        out_term,
        in_scale_grad,
        post_scale_grad,
        query_scale_grad,
        key_scale_grad,
    )


def adam_update(weight, grad, first_moment, second_moment):
    first_new = beta_one * first_moment + (1.0 - beta_one) * grad
    second_new = beta_two * second_moment + (1.0 - beta_two) * grad * grad
    corr_one = 1.0 - beta_one**adam_step
    corr_two = 1.0 - beta_two**adam_step
    step_dir = (
        first_new / corr_one / (jnp.sqrt(second_new / corr_two) + adam_eps) + weight_decay * weight
    )
    return (weight - learn_rate * step_dir, first_new, second_new)


LOGICAL = pl.DeviceIdType.LOGICAL
ALL = slice(None)
SLOTS = 10


def grid_dims(count):
    return (count // 8, 2, 2, 2)


def my_place(dims):
    index = lax.axis_index("dp")
    core = lax.rem(index, dims[3])
    index = lax.div(index, dims[3])
    x = lax.rem(index, dims[2])
    index = lax.div(index, dims[2])
    return (lax.div(index, dims[1]), lax.rem(index, dims[1]), x, core)


def device_at(dims, z, y, x, core):
    return ((z * dims[1] + y) * dims[2] + x) * dims[3] + core


def enter(dims, place):
    z, y, x, core = place
    barrier = pltpu.get_barrier_semaphore()
    peers = [device_at(dims, lax.rem(z + k, dims[0]), y, x, core) for k in range(1, dims[0])]
    peers.append(device_at(dims, z, 1 - y, x, core))
    peers.append(device_at(dims, z, y, 1 - x, core))
    peers.append(device_at(dims, z, y, x, 1 - core))
    for peer in peers:
        pl.semaphore_signal(barrier, inc=1, device_id=peer, device_id_type=LOGICAL)
    pl.semaphore_wait(barrier, len(peers))


class Link:
    def __init__(self, dims, place, send_sems, recv_sems, base):
        self.dims, self.place = dims, place
        self.send_sems, self.recv_sems, self.base = send_sems, recv_sems, base
        self.pending = []

    def copy(self, src, dst, target, slot):
        return pltpu.make_async_remote_copy(
            src_ref=src,
            dst_ref=dst,
            send_sem=self.send_sems.at[self.base + slot],
            recv_sem=self.recv_sems.at[self.base + slot],
            device_id=target,
            device_id_type=LOGICAL,
        )

    def send(self, src, dst, target, slot):
        copy = self.copy(src, dst, target, slot)
        copy.start()
        self.pending.append(copy)

    def finish(self):
        for copy in self.pending:
            copy.wait_send()
        self.pending = []

    def z_peer(self, k):
        z, y, x, core = self.place
        return device_at(self.dims, lax.rem(z + k, self.dims[0]), y, x, core)

    def y_peer(self):
        z, y, x, core = self.place
        return device_at(self.dims, z, 1 - y, x, core)

    def x_peer(self):
        z, y, x, core = self.place
        return device_at(self.dims, z, y, 1 - x, core)

    def core_peer(self):
        z, y, x, core = self.place
        return device_at(self.dims, z, y, x, 1 - core)


class Gather(Link):
    def __init__(self, dims, place, view, swap, send_sems, recv_sems, base):
        super().__init__(dims, place, send_sems, recv_sems, base)
        self.view, self.swap = view, swap

    def plan(self, stage):
        z, y, x, core = self.place
        count = self.dims[0]
        view = self.view
        if stage == 0:
            return [
                (view(z, y, x, core), self.z_peer(k), k - 1, view(lax.rem(z + count - k, count), y, x, core))
                for k in range(1, count)
            ]
        slot = count + stage
        near, far = (self.y_peer(), self.x_peer()) if self.swap else (self.x_peer(), self.y_peer())
        if stage == 1:
            got = view(ALL, 1 - y, x, core) if self.swap else view(ALL, y, 1 - x, core)
            return [(view(ALL, y, x, core), near, slot, got)]
        if stage == 2:
            mine = view(ALL, ALL, x, core) if self.swap else view(ALL, y, ALL, core)
            got = view(ALL, ALL, 1 - x, core) if self.swap else view(ALL, 1 - y, ALL, core)
            return [(mine, far, slot, got)]
        if stage == 3:
            mine = view(ALL, ALL, x, core) if self.swap else view(ALL, y, ALL, core)
            got = view(ALL, ALL, x, 1 - core) if self.swap else view(ALL, y, ALL, 1 - core)
        else:
            mine = view(ALL, ALL, 1 - x, core) if self.swap else view(ALL, 1 - y, ALL, core)
            got = view(ALL, ALL, 1 - x, 1 - core) if self.swap else view(ALL, 1 - y, ALL, 1 - core)
        return [(mine, self.core_peer(), slot, got)]

    def start(self, stage):
        for src, target, slot, _ in self.plan(stage):
            self.send(src, src, target, slot)

    def wait(self, stage):
        for _, target, slot, got in self.plan(stage):
            self.copy(got, got, target, slot).wait_recv()


class Scatter(Link):
    def __init__(self, dims, place, given, held, near, far, last, swap, send_sems, recv_sems, base):
        super().__init__(dims, place, send_sems, recv_sems, base)
        self.given, self.held, self.near, self.far, self.last, self.swap = given, held, near, far, last, swap

    def start(self, stage):
        z, y, x, core = self.place
        count = self.dims[0]
        held = self.held
        if stage == 0:
            self.send(self.given(1 - core), held, self.core_peer(), 0)
        elif stage == 1:
            if self.swap:
                self.send(held.at[:, :, 1 - x], self.near, self.x_peer(), 1)
            else:
                self.send(held.at[:, 1 - y], self.near, self.y_peer(), 1)
        elif stage == 2:
            if self.swap:
                self.send(held.at[:, 1 - y, x], self.far, self.y_peer(), 2)
            else:
                self.send(held.at[:, y, 1 - x], self.far, self.x_peer(), 2)
        else:
            for k in range(1, count):
                self.send(held.at[lax.rem(z + k, count), y, x], self.last.at[k - 1], self.z_peer(k), 2 + k)

    def wait(self, stage):
        z, y, x, core = self.place
        count = self.dims[0]
        held = self.held
        if stage == 0:
            self.copy(self.given(1 - core), held, self.core_peer(), 0).wait_recv()
            mine = self.given(core)

            def add(row, carry):
                held[row] = held[row] + mine[row]
                return carry

            lax.fori_loop(0, count, add, 0)
        elif stage == 1:
            self.copy(self.near, self.near, self.core_peer(), 1).wait_recv()

            def add(row, carry):
                if self.swap:
                    held[row, :, x] = held[row, :, x] + self.near[row]
                else:
                    held[row, y] = held[row, y] + self.near[row]
                return carry

            lax.fori_loop(0, count, add, 0)
        elif stage == 2:
            self.copy(self.far, self.far, self.core_peer(), 2).wait_recv()

            def add(row, carry):
                held[row, y, x] = held[row, y, x] + self.far[row]
                return carry

            lax.fori_loop(0, count, add, 0)
        else:
            total = held[z, y, x].astype(jnp.float32)
            for k in range(1, count):
                self.copy(self.last.at[k - 1], self.last.at[k - 1], self.core_peer(), 2 + k).wait_recv()
                total = total + self.last[k - 1].astype(jnp.float32)
            return total


def own_transfers(count, width, rows):
    return count % 8 == 0 and rows * 2 % 8 == 0 and width % 512 == 0


BF16 = jnp.bfloat16
F32 = jnp.float32
LOG2E = 1.4426950408889634
ROWS = 256


def dot(left, right):
    return jnp.dot(left, right, preferred_element_type=F32)


def dot_nt(left, right):
    return lax.dot_general(left, right, (((1,), (1,)), ((), ())), preferred_element_type=F32)


def dot_tn(left, right):
    return lax.dot_general(left, right, (((0,), (0,)), ((), ())), preferred_element_type=F32)


def fold(values):
    return jnp.sum(values.reshape(values.shape[0] // 8, 8, values.shape[1]), axis=0)


def unit(values):
    scale = lax.rsqrt(jnp.mean(values * values, axis=-1, keepdims=True) + norm_eps)
    return values * scale, scale


def unit_back(grad, normal, scale):
    return scale * (grad - normal * jnp.mean(grad * normal, axis=-1, keepdims=True))


def turn_pairs(values, cosine, sine, sign):
    front, back = values[:, : HD // 2], values[:, HD // 2 :]
    if sign > 0:
        return jnp.concatenate([front * cosine - back * sine, back * cosine + front * sine], axis=1)
    return jnp.concatenate([front * cosine + back * sine, back * cosine - front * sine], axis=1)


def column_of(row):
    return jnp.broadcast_to(row, (128, 128)).T


def chunk_masks(per, start, width):
    def owner(count):
        column = lax.broadcasted_iota(jnp.int32, (count, width), 1) + start
        first = lax.broadcasted_iota(jnp.int32, (count, width), 0) * per
        return (column >= first) & (column < first + per)

    entry = lax.broadcasted_iota(jnp.int32, (128, width), 0)
    gap = (lax.broadcasted_iota(jnp.int32, (128, width), 1) + start - entry).astype(F32)
    place = (jnp.floor((gap + 0.5) * (1.0 / per)) * per == gap) & (entry < per)
    return owner, place


def spread_scales(norm_all, rows_ref, scale_ref, per, count):
    flat = norm_all.reshape(count, 8, 128)
    for device in range(count):
        rows_ref[device : device + 1, :] = flat[device, 0:1, :]
    table = rows_ref[...].astype(BF16)
    step = 512

    def part(index, carry):
        start = pl.multiple_of(index * step, step)
        owner, place = chunk_masks(per, start, step)
        spread = dot_tn(table, owner(count).astype(F32).astype(BF16))
        scale_ref[:, pl.ds(start, step)] = jnp.sum(jnp.where(place, spread, 0.0), axis=0, keepdims=True)
        return carry

    lax.fori_loop(0, count * per // step, part, 0)


class Pump:
    RATE = 46500.0
    CORE_RATE = 500000.0
    LATENCY = {"z": 2.8, "x": 1.4, "y": 1.4, "core": 1.0}

    def __init__(self):
        self.now, self.free, self.entries = 0.0, {}, []

    def launch(self, flows):
        done = self.now
        for link, size in flows:
            begin = max(self.now, self.free.get(link, 0.0))
            self.free[link] = begin + size / (self.CORE_RATE if link == "core" else self.RATE)
            done = max(done, self.free[link] + self.LATENCY[link])
        return done

    def add(self, flows, steps):
        entry = [self.launch(flows), 0, steps]
        self.entries.append(entry)
        return entry

    def first(self):
        waiting = [entry for entry in self.entries if entry[1] < len(entry[2])]
        return min(waiting, key=lambda entry: entry[0]) if waiting else None

    def fire(self, entry):
        run, flows = entry[2][entry[1]]
        run()
        self.now = max(self.now, entry[0]) + 0.3
        entry[0] = self.launch(flows)
        entry[1] += 1

    def work(self, time):
        self.now += time
        entry = self.first()
        while entry is not None and entry[0] <= self.now + 0.3:
            self.fire(entry)
            entry = self.first()

    def until(self, target):
        while target[1] < len(target[2]):
            self.fire(self.first())

    def drain(self):
        entry = self.first()
        while entry is not None:
            self.fire(entry)
            entry = self.first()


QKV_CUTS = ((0, 256), (256, 128), (384, 128), (512, 256))


def forward_kernel(dims, x_hbm, cot_hbm, pos_ref, count_ref, freq_ref, qkv_ref, out_ref, gate_up_ref, down_ref, norm_ref,
                   *rest):
    outs, scratch = rest[:25], rest[25:]
    (o_q0, o_q1, o_q2, o_q3, o_wo, o_wgu, o_wd, o_scale, o_normed, o_raw, o_query, o_key, o_value, o_attn, o_cos, o_sin,
     o_ffn_in, o_mid, o_proj, o_hidden, o_gate, o_up, o_ddown, o_out, o_sgrad) = outs
    (q0, q1, q2, q3, wo, wgu, wd, scale, normed, raw, query, key, value, attn_t, cosine, sine,
     ffn_in_t, mid, proj, hidden, gate, up, ddown, out, sgrad,
     x_ref, cot_ref, attn, ffn_in, low, down, norm_all, norm_rows, qkv_got, gate_up_got, pair,
     send_sems, recv_sems, in_sems, out_sems) = scratch
    place = my_place(dims)
    z, y, x, core = place
    count = dims[0] * 8
    tokens = x_ref.shape[0]
    tiles = tokens // ROWS
    loads = [pltpu.make_async_copy(x_hbm, x_ref, in_sems.at[0]), pltpu.make_async_copy(cot_hbm, cot_ref, in_sems.at[1])]
    for load in loads:
        load.start()
    enter(dims, place)
    stores = []

    out_slots = iter(range(48))

    def put(index, part=None):
        src, dst = scratch[index], outs[index]
        if part is not None:
            src, dst = src.at[part], dst.at[part]
        store = pltpu.make_async_copy(src, dst, out_sems.at[next(out_slots)])
        store.start()
        stores.append(store)

    link = Link(dims, place, send_sems, recv_sems, 0)
    for slot, (ref, got) in enumerate(((qkv_ref, qkv_got), (gate_up_ref, gate_up_got))):
        half = got.shape[1]
        other = pl.multiple_of((1 - core) * half, 128)
        link.send(ref.at[:, pl.ds(other, half)], got, link.core_peer(), slot)
    norm_all[z, y, x, core] = jnp.zeros(norm_all.shape[4:], F32)
    norm_all[z, y, x, core, 0:1, 0 : norm_ref.shape[1]] = norm_ref[...].astype(BF16).astype(F32)

    def pair_up(ref, got, slot):
        rows, half = got.shape
        link.copy(got, got, link.core_peer(), slot).wait_recv()
        mine = ref[:, pl.ds(pl.multiple_of(core * half, 128), half)]
        other = got[...]
        first = core == 0
        pair[0:rows, 0:half] = jnp.where(first, mine, other)
        pair[rows : 2 * rows, 0:half] = jnp.where(first, other, mine)

    step = dims[0] + 5
    bases = iter(range(2, 2 + 17 * step, step))

    def item(views):
        return [Gather(dims, place, view, swap == 1, send_sems, recv_sems, next(bases)) for swap, view in enumerate(views)]

    def block(ref, *lead):
        return lambda z, y, x, core: ref.at[(*lead, core, z, y, x)]

    def rows_of(ref, part):
        return lambda z, y, x, core: ref.at[z, y, x, core, part]

    pump = Pump()
    links = [link]

    def gather(parts, sizes):
        links.extend(parts)
        ways = [("x", "y") if not part.swap else ("y", "x") for part in parts]

        def run_near():
            for part in parts:
                part.wait(0)
                part.start(1)

        def run_far():
            for part in parts:
                part.wait(1)
                part.start(2)
                part.start(3)

        def run_core():
            for part in parts:
                part.wait(2)
                part.start(4)

        def run_last():
            for part in parts:
                part.wait(3)
                part.wait(4)

        for part in parts:
            part.start(0)
        near = [(way[0], 4 * size) for way, size in zip(ways, sizes)]
        far = [(way[1], 8 * size) for way, size in zip(ways, sizes)]
        core_flows = [("core", 8 * size) for size in sizes]
        return pump.add(
            [("z", 4 * size) for size in sizes],
            [(run_near, near), (run_far, far + core_flows), (run_core, core_flows), (run_last, [])],
        )

    wo[z, y, x, core] = out_ref[...].astype(BF16).reshape(wo.shape[4:])
    out_entry = gather(item((rows_of(wo, 0), rows_of(wo, 1))), [wo.shape[5] * D * 2] * 2)
    pair_up(qkv_ref, qkv_got, 0)
    for ref, (start, width) in zip((q0, q1, q2, q3), QKV_CUTS):
        ref[core, z, y, x] = pair[:, start : start + width].astype(BF16)
    pump.work(1.5)
    pair_bytes = pair.shape[0] * 2
    sizes = [pair_bytes * width for _, width in QKV_CUTS]
    norm_entry = gather(item((lambda z, y, x, core: norm_all.at[z, y, x, core],)), [4096])
    q_entries = [gather(item((block(q0), block(q1))), sizes[:2]), gather(item((block(q2), block(q3))), sizes[2:])]
    wd[z, y, x, core] = down_ref[...].astype(BF16).reshape(wd.shape[4:])
    down_entry = gather(item((rows_of(wd, 0), rows_of(wd, 1))), [wd.shape[5] * D * 2] * 2)
    pair_up(gate_up_ref, gate_up_got, 1)
    quarters = wgu.shape[0]
    cut = wgu.shape[-1]
    wide_entries = []
    for quarter in range(quarters):
        for colour in range(2):
            start = (2 * quarter + colour) * cut
            wgu[quarter, colour, core, z, y, x] = pair[:, start : start + cut].astype(BF16)
        wide_entries.append(gather(item((block(wgu, quarter, 0), block(wgu, quarter, 1))), [pair_bytes * cut] * 2))
    pump.work(1.0)
    live_tiles = count_ref[0]
    def table_tile(tile, carry):
        span = pl.ds(pl.multiple_of(tile * 128, 128), 128)
        position = column_of(pos_ref[pl.ds(tile, 1), :].astype(F32))
        angle = position * freq_ref[...]
        cosine[span] = jnp.cos(angle)
        sine[span] = jnp.sin(angle)
        row = lax.broadcasted_iota(jnp.int32, (128, 128), 0) + tile * 128
        low[span] = row - jnp.where(tile < live_tiles, jnp.minimum(position.astype(jnp.int32), WIN - 1), 0)
        return carry

    for begin in range(0, tokens // 128, 4):
        lax.fori_loop(begin, begin + 4, table_tile, 0)
        pump.work(1.2)
    put(14)
    put(15)
    for load in loads:
        load.wait()
    pump.until(norm_entry)
    spread_scales(norm_all, norm_rows, scale, norm_ref.shape[1], count)
    put(7)
    pump.work(1.0)
    for entry in q_entries:
        pump.until(entry)
    for index in range(4):
        put(index)

    def scales(which):
        start = (0, D, 2 * D, 3 * D, 4 * D, 4 * D + HD)[which]
        return 1.0 + scale[:, start : start + (D if which < 4 else HD)]

    def weight(ref, c):
        return ref[c].reshape(-1, ref.shape[-1])

    def project(tile, carry):
        rows = pl.ds(pl.multiple_of(tile * ROWS, ROWS), ROWS)
        normal, _ = unit(x_ref[rows].astype(F32))
        inner = (normal * scales(0)).astype(BF16)
        normed[:, rows] = inner.T
        parts = []
        for c in range(2):
            parts.append(dot(inner, weight(q0, c)))
            parts.append(dot(inner, jnp.concatenate([weight(q1, c), weight(q2, c)], axis=1)))
            parts.append(dot(inner, weight(q3, c)))
        for head in range(HQ + 2):
            part = parts[head]
            if head == HQ + 1:
                value[rows] = part.astype(BF16)
                continue
            raw[rows, head * HD : (head + 1) * HD] = part.astype(BF16)
            normal, _ = unit(part)
            turned = turn_pairs(normal * scales(5 if head == HQ else 4), cosine[rows], sine[rows], 1).astype(BF16)
            if head == HQ:
                key[rows] = turned
            else:
                query[rows, head * HD : (head + 1) * HD] = turned
        return carry

    def attend(tile):
        start = tile * ROWS
        rows = slice(start, start + ROWS)
        first = max(0, start - WIN)
        keys = slice(first, start + ROWS)
        lane = lax.broadcasted_iota(jnp.int32, (ROWS, 128), 1)
        row = lax.broadcasted_iota(jnp.int32, (ROWS, 128), 0) + start
        least = low[rows]
        for head in range(HQ):
            span = slice(head * HD, (head + 1) * HD)
            scores = dot_nt(query[rows, span], key[keys])
            parts, total = [], None
            for at in range(first, start + ROWS, 128):
                column = lane + at
                allowed = column >= least
                if at >= start:
                    allowed = allowed & (column <= row)
                part = jnp.where(allowed, jnp.exp2(scores[:, at - first : at - first + 128] * (LOG2E / HD**0.5)), 0.0)
                parts.append(part)
                total = part if total is None else total + part
            inverse = 1.0 / jnp.sum(total, axis=1, keepdims=True)
            probs = jnp.concatenate([(part * inverse).astype(BF16) for part in parts], axis=1)
            attn[rows, span] = dot(probs, value[keys]).astype(BF16)
            attn_t[span, rows] = attn[rows, span].T

    def mix(tile, carry):
        rows = pl.ds(pl.multiple_of(tile * ROWS, ROWS), ROWS)
        projected = dot(attn[rows], wo[...].reshape(-1, D))
        proj[rows] = projected
        normal, _ = unit(projected)
        middle = x_ref[rows].astype(F32) + normal * scales(1)
        mid[rows] = middle
        normal, _ = unit(middle)
        inner = (normal * scales(2)).astype(BF16)
        ffn_in[rows] = inner
        ffn_in_t[:, rows] = inner.T
        return carry

    for begin in range(0, tiles, 2):
        lax.fori_loop(begin, begin + 2, project, 0)
        pump.work(2.6)
    for index in (8, 9, 10, 11, 12):
        put(index)
    for tile in range(tiles):
        attend(tile)
        pump.work(0.5 * min(tile + 1, 3))
    put(13)
    pump.until(out_entry)
    put(4)
    for begin in range(0, tiles, 2):
        lax.fori_loop(begin, begin + 2, mix, 0)
        pump.work(1.8)
    for index in (16, 17, 18):
        put(index)
    pump.until(down_entry)
    put(6)
    wide = 2 * cut
    for quarter in range(quarters):
        pump.until(wide_entries[quarter])

        def feed(tile, carry):
            rows = pl.ds(pl.multiple_of(tile * ROWS, ROWS), ROWS)
            inner = ffn_in[rows]
            total = None
            for colour in range(2):
                at = colour * cut
                gated = dot(inner, weight(wgu.at[quarter, colour], 0))
                upper = dot(inner, weight(wgu.at[quarter, colour], 1))
                square = gated * gated
                bend = jnp.tanh(0.7978845608028654 * (gated + 0.044715 * square * gated))
                half = 0.5 * (1.0 + bend)
                active = gated * half
                slope = half + 0.5 * gated * (1.0 - bend * bend) * (0.7978845608028654 * (1.0 + 0.134145 * square))
                gate[quarter, rows, at : at + cut] = (slope * upper).astype(BF16)
                up[quarter, rows, at : at + cut] = active.astype(BF16)
                inside = (active * upper).astype(BF16)
                first = quarter * wide + at
                hidden[first : first + cut, rows] = inside.T
                part = wd.reshape(FF, D)[first : first + cut, :]
                part = dot(inside, part)
                total = part if total is None else total + part
            if quarter == 0:
                down[rows] = total
            else:
                down[rows] = down[rows] + total
            return carry

        lax.fori_loop(0, tiles, feed, 0)
        pump.work(3.8)
        for index in (5, 20, 21):
            put(index, quarter)
        put(19, pl.ds(quarter * wide, wide))
    sgrad[...] = jnp.zeros_like(sgrad)

    def finish(tile, carry):
        start = pl.multiple_of(tile * ROWS, ROWS)
        rows = pl.ds(start, ROWS)
        normal, factor = unit(down[rows])
        out[rows] = (mid[rows] + normal * scales(3)).astype(BF16)
        row = start + lax.broadcasted_iota(jnp.int32, (ROWS, 1), 0)
        grad = jnp.where(row < live_tiles * TILE, cot_ref[rows].astype(F32), 0.0)
        sgrad[...] += fold(grad * normal)
        ddown[rows] = unit_back(grad * scales(3), normal, factor).astype(BF16)
        return carry

    lax.fori_loop(0, tiles, finish, 0)
    for index in (22, 23, 24):
        put(index)
    pump.drain()
    for each in links:
        each.finish()
    for store in stores:
        store.wait()


def forward_call(dims, block_input, out_cotangent, positions, tile_count, qkv_weight, out_weight, gate_up_weight,
                 down_weight, norm_scales):
    grid = dims[:3]
    tokens = block_input.shape[0]
    rows = qkv_weight.shape[0]
    width, wide = qkv_weight.shape[1], gate_up_weight.shape[1]
    shapes = [((2,) + grid + (2 * rows, cut), BF16) for _, cut in QKV_CUTS] + [
        (grid + (2, 2, out_weight.shape[0] // 2, D), BF16),
        ((4, 2, 2) + grid + (2 * rows, FF // 8), BF16),
        (grid + (2, 2, down_weight.shape[0] // 2, D), BF16),
        ((1, norm_scales.shape[0] * dims[0] * 8), F32),
        ((D, tokens), BF16),
        ((tokens, (HQ + 1) * HD), BF16),
        ((tokens, HQ * HD), BF16),
        ((tokens, HD), BF16),
        ((tokens, HD), BF16),
        ((HQ * HD, tokens), BF16),
        ((tokens, HD // 2), F32),
        ((tokens, HD // 2), F32),
        ((D, tokens), BF16),
        ((tokens, D), F32),
        ((tokens, D), F32),
        ((FF, tokens), BF16),
        ((4, tokens, FF // 4), BF16),
        ((4, tokens, FF // 4), BF16),
        ((tokens, D), BF16),
        ((tokens, D), BF16),
        ((8, D), F32),
    ]
    sems = 2 + 17 * (dims[0] + 5)
    scratch = [pltpu.VMEM(*shape) for shape in shapes] + [
        pltpu.VMEM((tokens, D), BF16),
        pltpu.VMEM((tokens, D), BF16),
        pltpu.VMEM((tokens, HQ * HD), BF16),
        pltpu.VMEM((tokens, D), BF16),
        pltpu.VMEM((tokens, 128), jnp.int32),
        pltpu.VMEM((tokens, D), F32),
        pltpu.VMEM(grid + (2, 8, 128), F32),
        pltpu.VMEM((dims[0] * 8, 128), F32),
        pltpu.VMEM((rows, width // 2), F32),
        pltpu.VMEM((rows, wide // 2), F32),
        pltpu.VMEM((2 * rows, wide // 2), F32),
        pltpu.SemaphoreType.DMA((sems,)),
        pltpu.SemaphoreType.DMA((sems,)),
        pltpu.SemaphoreType.DMA((2,)),
        pltpu.SemaphoreType.DMA((48,)),
    ]
    vmem = pl.BlockSpec(memory_space=pltpu.VMEM)
    hbm = pl.BlockSpec(memory_space=pltpu.HBM)
    frequency = np.power(rope_base, -np.arange(HD // 2) * (2.0 / HD)).astype(np.float32)[None, :]
    return pl.pallas_call(
        functools.partial(forward_kernel, dims),
        out_shape=[jax.ShapeDtypeStruct(*shape) for shape in shapes],
        in_specs=[hbm, hbm, vmem, pl.BlockSpec(memory_space=pltpu.SMEM)] + [vmem] * 6,
        out_specs=[hbm] * len(shapes),
        scratch_shapes=scratch,
        compiler_params=pltpu.CompilerParams(collective_id=0, has_side_effects=True, vmem_limit_bytes=63 << 20),
        name="forward",
    )(block_input, out_cotangent, positions.reshape(-1, 128), tile_count, frequency, qkv_weight, out_weight,
      gate_up_weight, down_weight, norm_scales[None, :])


def backward_kernel(dims, *refs):
    (h_q0, h_q1, h_q2, h_q3, h_wo, h_wgu, h_wd, scale, h_normed, h_raw, h_query, h_key, h_value, h_attn, h_cos, h_sin,
     h_ffn_in, h_mid, h_proj, h_hidden, h_gate, h_up, h_ddown, sgrad_out, h_x, h_cot, pos_ref, count_ref) = refs[:28]
    o_input, o_qkv, o_wo, o_wgu, o_wd, o_norm = refs[28:34]
    (wo, wgu, wd, gq0, gq1, gq2, gq3, go, gg, gd, gn,
     pool, dgu, ddown, ffn_in, attn, dproj, dmid, proj, sine, totals, grow, gtab, bounce, swaps, halves,
     in_sems, out_sem, send_sems, recv_sems) = refs[34:64]
    buffers = list(refs[64:])
    place = my_place(dims)
    z, y, x, core = place
    count = dims[0] * 8
    tokens = dmid.shape[0]
    tiles = tokens // ROWS
    cut = wgu.shape[-1]
    serial = iter(range(64))

    def load(src, dst):
        copy = pltpu.make_async_copy(src, dst, in_sems.at[next(serial)])
        copy.start()
        return copy

    c_ddown = load(h_ddown, ddown)
    c_hidden = [load(h_hidden.at[pl.ds(512 * j, 512)], pool.at[pl.ds(512 * j, 512)]) for j in range(4)]
    c_wd = load(h_wd, wd)
    c_gate = []
    for j in range(4):
        c_gate.append((load(h_gate.at[j], dgu.at[0, j]), load(h_up.at[j], dgu.at[1, j])))
    c_ffn_in = load(h_ffn_in, ffn_in)
    c_wgu = load(h_wgu, wgu)
    c_p3 = [load(h_mid, dmid), load(h_proj, proj), load(h_attn, attn), load(h_wo, wo)]
    enter(dims, place)

    pump = Pump()
    step = dims[0] + 5
    bases = iter(range(12, 12 + 19 * step, step))
    links = []

    def scatter(givens, done):
        parts = []
        for swap, given in enumerate(givens):
            held, near, far, last = buffers[:4]
            del buffers[:4]
            parts.append(Scatter(dims, place, given, held, near, far, last, swap == 1, send_sems, recv_sems, next(bases)))
        links.extend(parts)

        def stage(which):
            def run():
                for part in parts:
                    part.wait(which)
                    part.start(which + 1)

            return run

        def last_stage():
            for colour, part in enumerate(parts):
                done(colour, part.wait(3))

        for part in parts:
            part.start(0)
        sizes = [math.prod(part.last.shape[1:]) * part.last.dtype.itemsize for part in parts]
        ways = [("x", "y") if part.swap else ("y", "x") for part in parts]
        near = [(way[0], 8 * size) for way, size in zip(ways, sizes)]
        far = [(way[1], 4 * size) for way, size in zip(ways, sizes)]
        pump.add(
            [("core", 16 * size) for size in sizes],
            [(stage(0), near), (stage(1), far), (stage(2), [("z", 4 * size) for size in sizes]), (last_stage, [])],
        )

    swap_link = Link(dims, place, send_sems, recv_sems, 0)
    links.append(swap_link)
    fetched = []

    def split_rows(slot, target, start):
        def done(colour, total):
            at = slot + colour
            rows, width = target.shape[0], total.shape[1]
            first = start[colour]
            half = target.shape[1] // 2
            bounce[at % 2, :, 0:width] = total
            low, high = bounce[at % 2, 0:rows, 0:width], bounce[at % 2, rows : 2 * rows, 0:width]
            target[:, pl.ds(pl.multiple_of(core * half + first, 128), width)] = jnp.where(core == 0, low, high)
            swaps[at, :, 0:width] = jnp.where(core == 0, high, low)
            span = (at, slice(None), pl.ds(0, width))
            swap_link.send(swaps.at[span], halves.at[span], swap_link.core_peer(), at)

            def fetch():
                swap_link.copy(halves.at[span], halves.at[span], swap_link.core_peer(), at).wait_recv()
                target[:, pl.ds(pl.multiple_of((1 - core) * half + first, 128), width)] = halves[at, :, 0:width]

            fetched.append(fetch)

        return done

    def rows_done(target, start):
        def done(colour, total):
            height = total.shape[0]
            first = start + colour * height
            target[first : first + height, :] = total

        return done

    def scales(which):
        start = (0, D, 2 * D, 3 * D, 4 * D, 4 * D + HD)[which]
        return 1.0 + scale[:, start : start + (D if which < 4 else HD)]

    def weight(ref, c):
        return ref[c].reshape(-1, ref.shape[-1])

    def some_rows(tile):
        return pl.ds(pl.multiple_of(tile * ROWS, ROWS), ROWS)

    c_ddown.wait()
    grown = gd.reshape(FF, D)
    for copy in c_hidden:
        copy.wait()

    def down_part(part, carry):
        rows = pl.ds(pl.multiple_of(part * 512, 512), 512)
        grown[rows, :] = dot(pool[rows, :], ddown[...]).astype(BF16)
        return carry

    lax.fori_loop(0, FF // 512, down_part, 0)
    for sub in range(2):
        scatter([(lambda core, k=2 * sub + k: gd.at[:, :, :, core, k]) for k in range(2)],
                rows_done(o_wd, sub * 2 * gd.shape[5]))
    queries, others = pool.at[pl.ds(0, tokens)], pool.at[pl.ds(tokens, tokens)]
    c_query = [load(h_query, queries), load(h_key, others.at[:, pl.ds(0, HD)]), load(h_value, others.at[:, pl.ds(HD, HD)])]
    c_wd.wait()
    c_ffn_in.wait()
    down_rows = wd.reshape(FF, D)
    for quarter in range(4):
        for copy in c_gate[quarter]:
            copy.wait()
        last_rows = slice(quarter * 512, (quarter + 1) * 512)

        def spread(tile, carry, quarter=quarter, last_rows=last_rows):
            rows = some_rows(tile)
            grad = dot_nt(ddown[rows], down_rows[last_rows, :])
            dgu[0, quarter, rows] = (grad * dgu[0, quarter, rows].astype(F32)).astype(BF16)
            dgu[1, quarter, rows] = (grad * dgu[1, quarter, rows].astype(F32)).astype(BF16)
            return carry

        lax.fori_loop(0, tiles, spread, 0)
        pump.work(1.2)

        def wide_part(c, carry, quarter=quarter):
            for colour in range(2):
                span = slice(colour * cut, (colour + 1) * cut)
                gg[quarter, colour, c] = dot(ffn_in[...], dgu[c, quarter, :, span]).astype(BF16).reshape(gg.shape[3:])
            return carry

        lax.fori_loop(0, 2, wide_part, 0)
        pump.work(1.8)
        scatter([(lambda core, q=quarter, k=k: gg.at[q, k, core]) for k in range(2)],
                split_rows(2 * quarter, o_wgu, [(2 * quarter + k) * cut for k in range(2)]))
        pump.work(0.1)
    xc = ddown
    c_p3.append(load(h_cot, xc))
    c_normed = load(h_normed, ffn_in)
    c_wgu.wait()
    for copy in c_p3:
        copy.wait()
    names = ("in", "post", "ffn", "out", "query", "key")
    sums = dict(zip(names, (slice(8 * index, 8 * index + 8) for index in range(6))))
    totals[...] = jnp.zeros_like(totals)

    def collect(which, values):
        totals[sums[which], 0 : values.shape[1]] += fold(values)

    def middle_tile(tile, carry):
        rows = some_rows(tile)
        grad = None
        for quarter in range(4):
            for c in range(2):
                part = jnp.concatenate([weight(wgu.at[quarter, colour], c) for colour in range(2)], axis=1)
                part = dot_nt(dgu[c, quarter, rows], part)
                grad = part if grad is None else grad + part
        row = tile * ROWS + lax.broadcasted_iota(jnp.int32, (ROWS, 1), 0)
        given = jnp.where(row < count_ref[0] * TILE, xc[rows].astype(F32), 0.0)
        normal, factor = unit(dmid[rows])
        collect("ffn", grad * normal)
        middle = given + unit_back(grad * scales(2), normal, factor)
        dmid[rows] = middle
        normal, factor = unit(proj[rows])
        collect("post", middle * normal)
        dproj[rows] = unit_back(middle * scales(1), normal, factor).astype(BF16)
        return carry

    for begin in range(0, tiles, 2):
        lax.fori_loop(begin, begin + 2, middle_tile, 0)
        pump.work(4.4)
    c_raw = [load(h_raw.at[:, pl.ds(0, 512)], dgu.at[0, 0]), load(h_raw.at[:, pl.ds(512, 512)], dgu.at[0, 1]),
             load(h_raw.at[:, pl.ds(1024, HD)], dgu.at[0, 2, :, pl.ds(0, HD)])]
    cosine = proj.at[:, pl.ds(2 * HD, HD // 2)]
    c_rest = [load(h_cos, cosine), load(h_sin, sine), load(h_x, xc)]
    wq = wd.reshape(FF, D)
    c_qkv = []
    for c in range(2):
        for ref, within, lane in ((h_q0, 0, 0), (h_q1, 1, 0), (h_q2, 1, 128), (h_q3, 2, 0)):
            head = 3 * c + within
            at = pl.ds(head % 2 * HD + lane, ref.shape[-1])
            c_qkv.append(load(ref.at[c], wq.at[pl.ds(head // 2 * D, D), at]))
    grown_out = go.reshape(HQ * HD, D)
    for half in range(2):
        rows = slice(half * 512, (half + 1) * 512)
        grown_out[rows, :] = dot(attn[rows, :], dproj[...]).astype(BF16)
    scatter([(lambda core, k=k: go.at[:, :, :, core, k]) for k in range(2)], rows_done(o_wo, 0))
    out_rows = wo.reshape(HQ * HD, D)
    pump.work(1.9)

    def attn_grad(tile, carry):
        rows = some_rows(tile)
        attn[rows] = dot_nt(dproj[rows], out_rows[...]).astype(BF16)
        return carry

    lax.fori_loop(0, tiles, attn_grad, 0)
    pump.work(1.9)
    for copy in c_query + c_raw + c_rest:
        copy.wait()
    dkey, dvalue = proj.at[:, pl.ds(0, HD)], proj.at[:, pl.ds(HD, HD)]

    for tile in range(tiles):
        start = tile * ROWS
        rows = slice(start, start + ROWS)
        first = max(0, start - WIN)
        keys = slice(first, start + ROWS)
        height = start + ROWS - first
        position = jnp.concatenate([pos_ref[2 * tile : 2 * tile + 1, :], pos_ref[2 * tile + 1 : 2 * tile + 2, :]], axis=1)
        row = lax.broadcasted_iota(jnp.int32, (1, ROWS), 1) + start
        reach = jnp.where(row < count_ref[0] * TILE, jnp.minimum(position, WIN - 1), 0)
        column = lax.broadcasted_iota(jnp.int32, (height, ROWS), 0) + first
        allowed = (column >= row - reach) & (column <= row)
        dvalue[rows, :] = jnp.zeros((ROWS, HD), F32)
        dkey[rows, :] = jnp.zeros((ROWS, HD), F32)

        def two_heads(pair, carry, rows=rows, keys=keys, allowed=allowed):
            key, value = others[keys, 0:HD], others[keys, HD : 2 * HD]
            probs_all, scores_all, query_all, grads_all = [], [], [], []
            for each in range(2):
                span = pl.ds(pl.multiple_of((2 * pair + each) * HD, HD), HD)
                query = queries[rows, span]
                grad = attn[rows, span]
                weights = jnp.where(allowed, jnp.exp2(dot_nt(key, query) * (LOG2E / HD**0.5)), 0.0)
                probs = weights * (1.0 / jnp.sum(weights, axis=0, keepdims=True))
                grad_probs = dot_nt(value, grad)
                both = probs * grad_probs
                delta = jnp.sum(both, axis=0, keepdims=True)
                scores = ((both - probs * delta) * HD**-0.5).astype(BF16)
                probs_all.append(probs.astype(BF16))
                scores_all.append(scores)
                query_all.append(query)
                grads_all.append(grad)
            dvalue[keys, :] += dot(jnp.concatenate(probs_all, axis=1), jnp.concatenate(grads_all, axis=0))
            dkey[keys, :] += dot(jnp.concatenate(scores_all, axis=1), jnp.concatenate(query_all, axis=0))
            for each in range(2):
                span = pl.ds(pl.multiple_of((2 * pair + each) * HD, HD), HD)
                grad = turn_pairs(dot_tn(scores_all[each], key), cosine[rows, :], sine[rows, :], -1)
                normal, factor = unit(dgu[0, pair, rows, each * HD : (each + 1) * HD].astype(F32))
                collect("query", grad * normal)
                queries[rows, span] = unit_back(grad * scales(4), normal, factor).astype(BF16)
            return carry

        lax.fori_loop(0, HQ // 2, two_heads, 0)
        pump.work((1.3, 2.3, 3.3, 3.3)[min(tile, 3)])

    def key_tile(tile, carry):
        rows = some_rows(tile)
        grad = turn_pairs(dkey[rows, :], cosine[rows, :], sine[rows, :], -1)
        normal, factor = unit(dgu[0, 2, rows, 0:HD].astype(F32))
        collect("key", grad * normal)
        others[rows, 2 * HD : 3 * HD] = unit_back(grad * scales(5), normal, factor).astype(BF16)
        others[rows, 3 * HD : 4 * HD] = dvalue[rows, :].astype(BF16)
        return carry

    lax.fori_loop(0, tiles, key_tile, 0)
    pump.work(1.0)
    c_normed.wait()

    def grad_columns(rows, head):
        ref, at = (queries, head * HD) if head < HQ else (others, (head - HQ + 2) * HD)
        return ref[rows, at : at + HD]

    for head in range(HQ + 2):
        term = dot(ffn_in[...], grad_columns(slice(0, tokens), head)).astype(BF16)
        c, within = head // 3, head % 3
        if within == 0:
            gq0[c] = term.reshape(gq0.shape[1:])
        elif within == 2:
            gq3[c] = term.reshape(gq3.shape[1:])
        else:
            gq1[c] = term[:, 0:128].reshape(gq1.shape[1:])
            gq2[c] = term[:, 128:256].reshape(gq2.shape[1:])
    for sub, pair in enumerate(((gq0, gq1), (gq2, gq3))):
        scatter([(lambda core, ref=ref: ref.at[core]) for ref in pair],
                split_rows(8 + 2 * sub, o_qkv, [QKV_CUTS[2 * sub + k][0] for k in range(2)]))
    pump.work(2.8)
    for copy in c_qkv:
        copy.wait()

    def input_tile(tile, carry):
        rows = some_rows(tile)
        grad = None
        for head in range(HQ + 2):
            part = wq[head // 2 * D : (head // 2 + 1) * D, head % 2 * HD : (head % 2 + 1) * HD]
            part = dot_nt(grad_columns(rows, head), part)
            grad = part if grad is None else grad + part
        normal, factor = unit(xc[rows].astype(F32))
        collect("in", grad * normal)
        dmid[rows] = dmid[rows] + unit_back(grad * scales(0), normal, factor)
        return carry

    lax.fori_loop(0, tiles, input_tile, 0)
    pump.work(4.4)
    store = pltpu.make_async_copy(dmid, o_input, out_sem)
    store.start()
    totals[sums["out"]] = sgrad_out[...]
    at = 0
    for index, name in enumerate(names):
        size = D if index < 4 else HD
        grow[:, at : at + size] = jnp.sum(totals[sums[name], 0:size], axis=0, keepdims=True)
        at += size
    per = at // count

    def chunk_part(index, table):
        begin = pl.multiple_of(index * 512, 512)
        owner, entry = chunk_masks(per, begin, 512)
        picked = entry.astype(F32).astype(BF16)
        rest = jnp.where(owner(count), grow[:, pl.ds(begin, 512)], 0.0)
        for _ in range(3):
            piece = rest.astype(BF16)
            rest = rest - piece.astype(F32)
            table = table + dot_nt(piece, picked)
        return table

    gtab[...] = lax.fori_loop(0, at // 512, chunk_part, jnp.zeros((count, 128), F32))
    flat = gn.reshape(count, 8, 128)
    for device in range(count):
        flat[device] = jnp.broadcast_to(gtab[device : device + 1, :], (8, 128))

    def norm_done(colour, total):
        o_norm[...] = total

    scatter([lambda core: gn.at[:, :, :, core]], norm_done)
    pump.drain()
    for fetch in fetched:
        fetch()
    for link in links:
        link.finish()
    store.wait()


def backward_call(dims, saved, block_input, out_cotangent, positions, tile_count, shard_rows):
    grid = dims[:3]
    count = dims[0] * 8
    tokens = block_input.shape[0]
    qkv_rows, out_rows, down_rows, norm_rows = shard_rows
    width = (HQ + 2) * HD
    bf = lambda *shape: pltpu.VMEM(shape, BF16)
    fp = lambda *shape: pltpu.VMEM(shape, F32)
    pair = 2 * qkv_rows
    weights = [bf(*((2,) + grid + (pair, cut))) for _, cut in QKV_CUTS] + [
        bf(*(grid + (2, 2, out_rows // 2, D))),
        bf(*((4, 2, 2) + grid + (pair, FF // 8))),
        bf(*(grid + (2, 2, down_rows // 2, D))),
    ]
    scratch = weights[4:] + weights[:6] + [
        bf(*(grid + (2, 4, down_rows // 4, D))),
        fp(*(grid + (2, 8, 128))),
        bf(FF, tokens),
        bf(2, 4, tokens, FF // 4),
        bf(tokens, D),
        bf(D, tokens),
        bf(HQ * HD, tokens),
        bf(tokens, D),
        fp(tokens, D),
        fp(tokens, D),
        fp(tokens, HD // 2),
        fp(48, D),
        fp(1, 4 * D + 2 * HD),
        fp(count, 128),
        fp(2, pair, 256),
        fp(12, qkv_rows, 256),
        fp(12, qkv_rows, 256),
        pltpu.SemaphoreType.DMA((64,)),
        pltpu.SemaphoreType.DMA,
    ]
    sems = 12 + 19 * (dims[0] + 5)
    scratch += [pltpu.SemaphoreType.DMA((sems,)), pltpu.SemaphoreType.DMA((sems,))]
    blocks = [[(down_rows // 4, D)] * 2] * 2 + [[(pair, FF // 8)] * 2] * 4 + [[(out_rows // 2, D)] * 2]
    blocks += [[(pair, QKV_CUTS[0][1]), (pair, QKV_CUTS[1][1])], [(pair, QKV_CUTS[2][1]), (pair, QKV_CUTS[3][1])], [(8, 128)]]
    for colours in blocks:
        for swap, block in enumerate(colours):
            make = fp if block == (8, 128) else bf
            scratch.append(make(*(grid + block)))
            scratch.append(make(*(((grid[0], grid[1]) if swap else (grid[0], grid[2])) + block)))
            scratch.append(make(*((grid[0],) + block)))
            scratch.append(make(*((grid[0] - 1,) + block)))
    vmem = pl.BlockSpec(memory_space=pltpu.VMEM)
    hbm = pl.BlockSpec(memory_space=pltpu.HBM)
    outs = [(tokens, D), (qkv_rows, width), (out_rows, D), (qkv_rows, 2 * FF), (down_rows, D), (8, 128)]
    saved = list(saved)
    saved[:4] = [array.reshape(2, D, -1) for array in saved[:4]]
    inputs = saved[:23] + [saved[24], block_input, out_cotangent, positions.reshape(-1, 128), tile_count]
    specs = [hbm] * 28
    specs[7] = specs[23] = specs[26] = vmem
    specs[27] = pl.BlockSpec(memory_space=pltpu.SMEM)
    return pl.pallas_call(
        functools.partial(backward_kernel, dims),
        out_shape=[jax.ShapeDtypeStruct(shape, F32) for shape in outs],
        in_specs=specs,
        out_specs=[hbm] + [vmem] * 5,
        scratch_shapes=scratch,
        compiler_params=pltpu.CompilerParams(collective_id=1, has_side_effects=True, vmem_limit_bytes=67043328),
        name="backward",
    )(*inputs)


def adam_kernel(*refs):
    ins, outs, bufs = refs[:22], refs[22:44], refs[44:66]
    in_sems, out_sems = refs[66:]
    loads = [pltpu.make_async_copy(src, buf, in_sems.at[at]) for at, (src, buf) in enumerate(zip(ins, bufs))]
    stores = [pltpu.make_async_copy(buf, dst, out_sems.at[at]) for at, (buf, dst) in enumerate(zip(bufs, outs))]
    for load in loads:
        load.start()
    for item in range(5):
        span = range(4 * item, 4 * item + 4)
        for at in span:
            loads[at].wait()
        stores[4 * item].start()
        grad, weight, first, second = (bufs[at] for at in span)
        size = weight.shape[1]
        news = adam_update(weight[...], grad[0 : weight.shape[0], 0:size], first[...], second[...])
        for ref, new in zip((weight, first, second), news):
            ref[...] = new
        for at in span[1:]:
            stores[at].start()
    for at in (20, 21):
        loads[at].wait()
        stores[at].start()
    for store in stores:
        store.wait()


def adam_call(groups, passed):
    flat = [array if array.ndim == 2 else array[None, :] for group in groups for array in group] + list(passed)
    hbm = pl.BlockSpec(memory_space=pltpu.HBM)
    outs = pl.pallas_call(
        adam_kernel,
        out_shape=[jax.ShapeDtypeStruct(array.shape, array.dtype) for array in flat],
        in_specs=[hbm] * 22,
        out_specs=[hbm] * 22,
        scratch_shapes=[pltpu.VMEM(array.shape, array.dtype) for array in flat]
        + [pltpu.SemaphoreType.DMA((22,)), pltpu.SemaphoreType.DMA((22,))],
        compiler_params=pltpu.CompilerParams(vmem_limit_bytes=67043328),
        name="adam",
    )(*flat)
    results = []
    for item, group in enumerate(groups):
        shape = group[1].shape
        part = list(outs[4 * item : 4 * item + 4])
        if part[0].shape != part[1].shape:
            part[0] = part[0][0, : shape[0]]
        results.append([array.reshape(shape) for array in part])
    return results, outs[20:]


def plain_pass(
    block_input,
    out_cotangent,
    segment_ids,
    positions,
    tile_count,
    qkv_weight,
    out_weight,
    gate_up_weight,
    down_weight,
    norm_scales,
):
    qkv_full, out_full, gate_up_full, down_full, norm_full = (
        lax.all_gather(array.astype(jnp.bfloat16), "dp", axis=0, tiled=True)
        for array in (qkv_weight, out_weight, gate_up_weight, down_weight, norm_scales)
    )
    attn_full = (qkv_full, out_full, norm_full)
    ffn_full = (gate_up_full, down_full)
    row_count = block_input.shape[0]
    live_rows = jnp.arange(row_count, dtype=jnp.int32) // TILE < tile_count[0]
    block_output, attn_saved, ffn_saved = forward_pass(
        attn_full, ffn_full, block_input, segment_ids, positions, live_rows
    )
    attn_back, ffn_back = attn_full, ffn_full
    grad_out = out_cotangent.astype(jnp.float32) * live_rows[:, None].astype(jnp.float32)
    d_mid, gate_up_term, down_term, ffn_scale_grad, out_scale_grad = ffn_backward(
        ffn_back, attn_back[2].astype(jnp.float32), ffn_saved, grad_out
    )
    (
        input_grad,
        qkv_term,
        out_term,
        in_scale_grad,
        post_scale_grad,
        query_scale_grad,
        key_scale_grad,
    ) = attn_backward(attn_back, attn_saved, d_mid)
    norm_term = jnp.concatenate(
        [
            in_scale_grad,
            post_scale_grad,
            ffn_scale_grad,
            out_scale_grad,
            query_scale_grad,
            key_scale_grad,
        ]
    )
    sums = tuple(
        lax.psum_scatter(term, "dp", scatter_dimension=0, tiled=True)
        for term in (qkv_term, out_term, gate_up_term, down_term, norm_term)
    )
    return (block_output, input_grad) + sums


def shards(
    count,
    block_input,
    out_cotangent,
    segment_ids,
    positions,
    tile_count,
    qkv_weight,
    qkv_first,
    qkv_second,
    out_weight,
    out_first,
    out_second,
    gate_up_weight,
    gate_up_first,
    gate_up_second,
    down_weight,
    down_first,
    down_second,
    norm_scales,
    norm_first,
    norm_second,
):
    dims = grid_dims(count)
    if own_transfers(count, qkv_weight.shape[1], qkv_weight.shape[0]):
        saved = forward_call(
            dims, block_input, out_cotangent, positions, tile_count, qkv_weight, out_weight, gate_up_weight, down_weight,
            norm_scales,
        )
        block_output = saved[23]
        shard_rows = (qkv_weight.shape[0], out_weight.shape[0], down_weight.shape[0], norm_scales.shape[0])
        input_grad, qkv_grad, out_grad, gate_up_grad, down_grad, norm_grad = backward_call(
            dims, saved, block_input, out_cotangent, positions, tile_count, shard_rows
        )
    else:
        block_output, input_grad, qkv_grad, out_grad, gate_up_grad, down_grad, norm_grad = plain_pass(
            block_input, out_cotangent, segment_ids, positions, tile_count, qkv_weight, out_weight, gate_up_weight,
            down_weight, norm_scales,
        )
    (
        (
            (qkv_grad, qkv_new, qkv_first_new, qkv_second_new),
            (out_grad, out_new, out_first_new, out_second_new),
            (gate_up_grad, gate_up_new, gate_up_first_new, gate_up_second_new),
            (down_grad, down_new, down_first_new, down_second_new),
            (norm_grad, norms_new, norm_first_new, norm_second_new),
        ),
        (block_output, input_grad),
    ) = adam_call(
        (
            (qkv_grad, qkv_weight, qkv_first, qkv_second),
            (out_grad, out_weight, out_first, out_second),
            (gate_up_grad, gate_up_weight, gate_up_first, gate_up_second),
            (down_grad, down_weight, down_first, down_second),
            (norm_grad, norm_scales, norm_first, norm_second),
        ),
        (block_output, input_grad),
    )
    return (
        block_output,
        input_grad,
        qkv_grad,
        out_grad,
        gate_up_grad,
        down_grad,
        norm_grad,
        qkv_new,
        out_new,
        gate_up_new,
        down_new,
        norms_new,
        qkv_first_new,
        out_first_new,
        gate_up_first_new,
        down_first_new,
        norm_first_new,
        qkv_second_new,
        out_second_new,
        gate_up_second_new,
        down_second_new,
        norm_second_new,
    )


def solution(mesh):
    in_specs = (
        P("dp", None),
        P("dp", None),
        P("dp"),
        P("dp"),
        P("dp"),
        P("dp", None),
        P("dp", None),
        P("dp", None),
        P("dp", None),
        P("dp", None),
        P("dp", None),
        P("dp", None),
        P("dp", None),
        P("dp", None),
        P("dp", None),
        P("dp", None),
        P("dp", None),
        P("dp"),
        P("dp"),
        P("dp"),
    )
    out_specs = (
        P("dp", None),
        P("dp", None),
        P("dp", None),
        P("dp", None),
        P("dp", None),
        P("dp", None),
        P("dp"),
        P("dp", None),
        P("dp", None),
        P("dp", None),
        P("dp", None),
        P("dp"),
        P("dp", None),
        P("dp", None),
        P("dp", None),
        P("dp", None),
        P("dp"),
        P("dp", None),
        P("dp", None),
        P("dp", None),
        P("dp", None),
        P("dp"),
    )
    body = functools.partial(shards, mesh.shape["dp"])
    return jax.shard_map(body, mesh=mesh, in_specs=in_specs, out_specs=out_specs, check_vma=False)
```

```python
import functools
import math

import numpy as np

import jax
import jax.numpy as jnp
from jax import lax
from jax.experimental import pallas as pl
from jax.experimental.pallas import tpu as pltpu
from jax.sharding import PartitionSpec as P

D = 640
HQ = 4
HD = 256
FF = 2048
WIN = 512
TILE = 128


norm_eps = 1e-06
rope_base = 10000.0
beta_one = 0.9
beta_two = 0.999
adam_eps = 1e-08
learn_rate = 0.02
weight_decay = 0.1
adam_step = 3


def rms_scale(values, scales):
    mean_square = jnp.mean(values * values, axis=-1, keepdims=True)
    return values * lax.rsqrt(mean_square + norm_eps) * (1.0 + scales)


def gelu_tanh(values):
    inner_term = 0.7978845608028654 * (values + 0.044715 * values * values * values)
    return 0.5 * values * (1.0 + jnp.tanh(inner_term))


def gated_unit(gate_act, up_act):
    return gelu_tanh(gate_act) * up_act


def rotate(values, cosine, sine_table):
    half_dim = values.shape[-1] // 2
    front_half = values[..., :half_dim]
    back_half = values[..., half_dim:]
    return jnp.concatenate(
        [
            front_half * cosine - back_half * sine_table,
            back_half * cosine + front_half * sine_table,
        ],
        axis=-1,
    )


def rope_tables(positions, head_dim):
    exponent = jnp.arange(head_dim // 2, dtype=jnp.float32) * (2.0 / head_dim)
    frequency = jnp.power(jnp.float32(rope_base), -exponent)
    angles = positions.astype(jnp.float32)[:, None] * frequency[None, :]
    return (jnp.cos(angles)[:, None, :], jnp.sin(angles)[:, None, :])


def qk_prepare(query_raw, key_raw, q_scale, k_scale, cosine, sine_table):
    return (
        rotate(rms_scale(query_raw, q_scale), cosine, sine_table),
        rotate(rms_scale(key_raw, k_scale), cosine, sine_table),
    )


def contract(form, left, right):
    return jnp.einsum(form, left, right, preferred_element_type=jnp.float32)


def window_mask(block_index, window, segment_pad, live_pad):
    start_row = block_index * window
    query_rows = start_row + jnp.arange(window, dtype=jnp.int32)
    key_rows = start_row - window + jnp.arange(2 * window, dtype=jnp.int32)
    query_seg = segment_pad[start_row + window : start_row + 2 * window]
    key_seg = segment_pad[start_row : start_row + 2 * window]
    query_live = live_pad[start_row + window : start_row + 2 * window]
    key_live = live_pad[start_row : start_row + 2 * window]
    diagonal = key_rows[None, :] == query_rows[:, None]
    earlier = (key_rows[None, :] < query_rows[:, None]) & (
        query_rows[:, None] - key_rows[None, :] < window
    )
    same_seq = (query_seg[:, None] == key_seg[None, :]) & query_live[:, None] & key_live[None, :]
    return diagonal | earlier & same_seq


def front_pad(values, window):
    return jnp.concatenate([jnp.zeros((window,) + values.shape[1:], values.dtype), values], axis=0)


def attend_forward(query_bf, key_bf, value_bf, segment_pad, live_pad):
    row_count = query_bf.shape[0]
    score_scale = HD ** (-0.5)
    key_padded = front_pad(key_bf, WIN)
    value_padded = front_pad(value_bf, WIN)
    out_blocks = []
    log_blocks = []
    for block_index in range(row_count // WIN):
        start_row = block_index * WIN
        allowed = window_mask(block_index, WIN, segment_pad, live_pad)
        query_block = query_bf[start_row : start_row + WIN]
        key_block = key_padded[start_row : start_row + 2 * WIN]
        value_block = value_padded[start_row : start_row + 2 * WIN]
        scores = contract("qhd,kd->hqk", query_block, key_block) * score_scale
        exp_scores = jnp.where(allowed[None], jnp.exp(scores), 0.0)
        exp_total = jnp.sum(exp_scores, axis=-1)
        probs_bf = (exp_scores / exp_total[..., None]).astype(jnp.bfloat16)
        out_blocks.append(contract("hqk,kd->qhd", probs_bf, value_block).reshape(WIN, HQ * HD))
        log_blocks.append(jnp.log(exp_total))
    return (jnp.concatenate(out_blocks, axis=0), jnp.concatenate(log_blocks, axis=1))


def attend_backward(
    query_bf, key_bf, value_bf, attn_bf, dattn_bf, log_total, segment_pad, live_pad
):
    row_count = query_bf.shape[0]
    score_scale = HD ** (-0.5)
    key_padded = front_pad(key_bf, WIN)
    value_padded = front_pad(value_bf, WIN)
    attn_heads = attn_bf.reshape(row_count, HQ, HD)
    dattn_heads = dattn_bf.reshape(row_count, HQ, HD)
    delta_rows = jnp.sum(dattn_heads.astype(jnp.float32) * attn_heads.astype(jnp.float32), axis=-1)
    key_grad = jnp.zeros((row_count + WIN, HD), jnp.float32)
    value_grad = jnp.zeros((row_count + WIN, HD), jnp.float32)
    query_parts = []
    for block_index in range(row_count // WIN):
        start_row = block_index * WIN
        allowed = window_mask(block_index, WIN, segment_pad, live_pad)
        query_block = query_bf[start_row : start_row + WIN]
        key_block = key_padded[start_row : start_row + 2 * WIN]
        value_block = value_padded[start_row : start_row + 2 * WIN]
        dout_block = dattn_heads[start_row : start_row + WIN]
        scores = contract("qhd,kd->hqk", query_block, key_block) * score_scale
        probs = jnp.where(
            allowed[None], jnp.exp(scores - log_total[:, start_row : start_row + WIN, None]), 0.0
        )
        probs_bf = probs.astype(jnp.bfloat16)
        value_grad = value_grad.at[start_row : start_row + 2 * WIN].add(
            contract("hqk,qhd->kd", probs_bf, dout_block)
        )
        dprobs = contract("qhd,kd->hqk", dout_block, value_block)
        dscores = (
            probs * (dprobs - delta_rows[start_row : start_row + WIN].T[:, :, None]) * score_scale
        )
        dscores_bf = dscores.astype(jnp.bfloat16)
        query_parts.append(contract("hqk,kd->qhd", dscores_bf, key_block))
        key_grad = key_grad.at[start_row : start_row + 2 * WIN].add(
            contract("hqk,qhd->kd", dscores_bf, query_block)
        )
    return (jnp.concatenate(query_parts, axis=0), key_grad[WIN:], value_grad[WIN:])


def forward_pass(attn_full, ffn_full, block_input, segment_ids, positions, live_rows):
    qkv_w, out_w, norm_bf = attn_full
    gate_up_w, down_w = ffn_full
    norm_values = norm_bf.astype(jnp.float32)
    row_count = block_input.shape[0]
    resid_in = block_input.astype(jnp.float32)
    normed = rms_scale(resid_in, norm_values[0:D]).astype(jnp.bfloat16)
    qkv_proj = jnp.dot(normed, qkv_w, preferred_element_type=jnp.float32)
    query_raw = qkv_proj[:, : HQ * HD].reshape(row_count, HQ, HD)
    key_raw = qkv_proj[:, HQ * HD : (HQ + 1) * HD].reshape(row_count, 1, HD)
    value_bf = qkv_proj[:, (HQ + 1) * HD :].astype(jnp.bfloat16)
    cosine, sine_table = rope_tables(positions, HD)
    query_rot, key_rot = qk_prepare(
        query_raw,
        key_raw,
        norm_values[4 * D : 4 * D + HD],
        norm_values[4 * D + HD : 4 * D + 2 * HD],
        cosine,
        sine_table,
    )
    query_bf = query_rot.astype(jnp.bfloat16)
    key_bf = key_rot[:, 0, :].astype(jnp.bfloat16)
    segment_pad = front_pad(segment_ids, WIN)
    position_pad = front_pad(positions, WIN)
    live_pad = front_pad(live_rows, WIN)
    attn_out, log_total = attend_forward(query_bf, key_bf, value_bf, segment_pad, live_pad)
    attn_bf = attn_out.astype(jnp.bfloat16)
    attn_proj = jnp.dot(attn_bf, out_w, preferred_element_type=jnp.float32)
    mid_resid = resid_in + rms_scale(attn_proj, norm_values[D : 2 * D])
    ffn_in = rms_scale(mid_resid, norm_values[2 * D : 3 * D]).astype(jnp.bfloat16)
    gate_up = jnp.dot(ffn_in, gate_up_w, preferred_element_type=jnp.float32)
    gate_act = gate_up[:, :FF]
    up_act = gate_up[:, FF:]
    hidden = gated_unit(gate_act, up_act).astype(jnp.bfloat16)
    down_act = jnp.dot(hidden, down_w, preferred_element_type=jnp.float32)
    block_output = (mid_resid + rms_scale(down_act, norm_values[3 * D : 4 * D])).astype(
        jnp.bfloat16
    )
    attn_saved = (
        resid_in,
        normed,
        query_raw,
        key_raw,
        query_bf,
        key_bf,
        value_bf,
        cosine,
        sine_table,
        segment_pad,
        position_pad,
        live_pad,
        attn_bf,
        log_total,
        attn_proj,
    )
    ffn_saved = (mid_resid, ffn_in, gate_act, up_act, hidden, down_act)
    return (block_output, attn_saved, ffn_saved)


def ffn_backward(ffn_back, norm_values, ffn_saved, grad_out):
    gate_up_w, down_w = ffn_back
    mid_resid, ffn_in, gate_act, up_act, hidden, down_act = ffn_saved
    d_down, out_scale_grad = jax.vjp(rms_scale, down_act, norm_values[3 * D : 4 * D])[1](grad_out)
    d_down_bf = d_down.astype(jnp.bfloat16)
    d_hidden = jnp.dot(d_down_bf, down_w.T, preferred_element_type=jnp.float32)
    down_term = jnp.dot(hidden.T, d_down_bf, preferred_element_type=jnp.float32)
    d_gate, d_up = jax.vjp(gated_unit, gate_act, up_act)[1](d_hidden)
    d_gate_up = jnp.concatenate([d_gate, d_up], axis=1).astype(jnp.bfloat16)
    d_ffn_in = jnp.dot(d_gate_up, gate_up_w.T, preferred_element_type=jnp.float32)
    gate_up_term = jnp.dot(ffn_in.T, d_gate_up, preferred_element_type=jnp.float32)
    d_mid_part, ffn_scale_grad = jax.vjp(rms_scale, mid_resid, norm_values[2 * D : 3 * D])[1](
        d_ffn_in
    )
    return (grad_out + d_mid_part, gate_up_term, down_term, ffn_scale_grad, out_scale_grad)


def attn_backward(attn_back, attn_saved, d_mid):
    qkv_w, out_w, norm_bf = attn_back
    norm_values = norm_bf.astype(jnp.float32)
    (
        resid_in,
        normed,
        query_raw,
        key_raw,
        query_bf,
        key_bf,
        value_bf,
        cosine,
        sine_table,
        segment_pad,
        position_pad,
        live_pad,
        attn_bf,
        log_total,
        attn_proj,
    ) = attn_saved
    row_count = resid_in.shape[0]
    d_proj, post_scale_grad = jax.vjp(rms_scale, attn_proj, norm_values[D : 2 * D])[1](d_mid)
    d_proj_bf = d_proj.astype(jnp.bfloat16)
    out_term = jnp.dot(attn_bf.T, d_proj_bf, preferred_element_type=jnp.float32)
    dattn_bf = jnp.dot(d_proj_bf, out_w.T, preferred_element_type=jnp.float32).astype(jnp.bfloat16)
    d_query, d_key, d_value = attend_backward(
        query_bf, key_bf, value_bf, attn_bf, dattn_bf, log_total, segment_pad, live_pad
    )

    def prepare(query_in, key_in, q_in, k_in):
        return qk_prepare(query_in, key_in, q_in, k_in, cosine, sine_table)

    d_query_raw, d_key_raw, query_scale_grad, key_scale_grad = jax.vjp(
        prepare,
        query_raw,
        key_raw,
        norm_values[4 * D : 4 * D + HD],
        norm_values[4 * D + HD : 4 * D + 2 * HD],
    )[1]((d_query, d_key[:, None, :]))
    d_qkv = jnp.concatenate(
        [d_query_raw.reshape(row_count, HQ * HD), d_key_raw.reshape(row_count, HD), d_value], axis=1
    ).astype(jnp.bfloat16)
    d_normed = jnp.dot(d_qkv, qkv_w.T, preferred_element_type=jnp.float32)
    qkv_term = jnp.dot(normed.T, d_qkv, preferred_element_type=jnp.float32)
    d_input_part, in_scale_grad = jax.vjp(rms_scale, resid_in, norm_values[0:D])[1](d_normed)
    return (
        d_mid + d_input_part,
        qkv_term,
        out_term,
        in_scale_grad,
        post_scale_grad,
        query_scale_grad,
        key_scale_grad,
    )


def adam_update(weight, grad, first_moment, second_moment):
    first_new = beta_one * first_moment + (1.0 - beta_one) * grad
    second_new = beta_two * second_moment + (1.0 - beta_two) * grad * grad
    corr_one = 1.0 - beta_one**adam_step
    corr_two = 1.0 - beta_two**adam_step
    step_dir = (
        first_new / corr_one / (jnp.sqrt(second_new / corr_two) + adam_eps) + weight_decay * weight
    )
    return (weight - learn_rate * step_dir, first_new, second_new)


LOGICAL = pl.DeviceIdType.LOGICAL
ALL = slice(None)
SLOTS = 10


def grid_dims(count):
    return (count // 8, 2, 2, 2)


def my_place(dims):
    index = lax.axis_index("dp")
    core = lax.rem(index, dims[3])
    index = lax.div(index, dims[3])
    x = lax.rem(index, dims[2])
    index = lax.div(index, dims[2])
    return (lax.div(index, dims[1]), lax.rem(index, dims[1]), x, core)


def device_at(dims, z, y, x, core):
    return ((z * dims[1] + y) * dims[2] + x) * dims[3] + core


def enter(dims, place):
    z, y, x, core = place
    barrier = pltpu.get_barrier_semaphore()
    peers = [device_at(dims, lax.rem(z + k, dims[0]), y, x, core) for k in range(1, dims[0])]
    peers.append(device_at(dims, z, 1 - y, x, core))
    peers.append(device_at(dims, z, y, 1 - x, core))
    peers.append(device_at(dims, z, y, x, 1 - core))
    for peer in peers:
        pl.semaphore_signal(barrier, inc=1, device_id=peer, device_id_type=LOGICAL)
    pl.semaphore_wait(barrier, len(peers))


class Link:
    def __init__(self, dims, place, send_sems, recv_sems, base):
        self.dims, self.place = dims, place
        self.send_sems, self.recv_sems, self.base = send_sems, recv_sems, base
        self.pending = []

    def copy(self, src, dst, target, slot):
        return pltpu.make_async_remote_copy(
            src_ref=src,
            dst_ref=dst,
            send_sem=self.send_sems.at[self.base + slot],
            recv_sem=self.recv_sems.at[self.base + slot],
            device_id=target,
            device_id_type=LOGICAL,
        )

    def send(self, src, dst, target, slot):
        copy = self.copy(src, dst, target, slot)
        copy.start()
        self.pending.append(copy)

    def finish(self):
        for copy in self.pending:
            copy.wait_send()
        self.pending = []

    def z_peer(self, k):
        z, y, x, core = self.place
        return device_at(self.dims, lax.rem(z + k, self.dims[0]), y, x, core)

    def y_peer(self):
        z, y, x, core = self.place
        return device_at(self.dims, z, 1 - y, x, core)

    def x_peer(self):
        z, y, x, core = self.place
        return device_at(self.dims, z, y, 1 - x, core)

    def core_peer(self):
        z, y, x, core = self.place
        return device_at(self.dims, z, y, x, 1 - core)


class Gather(Link):
    def __init__(self, dims, place, view, swap, send_sems, recv_sems, base):
        super().__init__(dims, place, send_sems, recv_sems, base)
        self.view, self.swap = view, swap

    def plan(self, stage):
        z, y, x, core = self.place
        count = self.dims[0]
        view = self.view
        if stage == 0:
            return [
                (view(z, y, x, core), self.z_peer(k), k - 1, view(lax.rem(z + count - k, count), y, x, core))
                for k in range(1, count)
            ]
        slot = count + stage
        near, far = (self.y_peer(), self.x_peer()) if self.swap else (self.x_peer(), self.y_peer())
        if stage == 1:
            got = view(ALL, 1 - y, x, core) if self.swap else view(ALL, y, 1 - x, core)
            return [(view(ALL, y, x, core), near, slot, got)]
        if stage == 2:
            mine = view(ALL, ALL, x, core) if self.swap else view(ALL, y, ALL, core)
            got = view(ALL, ALL, 1 - x, core) if self.swap else view(ALL, 1 - y, ALL, core)
            return [(mine, far, slot, got)]
        if stage == 3:
            mine = view(ALL, ALL, x, core) if self.swap else view(ALL, y, ALL, core)
            got = view(ALL, ALL, x, 1 - core) if self.swap else view(ALL, y, ALL, 1 - core)
        else:
            mine = view(ALL, ALL, 1 - x, core) if self.swap else view(ALL, 1 - y, ALL, core)
            got = view(ALL, ALL, 1 - x, 1 - core) if self.swap else view(ALL, 1 - y, ALL, 1 - core)
        return [(mine, self.core_peer(), slot, got)]

    def start(self, stage):
        for src, target, slot, _ in self.plan(stage):
            self.send(src, src, target, slot)

    def wait(self, stage):
        for _, target, slot, got in self.plan(stage):
            self.copy(got, got, target, slot).wait_recv()


class Scatter(Link):
    def __init__(self, dims, place, given, held, near, far, last, swap, send_sems, recv_sems, base):
        super().__init__(dims, place, send_sems, recv_sems, base)
        self.given, self.held, self.near, self.far, self.last, self.swap = given, held, near, far, last, swap

    def start(self, stage):
        z, y, x, core = self.place
        count = self.dims[0]
        held = self.held
        if stage == 0:
            self.send(self.given(1 - core), held, self.core_peer(), 0)
        elif stage == 1:
            if self.swap:
                self.send(held.at[:, :, 1 - x], self.near, self.x_peer(), 1)
            else:
                self.send(held.at[:, 1 - y], self.near, self.y_peer(), 1)
        elif stage == 2:
            if self.swap:
                self.send(held.at[:, 1 - y, x], self.far, self.y_peer(), 2)
            else:
                self.send(held.at[:, y, 1 - x], self.far, self.x_peer(), 2)
        else:
            for k in range(1, count):
                self.send(held.at[lax.rem(z + k, count), y, x], self.last.at[k - 1], self.z_peer(k), 2 + k)

    def wait(self, stage):
        z, y, x, core = self.place
        count = self.dims[0]
        held = self.held
        if stage == 0:
            self.copy(self.given(1 - core), held, self.core_peer(), 0).wait_recv()
            mine = self.given(core)

            def add(row, carry):
                held[row] = held[row] + mine[row]
                return carry

            lax.fori_loop(0, count, add, 0)
        elif stage == 1:
            self.copy(self.near, self.near, self.core_peer(), 1).wait_recv()

            def add(row, carry):
                if self.swap:
                    held[row, :, x] = held[row, :, x] + self.near[row]
                else:
                    held[row, y] = held[row, y] + self.near[row]
                return carry

            lax.fori_loop(0, count, add, 0)
        elif stage == 2:
            self.copy(self.far, self.far, self.core_peer(), 2).wait_recv()

            def add(row, carry):
                held[row, y, x] = held[row, y, x] + self.far[row]
                return carry

            lax.fori_loop(0, count, add, 0)
        else:
            total = held[z, y, x].astype(jnp.float32)
            for k in range(1, count):
                self.copy(self.last.at[k - 1], self.last.at[k - 1], self.core_peer(), 2 + k).wait_recv()
                total = total + self.last[k - 1].astype(jnp.float32)
            return total


def own_transfers(count, width, rows):
    return count % 8 == 0 and rows * 2 % 8 == 0 and width % 512 == 0


BF16 = jnp.bfloat16
F32 = jnp.float32
LOG2E = 1.4426950408889634
ROWS = 256


def dot(left, right):
    return jnp.dot(left, right, preferred_element_type=F32)


def dot_nt(left, right):
    return lax.dot_general(left, right, (((1,), (1,)), ((), ())), preferred_element_type=F32)


def dot_tn(left, right):
    return lax.dot_general(left, right, (((0,), (0,)), ((), ())), preferred_element_type=F32)


def fold(values):
    return jnp.sum(values.reshape(values.shape[0] // 8, 8, values.shape[1]), axis=0)


def unit(values):
    scale = lax.rsqrt(jnp.mean(values * values, axis=-1, keepdims=True) + norm_eps)
    return values * scale, scale


def unit_back(grad, normal, scale):
    return scale * (grad - normal * jnp.mean(grad * normal, axis=-1, keepdims=True))


def turn_pairs(values, cosine, sine, sign):
    front, back = values[:, : HD // 2], values[:, HD // 2 :]
    if sign > 0:
        return jnp.concatenate([front * cosine - back * sine, back * cosine + front * sine], axis=1)
    return jnp.concatenate([front * cosine + back * sine, back * cosine - front * sine], axis=1)


def column_of(row):
    return jnp.broadcast_to(row, (128, 128)).T


def chunk_masks(per, start, width):
    def owner(count):
        column = lax.broadcasted_iota(jnp.int32, (count, width), 1) + start
        first = lax.broadcasted_iota(jnp.int32, (count, width), 0) * per
        return (column >= first) & (column < first + per)

    entry = lax.broadcasted_iota(jnp.int32, (128, width), 0)
    gap = (lax.broadcasted_iota(jnp.int32, (128, width), 1) + start - entry).astype(F32)
    place = (jnp.floor((gap + 0.5) * (1.0 / per)) * per == gap) & (entry < per)
    return owner, place


def spread_scales(norm_all, rows_ref, scale_ref, per, count):
    flat = norm_all.reshape(count, 8, 128)
    for device in range(count):
        rows_ref[device : device + 1, :] = flat[device, 0:1, :]
    table = rows_ref[...].astype(BF16)
    step = 512

    def part(index, carry):
        start = pl.multiple_of(index * step, step)
        owner, place = chunk_masks(per, start, step)
        spread = dot_tn(table, owner(count).astype(F32).astype(BF16))
        scale_ref[:, pl.ds(start, step)] = jnp.sum(jnp.where(place, spread, 0.0), axis=0, keepdims=True)
        return carry

    lax.fori_loop(0, count * per // step, part, 0)


class Pump:
    RATE = 46500.0
    CORE_RATE = 500000.0
    LATENCY = {"z": 2.8, "x": 1.4, "y": 1.4, "core": 1.0}

    def __init__(self):
        self.now, self.free, self.entries = 0.0, {}, []

    def launch(self, flows):
        done = self.now
        for link, size in flows:
            begin = max(self.now, self.free.get(link, 0.0))
            self.free[link] = begin + size / (self.CORE_RATE if link == "core" else self.RATE)
            done = max(done, self.free[link] + self.LATENCY[link])
        return done

    def add(self, flows, steps):
        entry = [self.launch(flows), 0, steps]
        self.entries.append(entry)
        return entry

    def first(self):
        waiting = [entry for entry in self.entries if entry[1] < len(entry[2])]
        return min(waiting, key=lambda entry: entry[0]) if waiting else None

    def fire(self, entry):
        run, flows = entry[2][entry[1]]
        run()
        self.now = max(self.now, entry[0]) + 0.3
        entry[0] = self.launch(flows)
        entry[1] += 1

    def work(self, time):
        self.now += time
        entry = self.first()
        while entry is not None and entry[0] <= self.now + 0.3:
            self.fire(entry)
            entry = self.first()

    def until(self, target):
        while target[1] < len(target[2]):
            self.fire(self.first())

    def drain(self):
        entry = self.first()
        while entry is not None:
            self.fire(entry)
            entry = self.first()


QKV_CUTS = ((0, 256), (256, 128), (384, 128), (512, 256))


def forward_kernel(dims, x_hbm, cot_hbm, pos_ref, count_ref, freq_ref, qkv_hbm, out_hbm, gate_up_hbm, down_hbm,
                   norm_ref, *rest):
    outs, scratch = rest[:25], rest[25:]
    (o_q0, o_q1, o_q2, o_q3, o_wo, o_wgu, o_wd, o_scale, o_normed, o_raw, o_query, o_key, o_value, o_attn, o_cos, o_sin,
     o_ffn_in, o_mid, o_proj, o_hidden, o_gate, o_up, o_ddown, o_out, o_sgrad) = outs
    (q0, q1, q2, q3, wo, wgu, wd, scale, normed, raw, query, key, value, attn_t, cosine, sine,
     ffn_in_t, mid, proj, hidden, gate, up, ddown, out, sgrad,
     x_ref, cot_ref, qkv_ref, out_ref, gate_up_ref, down_ref, attn, ffn_in, low, down, norm_all, norm_rows, qkv_got, gate_up_got, pair,
     send_sems, recv_sems, in_sems, out_sems) = scratch
    place = my_place(dims)
    z, y, x, core = place
    count = dims[0] * 8
    tokens = x_ref.shape[0]
    tiles = tokens // ROWS
    sources = ((qkv_hbm, qkv_ref), (out_hbm, out_ref), (gate_up_hbm, gate_up_ref), (down_hbm, down_ref), (x_hbm, x_ref), (cot_hbm, cot_ref))
    loads = [pltpu.make_async_copy(src, dst, in_sems.at[at]) for at, (src, dst) in enumerate(sources)]
    for load in loads:
        load.start()
    enter(dims, place)
    for load in loads[:4]:
        load.wait()
    stores = []

    out_slots = iter(range(48))

    def put(index, part=None):
        src, dst = scratch[index], outs[index]
        if part is not None:
            src, dst = src.at[part], dst.at[part]
        store = pltpu.make_async_copy(src, dst, out_sems.at[next(out_slots)])
        store.start()
        stores.append(store)

    link = Link(dims, place, send_sems, recv_sems, 0)
    for slot, (ref, got) in enumerate(((qkv_ref, qkv_got), (gate_up_ref, gate_up_got))):
        half = got.shape[1]
        other = pl.multiple_of((1 - core) * half, 128)
        link.send(ref.at[:, pl.ds(other, half)], got, link.core_peer(), slot)
    norm_all[z, y, x, core] = jnp.zeros(norm_all.shape[4:], F32)
    norm_all[z, y, x, core, 0:1, 0 : norm_ref.shape[1]] = norm_ref[...].astype(BF16).astype(F32)

    def pair_up(ref, got, slot):
        rows, half = got.shape
        link.copy(got, got, link.core_peer(), slot).wait_recv()
        mine = ref[:, pl.ds(pl.multiple_of(core * half, 128), half)]
        other = got[...]
        first = core == 0
        pair[0:rows, 0:half] = jnp.where(first, mine, other)
        pair[rows : 2 * rows, 0:half] = jnp.where(first, other, mine)

    step = dims[0] + 5
    bases = iter(range(2, 2 + 17 * step, step))

    def item(views):
        return [Gather(dims, place, view, swap == 1, send_sems, recv_sems, next(bases)) for swap, view in enumerate(views)]

    def block(ref, *lead):
        return lambda z, y, x, core: ref.at[(*lead, core, z, y, x)]

    def rows_of(ref, part):
        return lambda z, y, x, core: ref.at[z, y, x, core, part]

    pump = Pump()
    links = [link]

    def gather(parts, sizes):
        links.extend(parts)
        ways = [("x", "y") if not part.swap else ("y", "x") for part in parts]

        def run_near():
            for part in parts:
                part.wait(0)
                part.start(1)

        def run_far():
            for part in parts:
                part.wait(1)
                part.start(2)
                part.start(3)

        def run_core():
            for part in parts:
                part.wait(2)
                part.start(4)

        def run_last():
            for part in parts:
                part.wait(3)
                part.wait(4)

        for part in parts:
            part.start(0)
        near = [(way[0], 4 * size) for way, size in zip(ways, sizes)]
        far = [(way[1], 8 * size) for way, size in zip(ways, sizes)]
        core_flows = [("core", 8 * size) for size in sizes]
        return pump.add(
            [("z", 4 * size) for size in sizes],
            [(run_near, near), (run_far, far + core_flows), (run_core, core_flows), (run_last, [])],
        )

    wo[z, y, x, core] = out_ref[...].astype(BF16).reshape(wo.shape[4:])
    out_entry = gather(item((rows_of(wo, 0), rows_of(wo, 1))), [wo.shape[5] * D * 2] * 2)
    pair_up(qkv_ref, qkv_got, 0)
    for ref, (start, width) in zip((q0, q1, q2, q3), QKV_CUTS):
        ref[core, z, y, x] = pair[:, start : start + width].astype(BF16)
    pump.work(1.5)
    pair_bytes = pair.shape[0] * 2
    sizes = [pair_bytes * width for _, width in QKV_CUTS]
    norm_entry = gather(item((lambda z, y, x, core: norm_all.at[z, y, x, core],)), [4096])
    q_entries = [gather(item((block(q0), block(q1))), sizes[:2]), gather(item((block(q2), block(q3))), sizes[2:])]
    wd[z, y, x, core] = down_ref[...].astype(BF16).reshape(wd.shape[4:])
    down_entry = gather(item((rows_of(wd, 0), rows_of(wd, 1))), [wd.shape[5] * D * 2] * 2)
    pair_up(gate_up_ref, gate_up_got, 1)
    quarters = wgu.shape[0]
    cut = wgu.shape[-1]
    wide_entries = []
    for quarter in range(quarters):
        for colour in range(2):
            start = (2 * quarter + colour) * cut
            wgu[quarter, colour, core, z, y, x] = pair[:, start : start + cut].astype(BF16)
        wide_entries.append(gather(item((block(wgu, quarter, 0), block(wgu, quarter, 1))), [pair_bytes * cut] * 2))
    pump.work(1.0)
    live_tiles = count_ref[0]
    def table_tile(tile, carry):
        span = pl.ds(pl.multiple_of(tile * 128, 128), 128)
        position = column_of(pos_ref[pl.ds(tile, 1), :].astype(F32))
        angle = position * freq_ref[...]
        cosine[span] = jnp.cos(angle)
        sine[span] = jnp.sin(angle)
        row = lax.broadcasted_iota(jnp.int32, (128, 128), 0) + tile * 128
        low[span] = row - jnp.where(tile < live_tiles, jnp.minimum(position.astype(jnp.int32), WIN - 1), 0)
        return carry

    for begin in range(0, tokens // 128, 4):
        lax.fori_loop(begin, begin + 4, table_tile, 0)
        pump.work(1.2)
    put(14)
    put(15)
    for load in loads[4:]:
        load.wait()
    pump.until(norm_entry)
    spread_scales(norm_all, norm_rows, scale, norm_ref.shape[1], count)
    put(7)
    pump.work(1.0)
    for entry in q_entries:
        pump.until(entry)
    for index in range(4):
        put(index)

    def scales(which):
        start = (0, D, 2 * D, 3 * D, 4 * D, 4 * D + HD)[which]
        return 1.0 + scale[:, start : start + (D if which < 4 else HD)]

    def weight(ref, c):
        return ref[c].reshape(-1, ref.shape[-1])

    def project(tile, carry):
        rows = pl.ds(pl.multiple_of(tile * ROWS, ROWS), ROWS)
        normal, _ = unit(x_ref[rows].astype(F32))
        inner = (normal * scales(0)).astype(BF16)
        normed[:, rows] = inner.T
        parts = []
        for c in range(2):
            parts.append(dot(inner, weight(q0, c)))
            parts.append(dot(inner, jnp.concatenate([weight(q1, c), weight(q2, c)], axis=1)))
            parts.append(dot(inner, weight(q3, c)))
        for head in range(HQ + 2):
            part = parts[head]
            if head == HQ + 1:
                value[rows] = part.astype(BF16)
                continue
            raw[rows, head * HD : (head + 1) * HD] = part.astype(BF16)
            normal, _ = unit(part)
            turned = turn_pairs(normal * scales(5 if head == HQ else 4), cosine[rows], sine[rows], 1).astype(BF16)
            if head == HQ:
                key[rows] = turned
            else:
                query[rows, head * HD : (head + 1) * HD] = turned
        return carry

    def attend(tile):
        start = tile * ROWS
        rows = slice(start, start + ROWS)
        first = max(0, start - WIN)
        keys = slice(first, start + ROWS)
        lane = lax.broadcasted_iota(jnp.int32, (ROWS, 128), 1)
        row = lax.broadcasted_iota(jnp.int32, (ROWS, 128), 0) + start
        least = low[rows]
        for head in range(HQ):
            span = slice(head * HD, (head + 1) * HD)
            scores = dot_nt(query[rows, span], key[keys])
            parts, total = [], None
            for at in range(first, start + ROWS, 128):
                column = lane + at
                allowed = column >= least
                if at >= start:
                    allowed = allowed & (column <= row)
                part = jnp.where(allowed, jnp.exp2(scores[:, at - first : at - first + 128] * (LOG2E / HD**0.5)), 0.0)
                parts.append(part)
                total = part if total is None else total + part
            inverse = 1.0 / jnp.sum(total, axis=1, keepdims=True)
            probs = jnp.concatenate([(part * inverse).astype(BF16) for part in parts], axis=1)
            attn[rows, span] = dot(probs, value[keys]).astype(BF16)
            attn_t[span, rows] = attn[rows, span].T

    def mix(tile, carry):
        rows = pl.ds(pl.multiple_of(tile * ROWS, ROWS), ROWS)
        projected = dot(attn[rows], wo[...].reshape(-1, D))
        proj[rows] = projected
        normal, _ = unit(projected)
        middle = x_ref[rows].astype(F32) + normal * scales(1)
        mid[rows] = middle
        normal, _ = unit(middle)
        inner = (normal * scales(2)).astype(BF16)
        ffn_in[rows] = inner
        ffn_in_t[:, rows] = inner.T
        return carry

    for begin in range(0, tiles, 2):
        lax.fori_loop(begin, begin + 2, project, 0)
        pump.work(2.6)
    for index in (8, 9, 10, 11, 12):
        put(index)
    for tile in range(tiles):
        attend(tile)
        pump.work(0.5 * min(tile + 1, 3))
    put(13)
    pump.until(out_entry)
    put(4)
    for begin in range(0, tiles, 2):
        lax.fori_loop(begin, begin + 2, mix, 0)
        pump.work(1.8)
    for index in (16, 17, 18):
        put(index)
    pump.until(down_entry)
    put(6)
    wide = 2 * cut
    sgrad[...] = jnp.zeros_like(sgrad)

    def finish(rows, start, total):
        normal, factor = unit(total)
        out[rows] = (mid[rows] + normal * scales(3)).astype(BF16)
        row = start + lax.broadcasted_iota(jnp.int32, (ROWS, 1), 0)
        grad = jnp.where(row < live_tiles * TILE, cot_ref[rows].astype(F32), 0.0)
        sgrad[...] += fold(grad * normal)
        ddown[rows] = unit_back(grad * scales(3), normal, factor).astype(BF16)

    for quarter in range(quarters):
        pump.until(wide_entries[quarter])

        def feed(tile, carry):
            begin = pl.multiple_of(tile * ROWS, ROWS)
            rows = pl.ds(begin, ROWS)
            inner = ffn_in[rows]
            total = None
            for colour in range(2):
                at = colour * cut
                gated = dot(inner, weight(wgu.at[quarter, colour], 0))
                upper = dot(inner, weight(wgu.at[quarter, colour], 1))
                square = gated * gated
                bend = jnp.tanh(0.7978845608028654 * (gated + 0.044715 * square * gated))
                half = 0.5 * (1.0 + bend)
                active = gated * half
                slope = half + 0.5 * gated * (1.0 - bend * bend) * (0.7978845608028654 * (1.0 + 0.134145 * square))
                gate[quarter, rows, at : at + cut] = (slope * upper).astype(BF16)
                up[quarter, rows, at : at + cut] = active.astype(BF16)
                inside = (active * upper).astype(BF16)
                first = quarter * wide + at
                hidden[first : first + cut, rows] = inside.T
                part = wd.reshape(FF, D)[first : first + cut, :]
                part = dot(inside, part)
                total = part if total is None else total + part
            if quarter == 0:
                down[rows] = total
            elif quarter < quarters - 1:
                down[rows] = down[rows] + total
            else:
                finish(rows, begin, down[rows] + total)
            return carry

        lax.fori_loop(0, tiles, feed, 0)
        pump.work(3.8)
        for index in (5, 20, 21):
            put(index, quarter)
        put(19, pl.ds(quarter * wide, wide))
    for index in (22, 23, 24):
        put(index)
    pump.drain()
    for each in links:
        each.finish()
    for store in stores:
        store.wait()


def forward_call(dims, block_input, out_cotangent, positions, tile_count, qkv_weight, out_weight, gate_up_weight,
                 down_weight, norm_scales):
    grid = dims[:3]
    tokens = block_input.shape[0]
    rows = qkv_weight.shape[0]
    width, wide = qkv_weight.shape[1], gate_up_weight.shape[1]
    shapes = [((2,) + grid + (2 * rows, cut), BF16) for _, cut in QKV_CUTS] + [
        (grid + (2, 2, out_weight.shape[0] // 2, D), BF16),
        ((4, 2, 2) + grid + (2 * rows, FF // 8), BF16),
        (grid + (2, 2, down_weight.shape[0] // 2, D), BF16),
        ((1, norm_scales.shape[0] * dims[0] * 8), F32),
        ((D, tokens), BF16),
        ((tokens, (HQ + 1) * HD), BF16),
        ((tokens, HQ * HD), BF16),
        ((tokens, HD), BF16),
        ((tokens, HD), BF16),
        ((HQ * HD, tokens), BF16),
        ((tokens, HD // 2), F32),
        ((tokens, HD // 2), F32),
        ((D, tokens), BF16),
        ((tokens, D), F32),
        ((tokens, D), F32),
        ((FF, tokens), BF16),
        ((4, tokens, FF // 4), BF16),
        ((4, tokens, FF // 4), BF16),
        ((tokens, D), BF16),
        ((tokens, D), BF16),
        ((8, D), F32),
    ]
    sems = 2 + 17 * (dims[0] + 5)
    scratch = [pltpu.VMEM(*shape) for shape in shapes] + [
        pltpu.VMEM((tokens, D), BF16),
        pltpu.VMEM((tokens, D), BF16),
        pltpu.VMEM(qkv_weight.shape, F32),
        pltpu.VMEM(out_weight.shape, F32),
        pltpu.VMEM(gate_up_weight.shape, F32),
        pltpu.VMEM(down_weight.shape, F32),
        pltpu.VMEM((tokens, HQ * HD), BF16),
        pltpu.VMEM((tokens, D), BF16),
        pltpu.VMEM((tokens, 128), jnp.int32),
        pltpu.VMEM((tokens, D), F32),
        pltpu.VMEM(grid + (2, 8, 128), F32),
        pltpu.VMEM((dims[0] * 8, 128), F32),
        pltpu.VMEM((rows, width // 2), F32),
        pltpu.VMEM((rows, wide // 2), F32),
        pltpu.VMEM((2 * rows, wide // 2), F32),
        pltpu.SemaphoreType.DMA((sems,)),
        pltpu.SemaphoreType.DMA((sems,)),
        pltpu.SemaphoreType.DMA((6,)),
        pltpu.SemaphoreType.DMA((48,)),
    ]
    vmem = pl.BlockSpec(memory_space=pltpu.VMEM)
    hbm = pl.BlockSpec(memory_space=pltpu.HBM)
    frequency = np.power(rope_base, -np.arange(HD // 2) * (2.0 / HD)).astype(np.float32)[None, :]
    return pl.pallas_call(
        functools.partial(forward_kernel, dims),
        out_shape=[jax.ShapeDtypeStruct(*shape) for shape in shapes],
        in_specs=[hbm, hbm, vmem, pl.BlockSpec(memory_space=pltpu.SMEM), vmem] + [hbm] * 4 + [vmem],
        out_specs=[hbm] * len(shapes),
        scratch_shapes=scratch,
        compiler_params=pltpu.CompilerParams(collective_id=0, has_side_effects=True, vmem_limit_bytes=63 << 20),
        name="forward",
    )(block_input, out_cotangent, positions.reshape(-1, 128), tile_count, frequency, qkv_weight, out_weight,
      gate_up_weight, down_weight, norm_scales[None, :])


def backward_kernel(dims, *refs):
    (h_q0, h_q1, h_q2, h_q3, h_wo, h_wgu, h_wd, scale, h_normed, h_raw, h_query, h_key, h_value, h_attn, h_cos, h_sin,
     h_ffn_in, h_mid, h_proj, h_hidden, h_gate, h_up, h_ddown, sgrad_out, h_x, h_cot, pos_ref, count_ref) = refs[:28]
    o_input, o_qkv, o_wo, o_wgu, o_wd, o_norm = refs[28:34]
    (wo, wgu, wd, gq0, gq1, gq2, gq3, go, gg, gd, gn,
     pool, dgu, ddown, ffn_in, attn, dproj, dmid, proj, sine, totals, grow, gtab, bounce, swaps, halves,
     in_sems, out_sem, send_sems, recv_sems) = refs[34:64]
    buffers = list(refs[64:])
    place = my_place(dims)
    z, y, x, core = place
    count = dims[0] * 8
    tokens = dmid.shape[0]
    tiles = tokens // ROWS
    cut = wgu.shape[-1]
    serial = iter(range(64))

    def load(src, dst):
        copy = pltpu.make_async_copy(src, dst, in_sems.at[next(serial)])
        copy.start()
        return copy

    c_ddown = load(h_ddown, ddown)
    c_hidden = [load(h_hidden.at[pl.ds(512 * j, 512)], pool.at[pl.ds(512 * j, 512)]) for j in range(4)]
    c_wd = load(h_wd, wd)
    c_gate = [(load(h_gate.at[j], dgu.at[0, j]), load(h_up.at[j], dgu.at[1, j])) for j in range(4)]
    c_ffn_in = load(h_ffn_in, ffn_in)
    c_p3 = [load(h_wgu, wgu), load(h_mid, dmid), load(h_proj, proj), load(h_attn, attn), load(h_wo, wo)]
    enter(dims, place)

    pump = Pump()
    step = dims[0] + 5
    bases = iter(range(12, 12 + 19 * step, step))
    links = []

    def scatter(givens, done):
        parts = []
        for swap, given in enumerate(givens):
            held, near, far, last = buffers[:4]
            del buffers[:4]
            parts.append(Scatter(dims, place, given, held, near, far, last, swap == 1, send_sems, recv_sems, next(bases)))
        links.extend(parts)

        def stage(which):
            def run():
                for part in parts:
                    part.wait(which)
                    part.start(which + 1)

            return run

        def last_stage():
            for colour, part in enumerate(parts):
                done(colour, part.wait(3))

        for part in parts:
            part.start(0)
        sizes = [math.prod(part.last.shape[1:]) * part.last.dtype.itemsize for part in parts]
        ways = [("x", "y") if part.swap else ("y", "x") for part in parts]
        near = [(way[0], 8 * size) for way, size in zip(ways, sizes)]
        far = [(way[1], 4 * size) for way, size in zip(ways, sizes)]
        pump.add(
            [("core", 16 * size) for size in sizes],
            [(stage(0), near), (stage(1), far), (stage(2), [("z", 4 * size) for size in sizes]), (last_stage, [])],
        )

    swap_link = Link(dims, place, send_sems, recv_sems, 0)
    links.append(swap_link)
    fetched = []

    def split_rows(slot, target, start):
        def done(colour, total):
            at = slot + colour
            rows, width = target.shape[0], total.shape[1]
            first = start[colour]
            half = target.shape[1] // 2
            bounce[at % 2, :, 0:width] = total
            low, high = bounce[at % 2, 0:rows, 0:width], bounce[at % 2, rows : 2 * rows, 0:width]
            target[:, pl.ds(pl.multiple_of(core * half + first, 128), width)] = jnp.where(core == 0, low, high)
            swaps[at, :, 0:width] = jnp.where(core == 0, high, low)
            span = (at, slice(None), pl.ds(0, width))
            swap_link.send(swaps.at[span], halves.at[span], swap_link.core_peer(), at)

            def fetch():
                swap_link.copy(halves.at[span], halves.at[span], swap_link.core_peer(), at).wait_recv()
                target[:, pl.ds(pl.multiple_of((1 - core) * half + first, 128), width)] = halves[at, :, 0:width]

            fetched.append(fetch)

        return done

    def rows_done(target, start):
        def done(colour, total):
            height = total.shape[0]
            first = start + colour * height
            target[first : first + height, :] = total

        return done

    def scales(which):
        start = (0, D, 2 * D, 3 * D, 4 * D, 4 * D + HD)[which]
        return 1.0 + scale[:, start : start + (D if which < 4 else HD)]

    def weight(ref, c):
        return ref[c].reshape(-1, ref.shape[-1])

    def some_rows(tile):
        return pl.ds(pl.multiple_of(tile * ROWS, ROWS), ROWS)

    c_ddown.wait()
    grown = gd.reshape(FF, D)
    for copy in c_hidden:
        copy.wait()

    def down_part(part, carry):
        rows = pl.ds(pl.multiple_of(part * 512, 512), 512)
        grown[rows, :] = dot(pool[rows, :], ddown[...]).astype(BF16)
        return carry

    lax.fori_loop(0, FF // 512, down_part, 0)
    for sub in range(2):
        scatter([(lambda core, k=2 * sub + k: gd.at[:, :, :, core, k]) for k in range(2)],
                rows_done(o_wd, sub * 2 * gd.shape[5]))
    queries, others = pool.at[pl.ds(0, tokens)], pool.at[pl.ds(tokens, tokens)]
    c_query = [load(h_query, queries), load(h_key, others.at[:, pl.ds(0, HD)]), load(h_value, others.at[:, pl.ds(HD, HD)])]
    c_wd.wait()
    c_ffn_in.wait()
    down_rows = wd.reshape(FF, D)
    for quarter in range(4):
        for copy in c_gate[quarter]:
            copy.wait()
        last_rows = slice(quarter * 512, (quarter + 1) * 512)

        def spread(tile, carry, quarter=quarter, last_rows=last_rows):
            rows = some_rows(tile)
            grad = dot_nt(ddown[rows], down_rows[last_rows, :])
            dgu[0, quarter, rows] = (grad * dgu[0, quarter, rows].astype(F32)).astype(BF16)
            dgu[1, quarter, rows] = (grad * dgu[1, quarter, rows].astype(F32)).astype(BF16)
            return carry

        lax.fori_loop(0, tiles, spread, 0)
        pump.work(1.2)

        def wide_part(c, carry, quarter=quarter):
            for colour in range(2):
                span = slice(colour * cut, (colour + 1) * cut)
                gg[quarter, colour, c] = dot(ffn_in[...], dgu[c, quarter, :, span]).astype(BF16).reshape(gg.shape[3:])
            return carry

        lax.fori_loop(0, 2, wide_part, 0)
        pump.work(1.8)
        scatter([(lambda core, q=quarter, k=k: gg.at[q, k, core]) for k in range(2)],
                split_rows(2 * quarter, o_wgu, [(2 * quarter + k) * cut for k in range(2)]))
        pump.work(0.1)
    xc = ddown
    c_p3.append(load(h_cot, xc))
    c_normed = load(h_normed, ffn_in)
    for copy in c_p3:
        copy.wait()
    names = ("in", "post", "ffn", "out", "query", "key")
    sums = dict(zip(names, (slice(8 * index, 8 * index + 8) for index in range(6))))
    totals[...] = jnp.zeros_like(totals)

    def collect(which, values):
        totals[sums[which], 0 : values.shape[1]] += fold(values)

    def middle_tile(tile, carry):
        rows = some_rows(tile)
        grad = None
        for quarter in range(4):
            for c in range(2):
                part = jnp.concatenate([weight(wgu.at[quarter, colour], c) for colour in range(2)], axis=1)
                part = dot_nt(dgu[c, quarter, rows], part)
                grad = part if grad is None else grad + part
        row = tile * ROWS + lax.broadcasted_iota(jnp.int32, (ROWS, 1), 0)
        given = jnp.where(row < count_ref[0] * TILE, xc[rows].astype(F32), 0.0)
        normal, factor = unit(dmid[rows])
        collect("ffn", grad * normal)
        middle = given + unit_back(grad * scales(2), normal, factor)
        dmid[rows] = middle
        normal, factor = unit(proj[rows])
        collect("post", middle * normal)
        dproj[rows] = unit_back(middle * scales(1), normal, factor).astype(BF16)
        return carry

    for begin in range(0, tiles, 2):
        lax.fori_loop(begin, begin + 2, middle_tile, 0)
        pump.work(4.4)
    c_raw = [load(h_raw.at[:, pl.ds(0, 512)], dgu.at[0, 0]), load(h_raw.at[:, pl.ds(512, 512)], dgu.at[0, 1]),
             load(h_raw.at[:, pl.ds(1024, HD)], dgu.at[0, 2, :, pl.ds(0, HD)])]
    cosine = proj.at[:, pl.ds(2 * HD, HD // 2)]
    c_rest = [load(h_cos, cosine), load(h_sin, sine), load(h_x, xc)]
    wq = wd.reshape(FF, D)
    c_qkv = []
    for c in range(2):
        for ref, within, lane in ((h_q0, 0, 0), (h_q1, 1, 0), (h_q2, 1, 128), (h_q3, 2, 0)):
            head = 3 * c + within
            at = pl.ds(head % 2 * HD + lane, ref.shape[-1])
            c_qkv.append(load(ref.at[c], wq.at[pl.ds(head // 2 * D, D), at]))
    grown_out = go.reshape(HQ * HD, D)
    for half in range(2):
        rows = slice(half * 512, (half + 1) * 512)
        grown_out[rows, :] = dot(attn[rows, :], dproj[...]).astype(BF16)
    scatter([(lambda core, k=k: go.at[:, :, :, core, k]) for k in range(2)], rows_done(o_wo, 0))
    out_rows = wo.reshape(HQ * HD, D)
    pump.work(1.9)

    def attn_grad(tile, carry):
        rows = some_rows(tile)
        attn[rows] = dot_nt(dproj[rows], out_rows[...]).astype(BF16)
        return carry

    lax.fori_loop(0, tiles, attn_grad, 0)
    pump.work(1.9)
    for copy in c_query + c_raw + c_rest:
        copy.wait()
    dkey, dvalue = proj.at[:, pl.ds(0, HD)], proj.at[:, pl.ds(HD, HD)]

    for tile in range(tiles):
        start = tile * ROWS
        rows = slice(start, start + ROWS)
        first = max(0, start - WIN)
        keys = slice(first, start + ROWS)
        height = start + ROWS - first
        position = jnp.concatenate([pos_ref[2 * tile : 2 * tile + 1, :], pos_ref[2 * tile + 1 : 2 * tile + 2, :]], axis=1)
        row = lax.broadcasted_iota(jnp.int32, (1, ROWS), 1) + start
        reach = jnp.where(row < count_ref[0] * TILE, jnp.minimum(position, WIN - 1), 0)
        column = lax.broadcasted_iota(jnp.int32, (height, ROWS), 0) + first
        allowed = (column >= row - reach) & (column <= row)
        dvalue[rows, :] = jnp.zeros((ROWS, HD), F32)
        dkey[rows, :] = jnp.zeros((ROWS, HD), F32)

        def two_heads(pair, carry, rows=rows, keys=keys, allowed=allowed):
            key, value = others[keys, 0:HD], others[keys, HD : 2 * HD]
            probs_all, scores_all, query_all, grads_all = [], [], [], []
            for each in range(2):
                span = pl.ds(pl.multiple_of((2 * pair + each) * HD, HD), HD)
                query = queries[rows, span]
                grad = attn[rows, span]
                weights = jnp.where(allowed, jnp.exp2(dot_nt(key, query) * (LOG2E / HD**0.5)), 0.0)
                probs = weights * (1.0 / jnp.sum(weights, axis=0, keepdims=True))
                grad_probs = dot_nt(value, grad)
                both = probs * grad_probs
                delta = jnp.sum(both, axis=0, keepdims=True)
                scores = ((both - probs * delta) * HD**-0.5).astype(BF16)
                probs_all.append(probs.astype(BF16))
                scores_all.append(scores)
                query_all.append(query)
                grads_all.append(grad)
            dvalue[keys, :] += dot(jnp.concatenate(probs_all, axis=1), jnp.concatenate(grads_all, axis=0))
            dkey[keys, :] += dot(jnp.concatenate(scores_all, axis=1), jnp.concatenate(query_all, axis=0))
            for each in range(2):
                span = pl.ds(pl.multiple_of((2 * pair + each) * HD, HD), HD)
                grad = turn_pairs(dot_tn(scores_all[each], key), cosine[rows, :], sine[rows, :], -1)
                normal, factor = unit(dgu[0, pair, rows, each * HD : (each + 1) * HD].astype(F32))
                collect("query", grad * normal)
                queries[rows, span] = unit_back(grad * scales(4), normal, factor).astype(BF16)
            return carry

        lax.fori_loop(0, HQ // 2, two_heads, 0)
        pump.work((1.3, 2.3, 3.3, 3.3)[min(tile, 3)])

    def key_tile(tile, carry):
        rows = some_rows(tile)
        grad = turn_pairs(dkey[rows, :], cosine[rows, :], sine[rows, :], -1)
        normal, factor = unit(dgu[0, 2, rows, 0:HD].astype(F32))
        collect("key", grad * normal)
        others[rows, 2 * HD : 3 * HD] = unit_back(grad * scales(5), normal, factor).astype(BF16)
        others[rows, 3 * HD : 4 * HD] = dvalue[rows, :].astype(BF16)
        return carry

    lax.fori_loop(0, tiles, key_tile, 0)
    pump.work(1.0)
    c_normed.wait()

    def grad_columns(rows, head):
        ref, at = (queries, head * HD) if head < HQ else (others, (head - HQ + 2) * HD)
        return ref[rows, at : at + HD]

    for head in range(HQ + 2):
        term = dot(ffn_in[...], grad_columns(slice(0, tokens), head)).astype(BF16)
        c, within = head // 3, head % 3
        if within == 0:
            gq0[c] = term.reshape(gq0.shape[1:])
        elif within == 2:
            gq3[c] = term.reshape(gq3.shape[1:])
        else:
            gq1[c] = term[:, 0:128].reshape(gq1.shape[1:])
            gq2[c] = term[:, 128:256].reshape(gq2.shape[1:])
    for sub, pair in enumerate(((gq0, gq1), (gq2, gq3))):
        scatter([(lambda core, ref=ref: ref.at[core]) for ref in pair],
                split_rows(8 + 2 * sub, o_qkv, [QKV_CUTS[2 * sub + k][0] for k in range(2)]))
    pump.work(2.8)
    for copy in c_qkv:
        copy.wait()

    def input_tile(tile, carry):
        rows = some_rows(tile)
        grad = None
        for head in range(HQ + 2):
            part = wq[head // 2 * D : (head // 2 + 1) * D, head % 2 * HD : (head % 2 + 1) * HD]
            part = dot_nt(grad_columns(rows, head), part)
            grad = part if grad is None else grad + part
        normal, factor = unit(xc[rows].astype(F32))
        collect("in", grad * normal)
        dmid[rows] = dmid[rows] + unit_back(grad * scales(0), normal, factor)
        return carry

    lax.fori_loop(0, tiles, input_tile, 0)
    pump.work(4.4)
    store = pltpu.make_async_copy(dmid, o_input, out_sem)
    store.start()
    totals[sums["out"]] = sgrad_out[...]
    at = 0
    for index, name in enumerate(names):
        size = D if index < 4 else HD
        grow[:, at : at + size] = jnp.sum(totals[sums[name], 0:size], axis=0, keepdims=True)
        at += size
    per = at // count

    def chunk_part(index, table):
        begin = pl.multiple_of(index * 512, 512)
        owner, entry = chunk_masks(per, begin, 512)
        picked = entry.astype(F32).astype(BF16)
        rest = jnp.where(owner(count), grow[:, pl.ds(begin, 512)], 0.0)
        for _ in range(3):
            piece = rest.astype(BF16)
            rest = rest - piece.astype(F32)
            table = table + dot_nt(piece, picked)
        return table

    gtab[...] = lax.fori_loop(0, at // 512, chunk_part, jnp.zeros((count, 128), F32))
    flat = gn.reshape(count, 8, 128)
    for device in range(count):
        flat[device] = jnp.broadcast_to(gtab[device : device + 1, :], (8, 128))

    def norm_done(colour, total):
        o_norm[...] = total

    scatter([lambda core: gn.at[:, :, :, core]], norm_done)
    pump.drain()
    for fetch in fetched:
        fetch()
    for link in links:
        link.finish()
    store.wait()


def backward_call(dims, saved, block_input, out_cotangent, positions, tile_count, shard_rows):
    grid = dims[:3]
    count = dims[0] * 8
    tokens = block_input.shape[0]
    qkv_rows, out_rows, down_rows, norm_rows = shard_rows
    width = (HQ + 2) * HD
    bf = lambda *shape: pltpu.VMEM(shape, BF16)
    fp = lambda *shape: pltpu.VMEM(shape, F32)
    pair = 2 * qkv_rows
    weights = [bf(*((2,) + grid + (pair, cut))) for _, cut in QKV_CUTS] + [
        bf(*(grid + (2, 2, out_rows // 2, D))),
        bf(*((4, 2, 2) + grid + (pair, FF // 8))),
        bf(*(grid + (2, 2, down_rows // 2, D))),
    ]
    scratch = weights[4:] + weights[:6] + [
        bf(*(grid + (2, 4, down_rows // 4, D))),
        fp(*(grid + (2, 8, 128))),
        bf(FF, tokens),
        bf(2, 4, tokens, FF // 4),
        bf(tokens, D),
        bf(D, tokens),
        bf(HQ * HD, tokens),
        bf(tokens, D),
        fp(tokens, D),
        fp(tokens, D),
        fp(tokens, HD // 2),
        fp(48, D),
        fp(1, 4 * D + 2 * HD),
        fp(count, 128),
        fp(2, pair, 256),
        fp(12, qkv_rows, 256),
        fp(12, qkv_rows, 256),
        pltpu.SemaphoreType.DMA((64,)),
        pltpu.SemaphoreType.DMA,
    ]
    sems = 12 + 19 * (dims[0] + 5)
    scratch += [pltpu.SemaphoreType.DMA((sems,)), pltpu.SemaphoreType.DMA((sems,))]
    blocks = [[(down_rows // 4, D)] * 2] * 2 + [[(pair, FF // 8)] * 2] * 4 + [[(out_rows // 2, D)] * 2]
    blocks += [[(pair, QKV_CUTS[0][1]), (pair, QKV_CUTS[1][1])], [(pair, QKV_CUTS[2][1]), (pair, QKV_CUTS[3][1])], [(8, 128)]]
    for colours in blocks:
        for swap, block in enumerate(colours):
            make = fp if block == (8, 128) else bf
            scratch.append(make(*(grid + block)))
            scratch.append(make(*(((grid[0], grid[1]) if swap else (grid[0], grid[2])) + block)))
            scratch.append(make(*((grid[0],) + block)))
            scratch.append(make(*((grid[0] - 1,) + block)))
    vmem = pl.BlockSpec(memory_space=pltpu.VMEM)
    hbm = pl.BlockSpec(memory_space=pltpu.HBM)
    outs = [(tokens, D), (qkv_rows, width), (out_rows, D), (qkv_rows, 2 * FF), (down_rows, D), (8, 128)]
    saved = list(saved)
    saved[:4] = [array.reshape(2, D, -1) for array in saved[:4]]
    inputs = saved[:23] + [saved[24], block_input, out_cotangent, positions.reshape(-1, 128), tile_count]
    specs = [hbm] * 28
    specs[7] = specs[23] = specs[26] = vmem
    specs[27] = pl.BlockSpec(memory_space=pltpu.SMEM)
    return pl.pallas_call(
        functools.partial(backward_kernel, dims),
        out_shape=[jax.ShapeDtypeStruct(shape, F32) for shape in outs],
        in_specs=specs,
        out_specs=[hbm] + [vmem] * 5,
        scratch_shapes=scratch,
        compiler_params=pltpu.CompilerParams(collective_id=1, has_side_effects=True, vmem_limit_bytes=67043328),
        name="backward",
    )(*inputs)


def adam_kernel(*refs):
    ins, outs, bufs = refs[:22], refs[22:44], refs[44:66]
    last, in_sems, out_sems = refs[66:]
    loads = [pltpu.make_async_copy(src, buf, in_sems.at[at]) for at, (src, buf) in enumerate(zip(ins, bufs))]
    stores = [
        pltpu.make_async_copy(buf, dst, out_sems.at[at]) if buf.shape == dst.shape else None
        for at, (buf, dst) in enumerate(zip(bufs, outs))
    ]
    for load in loads:
        load.start()
    for item in range(5):
        span = range(4 * item, 4 * item + 4)
        for at in span:
            loads[at].wait()
        grad, weight, first, second = (bufs[at] for at in span)
        given = grad[0 : weight.shape[0], 0 : weight.shape[1]]
        if given.shape == grad.shape:
            stores[4 * item].start()
        else:
            last[...] = given
            pltpu.make_async_copy(last, outs[4 * item], out_sems.at[4 * item]).start()
        news = adam_update(weight[...], given, first[...], second[...])
        for ref, new in zip((weight, first, second), news):
            ref[...] = new
        for at in span[1:]:
            stores[at].start()
    for at in (20, 21):
        loads[at].wait()
        stores[at].start()
    for at, store in enumerate(stores):
        if bufs[at].shape == outs[at].shape:
            store.wait()
        else:
            pltpu.make_async_copy(last, outs[at], out_sems.at[at]).wait()


def adam_call(groups, passed):
    flat = [array if array.ndim == 2 else array[None, :] for group in groups for array in group] + list(passed)
    heads = [flat[at + 1] if at < 20 and at % 4 == 0 else array for at, array in enumerate(flat)]
    hbm = pl.BlockSpec(memory_space=pltpu.HBM)
    outs = pl.pallas_call(
        adam_kernel,
        out_shape=[jax.ShapeDtypeStruct(array.shape, array.dtype) for array in heads],
        in_specs=[hbm] * 22,
        out_specs=[hbm] * 22,
        scratch_shapes=[pltpu.VMEM(array.shape, array.dtype) for array in flat]
        + [pltpu.VMEM(flat[17].shape, F32), pltpu.SemaphoreType.DMA((22,)), pltpu.SemaphoreType.DMA((22,))],
        compiler_params=pltpu.CompilerParams(vmem_limit_bytes=67043328),
        name="adam",
    )(*flat)
    results = []
    for item, group in enumerate(groups):
        shape = group[1].shape
        results.append([array.reshape(shape) for array in outs[4 * item : 4 * item + 4]])
    return results, outs[20:]


def plain_pass(
    block_input,
    out_cotangent,
    segment_ids,
    positions,
    tile_count,
    qkv_weight,
    out_weight,
    gate_up_weight,
    down_weight,
    norm_scales,
):
    qkv_full, out_full, gate_up_full, down_full, norm_full = (
        lax.all_gather(array.astype(jnp.bfloat16), "dp", axis=0, tiled=True)
        for array in (qkv_weight, out_weight, gate_up_weight, down_weight, norm_scales)
    )
    attn_full = (qkv_full, out_full, norm_full)
    ffn_full = (gate_up_full, down_full)
    row_count = block_input.shape[0]
    live_rows = jnp.arange(row_count, dtype=jnp.int32) // TILE < tile_count[0]
    block_output, attn_saved, ffn_saved = forward_pass(
        attn_full, ffn_full, block_input, segment_ids, positions, live_rows
    )
    attn_back, ffn_back = attn_full, ffn_full
    grad_out = out_cotangent.astype(jnp.float32) * live_rows[:, None].astype(jnp.float32)
    d_mid, gate_up_term, down_term, ffn_scale_grad, out_scale_grad = ffn_backward(
        ffn_back, attn_back[2].astype(jnp.float32), ffn_saved, grad_out
    )
    (
        input_grad,
        qkv_term,
        out_term,
        in_scale_grad,
        post_scale_grad,
        query_scale_grad,
        key_scale_grad,
    ) = attn_backward(attn_back, attn_saved, d_mid)
    norm_term = jnp.concatenate(
        [
            in_scale_grad,
            post_scale_grad,
            ffn_scale_grad,
            out_scale_grad,
            query_scale_grad,
            key_scale_grad,
        ]
    )
    sums = tuple(
        lax.psum_scatter(term, "dp", scatter_dimension=0, tiled=True)
        for term in (qkv_term, out_term, gate_up_term, down_term, norm_term)
    )
    return (block_output, input_grad) + sums


def shards(
    count,
    block_input,
    out_cotangent,
    segment_ids,
    positions,
    tile_count,
    qkv_weight,
    qkv_first,
    qkv_second,
    out_weight,
    out_first,
    out_second,
    gate_up_weight,
    gate_up_first,
    gate_up_second,
    down_weight,
    down_first,
    down_second,
    norm_scales,
    norm_first,
    norm_second,
):
    dims = grid_dims(count)
    if own_transfers(count, qkv_weight.shape[1], qkv_weight.shape[0]):
        saved = forward_call(
            dims, block_input, out_cotangent, positions, tile_count, qkv_weight, out_weight, gate_up_weight, down_weight,
            norm_scales,
        )
        block_output = saved[23]
        shard_rows = (qkv_weight.shape[0], out_weight.shape[0], down_weight.shape[0], norm_scales.shape[0])
        input_grad, qkv_grad, out_grad, gate_up_grad, down_grad, norm_grad = backward_call(
            dims, saved, block_input, out_cotangent, positions, tile_count, shard_rows
        )
    else:
        block_output, input_grad, qkv_grad, out_grad, gate_up_grad, down_grad, norm_grad = plain_pass(
            block_input, out_cotangent, segment_ids, positions, tile_count, qkv_weight, out_weight, gate_up_weight,
            down_weight, norm_scales,
        )
    (
        (
            (qkv_grad, qkv_new, qkv_first_new, qkv_second_new),
            (out_grad, out_new, out_first_new, out_second_new),
            (gate_up_grad, gate_up_new, gate_up_first_new, gate_up_second_new),
            (down_grad, down_new, down_first_new, down_second_new),
            (norm_grad, norms_new, norm_first_new, norm_second_new),
        ),
        (block_output, input_grad),
    ) = adam_call(
        (
            (qkv_grad, qkv_weight, qkv_first, qkv_second),
            (out_grad, out_weight, out_first, out_second),
            (gate_up_grad, gate_up_weight, gate_up_first, gate_up_second),
            (down_grad, down_weight, down_first, down_second),
            (norm_grad, norm_scales, norm_first, norm_second),
        ),
        (block_output, input_grad),
    )
    return (
        block_output,
        input_grad,
        qkv_grad,
        out_grad,
        gate_up_grad,
        down_grad,
        norm_grad,
        qkv_new,
        out_new,
        gate_up_new,
        down_new,
        norms_new,
        qkv_first_new,
        out_first_new,
        gate_up_first_new,
        down_first_new,
        norm_first_new,
        qkv_second_new,
        out_second_new,
        gate_up_second_new,
        down_second_new,
        norm_second_new,
    )


def solution(mesh):
    in_specs = (
        P("dp", None),
        P("dp", None),
        P("dp"),
        P("dp"),
        P("dp"),
        P("dp", None),
        P("dp", None),
        P("dp", None),
        P("dp", None),
        P("dp", None),
        P("dp", None),
        P("dp", None),
        P("dp", None),
        P("dp", None),
        P("dp", None),
        P("dp", None),
        P("dp", None),
        P("dp"),
        P("dp"),
        P("dp"),
    )
    out_specs = (
        P("dp", None),
        P("dp", None),
        P("dp", None),
        P("dp", None),
        P("dp", None),
        P("dp", None),
        P("dp"),
        P("dp", None),
        P("dp", None),
        P("dp", None),
        P("dp", None),
        P("dp"),
        P("dp", None),
        P("dp", None),
        P("dp", None),
        P("dp", None),
        P("dp"),
        P("dp", None),
        P("dp", None),
        P("dp", None),
        P("dp", None),
        P("dp"),
    )
    body = functools.partial(shards, mesh.shape["dp"])
    return jax.shard_map(body, mesh=mesh, in_specs=in_specs, out_specs=out_specs, check_vma=False)
```
